32 devices in a mesh: dp: 4 (over y, x), ctx: 2 (over core), tensor: 4 (over z).
Axes of the slice: x: 2, y: 2, z: 4, core: 2. Of those that a mesh axis runs over, the one named last changes fastest.
Arguments:
- prompt_in: bfloat16 [4, 1024, 2048], P('dp', 'ctx'), may hold values from -6 to 6
- cont_in: bfloat16 [4, 8, 128, 2048], P('dp', 'ctx'), may hold values from -6 to 6
- prompt_len: int32 [4], P('dp'), may hold values from 256 to 1024, as said below
- norm_attn: bfloat16 [2048], replicated, may hold values from 0.5 to 1.5
- w_query: bfloat16 [2048, 2048], P(None, 'tensor'), may hold values from -0.4375 to 0.4375
- key_weight: bfloat16 [2048, 512], P(None, 'tensor'), may hold values from -0.4375 to 0.4375
- value_weight: bfloat16 [2048, 512], P(None, 'tensor'), may hold values from -0.125 to 0.125
- w_out: bfloat16 [2048, 2048], P('tensor'), may hold values from -4 to 4
- norm_mlp: bfloat16 [2048], replicated, may hold values from 0.5 to 1.5
- w_gate: bfloat16 [2048, 8192], P(None, 'tensor'), may hold values from -0.125 to 0.125
- w_up: bfloat16 [2048, 8192], P(None, 'tensor'), may hold values from -0.125 to 0.125
- w_down: bfloat16 [8192, 2048], P('tensor'), may hold values from -0.5 to 0.5
- prompt_cot: bfloat16 [4, 1024, 2048], P('dp', 'ctx'), may hold values from -6 to 6
- cont_cot: bfloat16 [4, 8, 128, 2048], P('dp', 'ctx'), may hold values from -6 to 6
Outputs:
- prompt_out: bfloat16 [4, 1024, 2048], P('dp', 'ctx')
- cont_out: bfloat16 [4, 8, 128, 2048], P('dp', 'ctx')
- prompt_grad: bfloat16 [4, 1024, 2048], P('dp', 'ctx')
- cont_grad: bfloat16 [4, 8, 128, 2048], P('dp', 'ctx')
- grad_norm_attn: float32 [2048], P(('dp', 'ctx'))
- grad_query: float32 [2048, 2048], P(('dp', 'ctx'), 'tensor')
- grad_key: float32 [2048, 512], P(('dp', 'ctx'), 'tensor')
- grad_value: float32 [2048, 512], P(('dp', 'ctx'), 'tensor')
- grad_out: float32 [2048, 2048], P('tensor', ('dp', 'ctx'))
- grad_norm_mlp: float32 [2048], P(('dp', 'ctx'))
- grad_gate: float32 [2048, 8192], P(('dp', 'ctx'), 'tensor')
- grad_up: float32 [2048, 8192], P(('dp', 'ctx'), 'tensor')
- grad_down: float32 [8192, 2048], P('tensor', ('dp', 'ctx'))
The draws below stay inside these ranges and needn't reach their ends.
Inputs may be any that keep to these rules, and one draw needn't show every extreme that they name: `prompt_len`: in every draw at least one prompt has all 1024 tokens valid.
All inputs are finite; a program needn't handle non-finite values.
Results may differ from the reference program's by a relative error of at most 0.015.
Values may be sent and summed in bfloat16 or wider, within the bound.
A program may use at most 320 MiB of HBM per device.

```python
import math
import jax
import jax.numpy as jnp
from jax import lax

MODEL_WIDTH = 2048
QUERY_HEADS = 32
KEY_VALUE_HEADS = 8
HEAD_WIDTH = 64
FF = 8192
PROMPT_LENGTH = 1024
CONT_LENGTH = 128
GROUPS = 4
CONTINUATIONS = 8


def draw_prompt_len(key, part):
    drawn = jax.random.randint(key, (GROUPS,), PROMPT_LENGTH // 4, PROMPT_LENGTH + 1, dtype=jnp.int32)
    chosen = jax.random.randint(jax.random.fold_in(key, 7), (), 0, GROUPS, dtype=jnp.int32)
    return jnp.where(jnp.arange(GROUPS, dtype=jnp.int32) == chosen, PROMPT_LENGTH, drawn).astype(jnp.int32)


def shard_levels(own_key, shape, cuts, least, largest):
    level, own = 1.0, jax.random.fold_in(own_key, 6)
    for dim, shards_of in cuts:
        heights = jnp.exp(jax.random.uniform(jax.random.fold_in(own, dim), (shards_of,), jnp.float32, least / len(cuts), largest / len(cuts)))
        level = level * jnp.repeat(heights, shape[dim] // shards_of).reshape([-1 if axis == dim else 1 for axis in range(len(shape))])
    return level


def gaussian(key, dims, scale, bound, shards=(), kind=jnp.bfloat16):
    level = shard_levels(key, dims, shards, -0.22, 0.18) if shards else 1.0
    values = jax.random.normal(key, dims, jnp.float32) * scale * level
    return jnp.minimum(jnp.maximum(values, -bound), bound).astype(kind)


def setup_inputs(seed: int = 0) -> dict:
    keys = jax.random.split(jax.random.key(seed), 15)
    return {
        "prompt_in": gaussian(keys[0], (GROUPS, PROMPT_LENGTH, MODEL_WIDTH), 1.0, 6.0, ((0, 4), (1, 2))),
        "cont_in": gaussian(keys[1], (GROUPS, CONTINUATIONS, CONT_LENGTH, MODEL_WIDTH), 1.0, 6.0, ((0, 4), (1, 2))),
        "prompt_len": draw_prompt_len(jax.random.fold_in(keys[14], 71), 0),
        "norm_attn": jnp.clip(1.0 + 0.1 * jax.random.normal(keys[3], (MODEL_WIDTH,), jnp.float32), 0.5, 1.5).astype(jnp.bfloat16),
        "w_query": gaussian(keys[4], (MODEL_WIDTH, QUERY_HEADS * HEAD_WIDTH), (MODEL_WIDTH // 12) ** -0.5, 0.4375, ((1, 4),)),
        "key_weight": gaussian(keys[5], (MODEL_WIDTH, KEY_VALUE_HEADS * HEAD_WIDTH), (MODEL_WIDTH // 12) ** -0.5, 0.4375, ((1, 4),)),
        "value_weight": gaussian(keys[6], (MODEL_WIDTH, KEY_VALUE_HEADS * HEAD_WIDTH), MODEL_WIDTH ** -0.5, 0.125, ((1, 4),)),
        "w_out": gaussian(keys[7], (QUERY_HEADS * HEAD_WIDTH, MODEL_WIDTH), 2 ** -0.5, 4.0, ((0, 4),)),
        "norm_mlp": jnp.clip(1.0 + 0.1 * jax.random.normal(keys[8], (MODEL_WIDTH,), jnp.float32), 0.5, 1.5).astype(jnp.bfloat16),
        "w_gate": gaussian(keys[9], (MODEL_WIDTH, FF), MODEL_WIDTH ** -0.5, 0.125, ((1, 4),)),
        "w_up": gaussian(keys[10], (MODEL_WIDTH, FF), MODEL_WIDTH ** -0.5, 0.125, ((1, 4),)),
        "w_down": gaussian(keys[11], (FF, MODEL_WIDTH), (FF // 64) ** -0.5, 0.5, ((0, 4),)),
        "prompt_cot": gaussian(keys[12], (GROUPS, PROMPT_LENGTH, MODEL_WIDTH), 1.0, 6.0, ((0, 4), (1, 2))),
        "cont_cot": gaussian(keys[13], (GROUPS, CONTINUATIONS, CONT_LENGTH, MODEL_WIDTH), 1.0, 6.0, ((0, 4), (1, 2))),
    }


norm_eps = 1e-05
rope_base = 10000000.0
score_scale = 0.015625
branch_scale = 0.22
masked_score = -1e+30
highest = lax.Precision.HIGHEST

@jax.custom_vjp
def low(v):
    return lax.optimization_barrier(v.astype(jnp.bfloat16)).astype(jnp.float32)

@jax.custom_vjp
def low_back(v):
    return v

def low_keep(v):
    return (low(v), None)

def low_pass(kept, grad):
    return (grad,)

def back_keep(v):
    return (v, None)

def back_low(kept, grad):
    return (low(grad),)
low.defvjp(low_keep, low_pass)
low_back.defvjp(back_keep, back_low)

def norm_rows(inputs, weight):
    return inputs * lax.rsqrt(lax.optimization_barrier(jnp.mean(inputs * inputs, axis=-1, keepdims=True)) + norm_eps) * weight

def angle_tables(position):
    freq = jnp.exp(jnp.arange(HEAD_WIDTH // 2, dtype=jnp.float32) * (-2.0 * math.log(rope_base) / HEAD_WIDTH))
    angle = position.astype(jnp.float32)[:, None] * freq[None, :]
    return (jnp.cos(angle), jnp.sin(angle))

def rotate(inputs, cos_table, sin_table):
    halves = inputs.reshape(inputs.shape[0], -1, 2, HEAD_WIDTH // 2)
    first_half = halves[:, :, 0]
    second_half = halves[:, :, 1]
    cos_rows = cos_table[:, None, :]
    sin_rows = sin_table[:, None, :]
    turned = jnp.stack([first_half * cos_rows - second_half * sin_rows, second_half * cos_rows + first_half * sin_rows], axis=2)
    return turned.reshape(inputs.shape)

def attend(query_rows, joined_keys, joined_values, allowed):
    query_total = query_rows.shape[0]
    key_total = joined_keys.shape[0]
    query_head_rows = query_rows.reshape(query_total, KEY_VALUE_HEADS, QUERY_HEADS // KEY_VALUE_HEADS, HEAD_WIDTH)
    key_head_rows = joined_keys.reshape(key_total, KEY_VALUE_HEADS, HEAD_WIDTH)
    value_head_rows = joined_values.reshape(key_total, KEY_VALUE_HEADS, HEAD_WIDTH)
    scores = low_back(jnp.einsum('bhgd,khd->hgbk', query_head_rows, key_head_rows, precision=highest) * score_scale)
    scores = jnp.where(allowed[None, None], scores, masked_score)
    weights = jax.nn.softmax(scores, axis=-1)
    mixed_heads = jnp.einsum('hgbk,khd->bhgd', low(weights), value_head_rows, precision=highest)
    return mixed_heads.reshape(query_total, QUERY_HEADS * HEAD_WIDTH)

def prompt_block(query_rows, joined_keys, joined_values, token_length, first_row):
    block_rows = min(512, PROMPT_LENGTH)
    query_place = first_row + jnp.arange(block_rows, dtype=jnp.int32)
    key_place = jnp.arange(PROMPT_LENGTH, dtype=jnp.int32)
    allowed = (key_place[None, :] <= query_place[:, None]) & (key_place[None, :] < token_length)
    picked = lax.dynamic_slice_in_dim(query_rows, first_row, block_rows, 0)
    return attend(picked, joined_keys, joined_values, allowed)

def cont_block(shared_prompt_keys, shared_prompt_values, token_length, query_rows, keys_own, values_own):
    key_valid = jnp.arange(PROMPT_LENGTH, dtype=jnp.int32) < token_length
    causal = jnp.arange(CONT_LENGTH, dtype=jnp.int32)[None, :] <= jnp.arange(CONT_LENGTH, dtype=jnp.int32)[:, None]
    allowed = jnp.concatenate([jnp.broadcast_to(key_valid[None, :], (CONT_LENGTH, PROMPT_LENGTH)), causal], axis=1)
    return attend(query_rows, jnp.concatenate([shared_prompt_keys, keys_own], axis=0), jnp.concatenate([shared_prompt_values, values_own], axis=0), allowed)

def layer_forward(params, prompt_x, cont_x, token_length):
    norm_attn, w_query, key_weight, value_weight, w_out, norm_mlp, w_gate, w_up, w_down = params
    inputs = jnp.concatenate([prompt_x, cont_x.reshape(CONTINUATIONS * CONT_LENGTH, MODEL_WIDTH)], axis=0)
    within = jnp.arange(CONTINUATIONS * CONT_LENGTH, dtype=jnp.int32) % CONT_LENGTH
    positions = jnp.concatenate([jnp.arange(PROMPT_LENGTH, dtype=jnp.int32), token_length + within])
    cos_table, sin_table = angle_tables(positions)
    act_a = low(norm_rows(inputs, norm_attn))
    query_rows = low(rotate(low_back(jnp.dot(act_a, w_query, precision=highest)), cos_table, sin_table))
    joined_keys = low(rotate(low_back(jnp.dot(act_a, key_weight, precision=highest)), cos_table, sin_table))
    joined_values = low(low_back(jnp.dot(act_a, value_weight, precision=highest)))
    prompt_queries = query_rows[:PROMPT_LENGTH]
    shared_prompt_keys = joined_keys[:PROMPT_LENGTH]
    shared_prompt_values = joined_values[:PROMPT_LENGTH]
    block_rows = min(512, PROMPT_LENGTH)
    prompt_step = jax.checkpoint(prompt_block)
    prompt_mixed = lax.map(lambda first_row: prompt_step(prompt_queries, shared_prompt_keys, shared_prompt_values, token_length, first_row), jnp.arange(PROMPT_LENGTH // block_rows, dtype=jnp.int32) * block_rows)
    prompt_mixed = prompt_mixed.reshape(PROMPT_LENGTH, QUERY_HEADS * HEAD_WIDTH)
    continuation_step = jax.checkpoint(cont_block)
    continuation_mixed = lax.map(lambda three_tuple: continuation_step(shared_prompt_keys, shared_prompt_values, token_length, three_tuple[0], three_tuple[1], three_tuple[2]), (query_rows[PROMPT_LENGTH:].reshape(CONTINUATIONS, CONT_LENGTH, QUERY_HEADS * HEAD_WIDTH), joined_keys[PROMPT_LENGTH:].reshape(CONTINUATIONS, CONT_LENGTH, KEY_VALUE_HEADS * HEAD_WIDTH), joined_values[PROMPT_LENGTH:].reshape(CONTINUATIONS, CONT_LENGTH, KEY_VALUE_HEADS * HEAD_WIDTH)))
    mixed_heads = low(low_back(jnp.concatenate([prompt_mixed, continuation_mixed.reshape(CONTINUATIONS * CONT_LENGTH, QUERY_HEADS * HEAD_WIDTH)], axis=0)))
    attn_out = low_back(jnp.dot(mixed_heads, w_out, precision=highest))
    hidden_res = inputs + branch_scale * attn_out
    act_b = low(norm_rows(hidden_res, norm_mlp))
    gate_proj = low_back(jnp.dot(act_b, w_gate, precision=highest))
    up_proj = low_back(jnp.dot(act_b, w_up, precision=highest))
    hidden_act = low(jax.nn.silu(gate_proj) * up_proj)
    mlp_out = low_back(jnp.dot(hidden_act, w_down, precision=highest))
    result = hidden_res + branch_scale * mlp_out
    return (result[:PROMPT_LENGTH], result[PROMPT_LENGTH:].reshape(CONTINUATIONS, CONT_LENGTH, MODEL_WIDTH))

def reference(prompt_in, cont_in, prompt_len, norm_attn, w_query, key_weight, value_weight, w_out, norm_mlp, w_gate, w_up, w_down, prompt_cot, cont_cot):
    params = tuple((weight.astype(jnp.float32) for weight in (norm_attn, w_query, key_weight, value_weight, w_out, norm_mlp, w_gate, w_up, w_down)))

    def one_group(totals, group_data):
        prompt_x, cont_x, prompt_dy, cont_dy, token_length = group_data

        def forward(weights, prompt_part, cont_part):
            return layer_forward(weights, prompt_part, cont_part, token_length)
        outputs, pullback = jax.vjp(forward, params, prompt_x.astype(jnp.float32), cont_x.astype(jnp.float32))
        grad_tuple, prompt_dx, cont_dx = pullback((prompt_dy.astype(jnp.float32), cont_dy.astype(jnp.float32)))
        totals = jax.tree.map(lambda first_term, second_term: first_term + second_term, totals, grad_tuple)
        return (totals, (outputs[0].astype(jnp.bfloat16), outputs[1].astype(jnp.bfloat16), prompt_dx.astype(jnp.bfloat16), cont_dx.astype(jnp.bfloat16)))
    zero_grads = jax.tree.map(jnp.zeros_like, params)
    totals, produced = lax.scan(one_group, zero_grads, (prompt_in, cont_in, prompt_cot, cont_cot, prompt_len))
    return (produced[0], produced[1], produced[2], produced[3], totals[0], totals[1], totals[2], totals[3], totals[4], totals[5], totals[6], totals[7], totals[8])
```

```python
import math

import jax
import jax.numpy as jnp
from jax import lax
from jax.sharding import PartitionSpec as P

QUERY_HEADS = 32
KEY_VALUE_HEADS = 8
HEAD_WIDTH = 64
CONT_LENGTH = 128


norm_eps = 1e-05
rope_base = 10000000.0
score_scale = 0.015625
branch_scale = 0.22
masked_score = -1e30


def norm_rows(inputs, weight):
    return inputs * lax.rsqrt(jnp.mean(inputs * inputs, axis=-1, keepdims=True) + norm_eps) * weight


def norm_back(inputs, weight, upstream):
    factor = lax.rsqrt(jnp.mean(inputs * inputs, axis=-1, keepdims=True) + norm_eps)
    scaled = inputs * factor
    weighted = upstream * weight
    through = factor * (weighted - scaled * jnp.mean(weighted * scaled, axis=-1, keepdims=True))
    return (through, jnp.sum(upstream * scaled, axis=0))


def angle_tables(position):
    freq = jnp.exp(
        jnp.arange(HEAD_WIDTH // 2, dtype=jnp.float32) * (-2.0 * math.log(rope_base) / HEAD_WIDTH)
    )
    angle = position.astype(jnp.float32)[:, None] * freq[None, :]
    return (jnp.cos(angle), jnp.sin(angle))


def rotate(inputs, cos_table, sin_table):
    halves = inputs.reshape(inputs.shape[0], -1, 2, HEAD_WIDTH // 2)
    first_half = halves[:, :, 0]
    second_half = halves[:, :, 1]
    cos_rows = cos_table[:, None, :]
    sin_rows = sin_table[:, None, :]
    turned = jnp.stack(
        [
            first_half * cos_rows - second_half * sin_rows,
            second_half * cos_rows + first_half * sin_rows,
        ],
        axis=2,
    )
    return turned.reshape(inputs.shape)


def score_block(query_rows, joined_keys, allowed):
    query_total = query_rows.shape[0]
    key_total = joined_keys.shape[0]
    key_value_heads = joined_keys.shape[1] // HEAD_WIDTH
    query_head_rows = query_rows.reshape(
        query_total, key_value_heads, QUERY_HEADS // KEY_VALUE_HEADS, HEAD_WIDTH
    )
    key_head_rows = joined_keys.reshape(key_total, key_value_heads, HEAD_WIDTH)
    scores = (
        jnp.einsum(
            "bhgd,khd->hgbk", query_head_rows, key_head_rows, preferred_element_type=jnp.float32
        )
        * score_scale
    )
    return (jnp.where(allowed[None, None], scores, masked_score), query_head_rows, key_head_rows)


def attend_forward(query_rows, joined_keys, joined_values, allowed):
    scores, query_head_rows, key_head_rows = score_block(query_rows, joined_keys, allowed)
    highest_score = jnp.max(scores, axis=-1, keepdims=True)
    log_total = highest_score + jnp.log(
        jnp.sum(jnp.exp(scores - highest_score), axis=-1, keepdims=True)
    )
    weights = jnp.exp(scores - log_total).astype(jnp.bfloat16)
    value_head_rows = joined_values.reshape(key_head_rows.shape)
    mixed_heads = jnp.einsum(
        "hgbk,khd->bhgd", weights, value_head_rows, preferred_element_type=jnp.float32
    )
    return (mixed_heads.reshape(query_rows.shape[0], -1), log_total)


def attend_backward(query_rows, joined_keys, joined_values, allowed, log_total, upstream):
    scores, query_head_rows, key_head_rows = score_block(query_rows, joined_keys, allowed)
    weights = jnp.exp(scores - log_total)
    value_head_rows = joined_values.reshape(key_head_rows.shape)
    grad_heads = upstream.reshape(query_head_rows.shape)
    grad_weights = jnp.einsum(
        "bhgd,khd->hgbk", grad_heads, value_head_rows, preferred_element_type=jnp.float32
    )
    grad_scores = (
        weights * (grad_weights - jnp.sum(grad_weights * weights, axis=-1, keepdims=True))
    ).astype(jnp.bfloat16)
    grad_query = (
        jnp.einsum("hgbk,khd->bhgd", grad_scores, key_head_rows, preferred_element_type=jnp.float32)
        * score_scale
    )
    grad_key = (
        jnp.einsum(
            "hgbk,bhgd->khd", grad_scores, query_head_rows, preferred_element_type=jnp.float32
        )
        * score_scale
    )
    grad_value = jnp.einsum(
        "hgbk,bhgd->khd",
        weights.astype(jnp.bfloat16),
        grad_heads,
        preferred_element_type=jnp.float32,
    )
    return (
        grad_query.reshape(query_rows.shape[0], -1),
        grad_key.reshape(joined_keys.shape[0], -1),
        grad_value.reshape(joined_keys.shape[0], -1),
    )


def sum_share(values):
    return lax.psum_scatter(
        values.astype(jnp.bfloat16), "tensor", scatter_dimension=0, tiled=True
    ).astype(jnp.float32)


def shards(
    prompt_in,
    cont_in,
    prompt_len,
    norm_attn,
    w_query,
    key_weight,
    value_weight,
    w_out,
    norm_mlp,
    w_gate,
    w_up,
    w_down,
    prompt_cot,
    cont_cot,
):
    own_rows = prompt_in.shape[1]
    cont_count = cont_in.shape[1]
    width = prompt_in.shape[2]
    cont_rows = cont_count * CONT_LENGTH
    total_rows = own_rows + cont_rows
    key_width = key_weight.shape[1]
    ctx_index = lax.axis_index("ctx")
    share_rows = total_rows // lax.axis_size("tensor")
    share_start = lax.axis_index("tensor") * share_rows
    token_length = prompt_len[0]
    gain_attn = norm_attn.astype(jnp.float32)
    gain_mlp = norm_mlp.astype(jnp.float32)

    def share_of(values):
        return lax.dynamic_slice_in_dim(values, share_start, share_rows, 0)

    all_rows = jnp.concatenate([prompt_in[0], cont_in[0].reshape(cont_rows, width)], axis=0).astype(
        jnp.float32
    )
    input_share = share_of(all_rows)
    within = jnp.arange(cont_rows, dtype=jnp.int32) % CONT_LENGTH
    owner = jnp.arange(cont_rows, dtype=jnp.int32) // CONT_LENGTH
    positions = jnp.concatenate(
        [ctx_index * own_rows + jnp.arange(own_rows, dtype=jnp.int32), token_length + within]
    )
    cos_table, sin_table = angle_tables(positions)
    act_a = norm_rows(all_rows, gain_attn).astype(jnp.bfloat16)
    query_rows = rotate(
        jnp.dot(act_a, w_query, preferred_element_type=jnp.float32), cos_table, sin_table
    ).astype(jnp.bfloat16)
    joined_keys = rotate(
        jnp.dot(act_a, key_weight, preferred_element_type=jnp.float32), cos_table, sin_table
    ).astype(jnp.bfloat16)
    joined_values = jnp.dot(act_a, value_weight, preferred_element_type=jnp.float32).astype(
        jnp.bfloat16
    )
    local_pairs = jnp.concatenate([joined_keys[:own_rows], joined_values[:own_rows]], axis=1)
    prompt_pairs = lax.all_gather(local_pairs, "ctx", axis=0, tiled=True)
    prompt_total = prompt_pairs.shape[0]
    shared_prompt_keys = prompt_pairs[:, :key_width]
    shared_prompt_values = prompt_pairs[:, key_width:]
    key_place = jnp.arange(prompt_total, dtype=jnp.int32)
    key_valid = key_place < token_length
    block_rows = min(512, own_rows)
    block_index = 0
    query_place = (
        ctx_index * own_rows + block_index * block_rows + jnp.arange(block_rows, dtype=jnp.int32)
    )
    block_masks = [(key_place[None, :] <= query_place[:, None]) & key_valid[None, :]]
    cont_mask = jnp.concatenate(
        [
            jnp.broadcast_to(key_valid[None, :], (cont_rows, prompt_total)),
            (owner[:, None] == owner[None, :]) & (within[None, :] <= within[:, None]),
        ],
        axis=1,
    )
    cont_keys = jnp.concatenate([shared_prompt_keys, joined_keys[own_rows:]], axis=0)
    cont_values = jnp.concatenate([shared_prompt_values, joined_values[own_rows:]], axis=0)
    block_index = 0
    block_queries = query_rows[block_index * block_rows : (block_index + 1) * block_rows]
    mixed_block, total_block = attend_forward(
        block_queries, shared_prompt_keys, shared_prompt_values, block_masks[block_index]
    )
    mixed_list = [mixed_block]
    total_list = [total_block]
    mixed_cont, total_cont = attend_forward(
        query_rows[own_rows:], cont_keys, cont_values, cont_mask
    )
    mixed_heads = jnp.concatenate(mixed_list + [mixed_cont], axis=0).astype(jnp.bfloat16)
    attn_share = sum_share(jnp.dot(mixed_heads, w_out, preferred_element_type=jnp.float32))
    hidden_share = input_share + branch_scale * attn_share
    act_b_share = norm_rows(hidden_share, gain_mlp).astype(jnp.bfloat16)
    act_b = lax.all_gather(act_b_share, "tensor", axis=0, tiled=True)
    gate_proj = jnp.dot(act_b, w_gate, preferred_element_type=jnp.float32)
    up_proj = jnp.dot(act_b, w_up, preferred_element_type=jnp.float32)
    sigmoid_gate = jax.nn.sigmoid(gate_proj)
    silu_gate = gate_proj * sigmoid_gate
    hidden_act = (silu_gate * up_proj).astype(jnp.bfloat16)
    mlp_share = sum_share(jnp.dot(hidden_act, w_down, preferred_element_type=jnp.float32))
    result_share = (hidden_share + branch_scale * mlp_share).astype(jnp.bfloat16)
    result = lax.all_gather(result_share, "tensor", axis=0, tiled=True)
    prompt_out = result[:own_rows][None]
    cont_out = result[own_rows:].reshape(1, cont_count, CONT_LENGTH, width)
    upstream = jnp.concatenate(
        [prompt_cot[0], cont_cot[0].reshape(cont_rows, width)], axis=0
    ).astype(jnp.float32)
    grad_mlp = (branch_scale * upstream).astype(jnp.bfloat16)
    grad_down = jnp.einsum("rf,rd->df", hidden_act, grad_mlp, preferred_element_type=jnp.float32)
    grad_hidden = jnp.einsum("rd,fd->rf", grad_mlp, w_down, preferred_element_type=jnp.float32)
    grad_gate_act = (
        grad_hidden * up_proj * sigmoid_gate * (1.0 + gate_proj * (1.0 - sigmoid_gate))
    ).astype(jnp.bfloat16)
    grad_up_act = (grad_hidden * silu_gate).astype(jnp.bfloat16)
    grad_gate = jnp.einsum("rd,rf->df", act_b, grad_gate_act, preferred_element_type=jnp.float32)
    grad_up = jnp.einsum("rd,rf->df", act_b, grad_up_act, preferred_element_type=jnp.float32)
    normed_grad = jnp.einsum(
        "rf,df->rd", grad_gate_act, w_gate, preferred_element_type=jnp.float32
    ) + jnp.einsum("rf,df->rd", grad_up_act, w_up, preferred_element_type=jnp.float32)
    normed_share = sum_share(normed_grad)
    through_mlp, gain_mlp_part = norm_back(hidden_share, gain_mlp, normed_share)
    res_share = share_of(upstream) + through_mlp
    grad_attn = lax.all_gather(
        (branch_scale * res_share).astype(jnp.bfloat16), "tensor", axis=0, tiled=True
    )
    grad_out = jnp.einsum("rq,rd->dq", mixed_heads, grad_attn, preferred_element_type=jnp.float32)
    grad_mixed = jnp.einsum(
        "rd,qd->rq", grad_attn, w_out, preferred_element_type=jnp.float32
    ).astype(jnp.bfloat16)
    query_grads = []
    block_index = 0
    low_row = block_index * block_rows
    block_queries = query_rows[low_row : low_row + block_rows]
    block_grad = grad_mixed[low_row : low_row + block_rows]
    grad_query_block, grad_key_block, grad_value_block = attend_backward(
        block_queries,
        shared_prompt_keys,
        shared_prompt_values,
        block_masks[block_index],
        total_list[block_index],
        block_grad,
    )
    query_grads.append(grad_query_block)
    prompt_key_grad = grad_key_block
    prompt_value_grad = grad_value_block
    grad_query_cont, grad_key_cont, grad_value_cont = attend_backward(
        query_rows[own_rows:], cont_keys, cont_values, cont_mask, total_cont, grad_mixed[own_rows:]
    )
    query_grads.append(grad_query_cont)
    prompt_key_grad = prompt_key_grad + grad_key_cont[:prompt_total]
    prompt_value_grad = prompt_value_grad + grad_value_cont[:prompt_total]
    pair_grads = lax.psum_scatter(
        jnp.concatenate([prompt_key_grad, prompt_value_grad], axis=1),
        "ctx",
        scatter_dimension=0,
        tiled=True,
    )
    key_grad_rows = jnp.concatenate(
        [pair_grads[:, :key_width], grad_key_cont[prompt_total:]], axis=0
    )
    value_grad_rows = jnp.concatenate(
        [pair_grads[:, key_width:], grad_value_cont[prompt_total:]], axis=0
    )
    query_grad_rows = jnp.concatenate(query_grads, axis=0)
    grad_query_lin = rotate(query_grad_rows, cos_table, -sin_table).astype(jnp.bfloat16)
    grad_key_lin = rotate(key_grad_rows, cos_table, -sin_table).astype(jnp.bfloat16)
    grad_value_lin = value_grad_rows.astype(jnp.bfloat16)
    grad_query = jnp.einsum("rd,rq->dq", act_a, grad_query_lin, preferred_element_type=jnp.float32)
    grad_key = jnp.einsum("rd,rq->dq", act_a, grad_key_lin, preferred_element_type=jnp.float32)
    grad_value = jnp.einsum("rd,rq->dq", act_a, grad_value_lin, preferred_element_type=jnp.float32)
    input_grad = (
        jnp.einsum("rq,dq->rd", grad_query_lin, w_query, preferred_element_type=jnp.float32)
        + jnp.einsum("rq,dq->rd", grad_key_lin, key_weight, preferred_element_type=jnp.float32)
        + jnp.einsum("rq,dq->rd", grad_value_lin, value_weight, preferred_element_type=jnp.float32)
    )
    input_grad_share = sum_share(input_grad)
    through_attn, gain_attn_part = norm_back(input_share, gain_attn, input_grad_share)
    grad_input = lax.all_gather(
        (res_share + through_attn).astype(jnp.bfloat16), "tensor", axis=0, tiled=True
    )
    prompt_grad = grad_input[:own_rows][None]
    cont_grad = grad_input[own_rows:].reshape(1, cont_count, CONT_LENGTH, width)
    gain_parts = lax.psum(jnp.stack([gain_attn_part, gain_mlp_part]), ("dp", "ctx", "tensor"))
    gain_rows = width // (lax.axis_size("dp") * lax.axis_size("ctx"))
    gain_start = (lax.axis_index("dp") * lax.axis_size("ctx") + ctx_index) * gain_rows
    gain_own = lax.dynamic_slice_in_dim(gain_parts, gain_start, gain_rows, 1)
    mlp_sum = lax.psum_scatter(
        jnp.concatenate([grad_gate, grad_up, grad_down], axis=1).astype(jnp.bfloat16),
        ("dp", "ctx"),
        scatter_dimension=0,
        tiled=True,
    ).astype(jnp.float32)
    attn_sum = lax.psum_scatter(
        jnp.concatenate([grad_query, grad_key, grad_value, grad_out], axis=1).astype(jnp.bfloat16),
        ("dp", "ctx"),
        scatter_dimension=0,
        tiled=True,
    ).astype(jnp.float32)
    ff = grad_gate.shape[1]
    qw = grad_query.shape[1]
    summed = (
        gain_own[0],
        attn_sum[:, :qw],
        attn_sum[:, qw : qw + key_width],
        attn_sum[:, qw + key_width : qw + 2 * key_width],
        attn_sum[:, qw + 2 * key_width :].T,
        gain_own[1],
        mlp_sum[:, :ff],
        mlp_sum[:, ff : 2 * ff],
        mlp_sum[:, 2 * ff :].T,
    )
    return (
        prompt_out,
        cont_out,
        prompt_grad,
        cont_grad,
        summed[0],
        summed[1],
        summed[2],
        summed[3],
        summed[4],
        summed[5],
        summed[6],
        summed[7],
        summed[8],
    )


def solution(mesh):
    in_specs = (
        P("dp", "ctx", None),
        P("dp", "ctx", None, None),
        P("dp"),
        P(),
        P(None, "tensor"),
        P(None, "tensor"),
        P(None, "tensor"),
        P("tensor", None),
        P(),
        P(None, "tensor"),
        P(None, "tensor"),
        P("tensor", None),
        P("dp", "ctx", None),
        P("dp", "ctx", None, None),
    )
    out_specs = (
        P("dp", "ctx", None),
        P("dp", "ctx", None, None),
        P("dp", "ctx", None),
        P("dp", "ctx", None, None),
        P(("dp", "ctx")),
        P(("dp", "ctx"), "tensor"),
        P(("dp", "ctx"), "tensor"),
        P(("dp", "ctx"), "tensor"),
        P("tensor", ("dp", "ctx")),
        P(("dp", "ctx")),
        P(("dp", "ctx"), "tensor"),
        P(("dp", "ctx"), "tensor"),
        P("tensor", ("dp", "ctx")),
    )
    return jax.shard_map(shards, mesh=mesh, in_specs=in_specs, out_specs=out_specs, check_vma=False)
```

```python
import functools
import math
import operator

import jax
import jax.numpy as jnp
from jax import lax
from jax.sharding import PartitionSpec as P

QUERY_HEADS = 32
KEY_VALUE_HEADS = 8
HEAD_WIDTH = 64
CONT_LENGTH = 128


norm_eps = 1e-05
rope_base = 10000000.0
score_scale = 0.015625
branch_scale = 0.22
masked_score = -1e30


def norm_rows(inputs, weight):
    return inputs * lax.rsqrt(jnp.mean(inputs * inputs, axis=-1, keepdims=True) + norm_eps) * weight


def norm_back(inputs, weight, upstream):
    factor = lax.rsqrt(jnp.mean(inputs * inputs, axis=-1, keepdims=True) + norm_eps)
    scaled = inputs * factor
    weighted = upstream * weight
    through = factor * (weighted - scaled * jnp.mean(weighted * scaled, axis=-1, keepdims=True))
    return (through, jnp.sum(upstream * scaled, axis=0))


def angle_tables(position):
    freq = jnp.exp(
        jnp.arange(HEAD_WIDTH // 2, dtype=jnp.float32) * (-2.0 * math.log(rope_base) / HEAD_WIDTH)
    )
    angle = position.astype(jnp.float32)[:, None] * freq[None, :]
    return (jnp.cos(angle), jnp.sin(angle))


def rotate(inputs, cos_table, sin_table):
    halves = inputs.reshape(inputs.shape[0], -1, 2, HEAD_WIDTH // 2)
    first_half = halves[:, :, 0]
    second_half = halves[:, :, 1]
    cos_rows = cos_table[:, None, :]
    sin_rows = sin_table[:, None, :]
    turned = jnp.stack(
        [
            first_half * cos_rows - second_half * sin_rows,
            second_half * cos_rows + first_half * sin_rows,
        ],
        axis=2,
    )
    return turned.reshape(inputs.shape)


def score_block(query_rows, joined_keys, allowed):
    query_total = query_rows.shape[0]
    key_total = joined_keys.shape[0]
    key_value_heads = joined_keys.shape[1] // HEAD_WIDTH
    query_head_rows = query_rows.reshape(
        query_total, key_value_heads, QUERY_HEADS // KEY_VALUE_HEADS, HEAD_WIDTH
    )
    key_head_rows = joined_keys.reshape(key_total, key_value_heads, HEAD_WIDTH)
    scores = (
        jnp.einsum(
            "bhgd,khd->hgbk", query_head_rows, key_head_rows, preferred_element_type=jnp.float32
        )
        * score_scale
    )
    return (jnp.where(allowed[None, None], scores, masked_score), query_head_rows, key_head_rows)


def attend_forward(query_rows, joined_keys, joined_values, allowed):
    scores, query_head_rows, key_head_rows = score_block(query_rows, joined_keys, allowed)
    highest_score = jnp.max(scores, axis=-1, keepdims=True)
    log_total = highest_score + jnp.log(
        jnp.sum(jnp.exp(scores - highest_score), axis=-1, keepdims=True)
    )
    weights = jnp.exp(scores - log_total).astype(jnp.bfloat16)
    value_head_rows = joined_values.reshape(key_head_rows.shape)
    mixed_heads = jnp.einsum(
        "hgbk,khd->bhgd", weights, value_head_rows, preferred_element_type=jnp.float32
    )
    return (mixed_heads.reshape(query_rows.shape[0], -1), log_total)


def attend_backward(query_rows, joined_keys, joined_values, allowed, log_total, upstream):
    scores, query_head_rows, key_head_rows = score_block(query_rows, joined_keys, allowed)
    weights = jnp.exp(scores - log_total)
    value_head_rows = joined_values.reshape(key_head_rows.shape)
    grad_heads = upstream.reshape(query_head_rows.shape)
    grad_weights = jnp.einsum(
        "bhgd,khd->hgbk", grad_heads, value_head_rows, preferred_element_type=jnp.float32
    )
    grad_scores = (
        weights * (grad_weights - jnp.sum(grad_weights * weights, axis=-1, keepdims=True))
    ).astype(jnp.bfloat16)
    grad_query = (
        jnp.einsum("hgbk,khd->bhgd", grad_scores, key_head_rows, preferred_element_type=jnp.float32)
        * score_scale
    )
    grad_key = (
        jnp.einsum(
            "hgbk,bhgd->khd", grad_scores, query_head_rows, preferred_element_type=jnp.float32
        )
        * score_scale
    )
    grad_value = jnp.einsum(
        "hgbk,bhgd->khd",
        weights.astype(jnp.bfloat16),
        grad_heads,
        preferred_element_type=jnp.float32,
    )
    return (
        grad_query.reshape(query_rows.shape[0], -1),
        grad_key.reshape(joined_keys.shape[0], -1),
        grad_value.reshape(joined_keys.shape[0], -1),
    )


def picked(me, arrays, keys):
    out = None
    for key in dict.fromkeys(keys.values()):
        if out is None:
            out = arrays[key]
        else:
            chosen = functools.reduce(
                operator.or_, [me == device for device, held in keys.items() if held == key]
            )
            out = jnp.where(chosen, arrays[key], out)
    return out


def slot_tables(count):
    chunk_of = []
    for device in range(count):
        near = min(device, count - 1 - device)
        far = 1 if device < count - 1 - device else -1
        order = [device]
        for slot in range(1, count):
            if slot <= 2 * near:
                distance = (slot + 1) // 2
                order.append(device - distance if slot % 2 else device + distance)
            else:
                order.append(device + far * (slot - near))
        chunk_of.append(order)
    return chunk_of


def line_hops(share, count):
    arrived = {0: share}
    forward = backward = share
    for step in range(1, count):
        forward = lax.ppermute(forward, "tensor", [(i, i + 1) for i in range(step - 1, count - 1)])
        backward = lax.ppermute(backward, "tensor", [(i, i - 1) for i in range(1, count - step + 1)])
        arrived[-step] = forward
        arrived[step] = backward
    return arrived


def line_sum(part_at, count):
    from_left = from_right = None
    for distance in range(count - 1, 0, -1):
        to_right = part_at(distance)
        to_left = part_at(-distance)
        if from_left is not None:
            to_right = (to_right.astype(jnp.float32) + from_left.astype(jnp.float32)).astype(
                jnp.bfloat16
            )
            to_left = (to_left.astype(jnp.float32) + from_right.astype(jnp.float32)).astype(
                jnp.bfloat16
            )
        from_left = lax.ppermute(
            to_right, "tensor", [(i, i + 1) for i in range(0, count - distance)]
        )
        from_right = lax.ppermute(to_left, "tensor", [(i, i - 1) for i in range(distance, count)])
    return (
        part_at(0).astype(jnp.float32)
        + from_left.astype(jnp.float32)
        + from_right.astype(jnp.float32)
    )


def shards(
    prompt_in,
    cont_in,
    prompt_len,
    norm_attn,
    w_query,
    key_weight,
    value_weight,
    w_out,
    norm_mlp,
    w_gate,
    w_up,
    w_down,
    prompt_cot,
    cont_cot,
):
    own_rows = prompt_in.shape[1]
    cont_count = cont_in.shape[1]
    width = prompt_in.shape[2]
    cont_rows = cont_count * CONT_LENGTH
    total_rows = own_rows + cont_rows
    key_width = key_weight.shape[1]
    ctx_index = lax.axis_index("ctx")
    count = lax.axis_size("tensor")
    me = lax.axis_index("tensor")
    share_rows = total_rows // count
    share_start = me * share_rows
    head_half = w_out.shape[0] // 2
    order = slot_tables(count)
    slot_chunks = [
        picked(me, {i: jnp.int32(i) for i in range(count)}, {i: order[i][s] for i in range(count)})
        for s in range(count)
    ]
    slot_of = [[order[i].index(c) for c in range(count)] for i in range(count)]
    token_length = prompt_len[0]
    gain_attn = norm_attn.astype(jnp.float32)
    gain_mlp = norm_mlp.astype(jnp.float32)

    def share_of(values):
        return lax.dynamic_slice_in_dim(values, share_start, share_rows, 0)

    def slot_order(values):
        return jnp.concatenate(
            [
                lax.dynamic_slice_in_dim(values, slot_chunks[s] * share_rows, share_rows, 0)
                for s in range(count)
            ],
            axis=0,
        )

    def slots_from(share):
        arrived = line_hops(share, count)
        return [
            picked(me, arrived, {i: order[i][s] - i for i in range(count)}) for s in range(count)
        ]

    own_out_half = lax.dynamic_slice_in_dim(w_out, ctx_index * head_half, head_half, 0)
    half_out = lax.all_gather(own_out_half, "tensor", axis=0, tiled=True)
    full_out = lax.all_gather(half_out, "ctx", axis=0, tiled=True)
    all_rows = jnp.concatenate([prompt_in[0], cont_in[0].reshape(cont_rows, width)], axis=0).astype(
        jnp.float32
    )
    input_share = share_of(all_rows)
    within = jnp.arange(cont_rows, dtype=jnp.int32) % CONT_LENGTH
    owner = jnp.arange(cont_rows, dtype=jnp.int32) // CONT_LENGTH
    positions = jnp.concatenate(
        [ctx_index * own_rows + jnp.arange(own_rows, dtype=jnp.int32), token_length + within]
    )
    cos_table, sin_table = angle_tables(positions)
    act_a = norm_rows(all_rows, gain_attn).astype(jnp.bfloat16)
    query_rows = rotate(
        jnp.dot(act_a, w_query, preferred_element_type=jnp.float32), cos_table, sin_table
    ).astype(jnp.bfloat16)
    joined_keys = rotate(
        jnp.dot(act_a, key_weight, preferred_element_type=jnp.float32), cos_table, sin_table
    ).astype(jnp.bfloat16)
    joined_values = jnp.dot(act_a, value_weight, preferred_element_type=jnp.float32).astype(
        jnp.bfloat16
    )
    local_pairs = jnp.concatenate([joined_keys[:own_rows], joined_values[:own_rows]], axis=1)
    prompt_pairs = lax.all_gather(local_pairs, "ctx", axis=0, tiled=True)
    prompt_total = prompt_pairs.shape[0]
    shared_prompt_keys = prompt_pairs[:, :key_width]
    shared_prompt_values = prompt_pairs[:, key_width:]
    key_place = jnp.arange(prompt_total, dtype=jnp.int32)
    key_valid = key_place < token_length
    block_rows = min(512, own_rows)
    block_index = 0
    query_place = (
        ctx_index * own_rows + block_index * block_rows + jnp.arange(block_rows, dtype=jnp.int32)
    )
    block_masks = [(key_place[None, :] <= query_place[:, None]) & key_valid[None, :]]
    cont_mask = jnp.concatenate(
        [
            jnp.broadcast_to(key_valid[None, :], (cont_rows, prompt_total)),
            (owner[:, None] == owner[None, :]) & (within[None, :] <= within[:, None]),
        ],
        axis=1,
    )
    cont_keys = jnp.concatenate([shared_prompt_keys, joined_keys[own_rows:]], axis=0)
    cont_values = jnp.concatenate([shared_prompt_values, joined_values[own_rows:]], axis=0)
    block_index = 0
    block_queries = query_rows[block_index * block_rows : (block_index + 1) * block_rows]
    mixed_block, total_block = attend_forward(
        block_queries, shared_prompt_keys, shared_prompt_values, block_masks[block_index]
    )
    mixed_list = [mixed_block]
    total_list = [total_block]
    mixed_cont, total_cont = attend_forward(
        query_rows[own_rows:], cont_keys, cont_values, cont_mask
    )
    mixed_heads = jnp.concatenate(mixed_list + [mixed_cont], axis=0).astype(jnp.bfloat16)
    mixed_share = jnp.concatenate(
        [
            lax.all_to_all(
                mixed_heads[:, h * head_half : (h + 1) * head_half],
                "tensor",
                split_axis=0,
                concat_axis=1,
                tiled=True,
            )
            for h in range(2)
        ],
        axis=1,
    )
    attn_share = jnp.dot(mixed_share, full_out, preferred_element_type=jnp.float32)
    hidden_share = input_share + branch_scale * attn_share
    act_b_share = norm_rows(hidden_share, gain_mlp).astype(jnp.bfloat16)
    upstream = jnp.concatenate([prompt_cot[0], cont_cot[0].reshape(cont_rows, width)], axis=0)
    grad_mlp = slot_order((branch_scale * upstream.astype(jnp.float32)).astype(jnp.bfloat16))
    grad_hidden = jnp.einsum("rd,fd->rf", grad_mlp, w_down, preferred_element_type=jnp.float32)
    act_b_slots = slots_from(act_b_share)
    hidden_list, gate_list, up_list, part_list = ([], [], [], [])
    for s in range(count):
        gate_proj = jnp.dot(act_b_slots[s], w_gate, preferred_element_type=jnp.float32)
        up_proj = jnp.dot(act_b_slots[s], w_up, preferred_element_type=jnp.float32)
        sigmoid_gate = jax.nn.sigmoid(gate_proj)
        silu_gate = gate_proj * sigmoid_gate
        grad_slot = grad_hidden[s * share_rows : (s + 1) * share_rows]
        hidden_list.append((silu_gate * up_proj).astype(jnp.bfloat16))
        gate_list.append(
            (grad_slot * up_proj * sigmoid_gate * (1.0 + gate_proj * (1.0 - sigmoid_gate))).astype(
                jnp.bfloat16
            )
        )
        up_list.append((grad_slot * silu_gate).astype(jnp.bfloat16))
        part_list.append(
            (
                jnp.einsum("rf,df->rd", gate_list[s], w_gate, preferred_element_type=jnp.float32)
                + jnp.einsum("rf,df->rd", up_list[s], w_up, preferred_element_type=jnp.float32)
            ).astype(jnp.bfloat16)
        )

    def slot_part(distance):
        return picked(
            me,
            part_list,
            {
                i: slot_of[i][i + distance]
                for i in range(count)
                if 0 <= i + distance < count
            },
        )

    normed_share = line_sum(slot_part, count)
    through_mlp, gain_mlp_part = norm_back(hidden_share, gain_mlp, normed_share)
    res_share = share_of(upstream).astype(jnp.float32) + through_mlp
    grad_attn_share = (branch_scale * res_share).astype(jnp.bfloat16)
    mixed_grad = jnp.einsum(
        "rd,qd->rq", grad_attn_share, full_out, preferred_element_type=jnp.float32
    ).astype(jnp.bfloat16)
    grad_mixed = jnp.concatenate(
        [
            lax.all_to_all(
                mixed_grad[:, h * count * head_half : (h + 1) * count * head_half],
                "tensor",
                split_axis=1,
                concat_axis=0,
                tiled=True,
            )
            for h in range(2)
        ],
        axis=1,
    )
    act_b = jnp.concatenate(act_b_slots, axis=0)
    hidden_act = jnp.concatenate(hidden_list, axis=0)
    grad_gate_act = jnp.concatenate(gate_list, axis=0)
    grad_up_act = jnp.concatenate(up_list, axis=0)
    grad_down = jnp.einsum("rf,rd->df", hidden_act, grad_mlp, preferred_element_type=jnp.float32)
    grad_gate = jnp.einsum("rd,rf->df", act_b, grad_gate_act, preferred_element_type=jnp.float32)
    grad_up = jnp.einsum("rd,rf->df", act_b, grad_up_act, preferred_element_type=jnp.float32)
    mlp_sum = lax.psum_scatter(
        jnp.concatenate([grad_gate, grad_up, grad_down], axis=1).astype(jnp.bfloat16),
        ("dp", "ctx"),
        scatter_dimension=0,
        tiled=True,
    )
    mlp_part = jnp.dot(hidden_act, w_down, preferred_element_type=jnp.float32).astype(jnp.bfloat16)
    mlp_part, mlp_sum = lax.optimization_barrier((mlp_part, mlp_sum))
    mlp_natural = jnp.concatenate(
        [
            lax.dynamic_slice_in_dim(
                mlp_part,
                picked(
                    me,
                    {s: jnp.int32(s * share_rows) for s in range(count)},
                    {i: slot_of[i][c] for i in range(count)},
                ),
                share_rows,
                0,
            )
            for c in range(count)
        ],
        axis=0,
    )
    mlp_share = lax.psum_scatter(
        mlp_natural, "tensor", scatter_dimension=0, tiled=True
    ).astype(jnp.float32)
    result_share = (hidden_share + branch_scale * mlp_share).astype(jnp.bfloat16)
    result = lax.all_gather(result_share, "tensor", axis=0, tiled=True)
    prompt_out = result[:own_rows][None]
    cont_out = result[own_rows:].reshape(1, cont_count, CONT_LENGTH, width)
    grad_attn = jnp.concatenate(slots_from(grad_attn_share), axis=0)
    grad_out = jnp.einsum(
        "rq,rd->dq", slot_order(mixed_heads), grad_attn, preferred_element_type=jnp.float32
    )
    query_grads = []
    block_index = 0
    low_row = block_index * block_rows
    block_queries = query_rows[low_row : low_row + block_rows]
    block_grad = grad_mixed[low_row : low_row + block_rows]
    grad_query_block, grad_key_block, grad_value_block = attend_backward(
        block_queries,
        shared_prompt_keys,
        shared_prompt_values,
        block_masks[block_index],
        total_list[block_index],
        block_grad,
    )
    query_grads.append(grad_query_block)
    prompt_key_grad = grad_key_block
    prompt_value_grad = grad_value_block
    grad_query_cont, grad_key_cont, grad_value_cont = attend_backward(
        query_rows[own_rows:], cont_keys, cont_values, cont_mask, total_cont, grad_mixed[own_rows:]
    )
    query_grads.append(grad_query_cont)
    prompt_key_grad = prompt_key_grad + grad_key_cont[:prompt_total]
    prompt_value_grad = prompt_value_grad + grad_value_cont[:prompt_total]
    pair_grads = lax.psum_scatter(
        jnp.concatenate([prompt_key_grad, prompt_value_grad], axis=1),
        "ctx",
        scatter_dimension=0,
        tiled=True,
    )
    key_grad_rows = jnp.concatenate(
        [pair_grads[:, :key_width], grad_key_cont[prompt_total:]], axis=0
    )
    value_grad_rows = jnp.concatenate(
        [pair_grads[:, key_width:], grad_value_cont[prompt_total:]], axis=0
    )
    query_grad_rows = jnp.concatenate(query_grads, axis=0)
    grad_query_lin = rotate(query_grad_rows, cos_table, -sin_table).astype(jnp.bfloat16)
    grad_key_lin = rotate(key_grad_rows, cos_table, -sin_table).astype(jnp.bfloat16)
    grad_value_lin = value_grad_rows.astype(jnp.bfloat16)
    grad_query = jnp.einsum("rd,rq->dq", act_a, grad_query_lin, preferred_element_type=jnp.float32)
    grad_key = jnp.einsum("rd,rq->dq", act_a, grad_key_lin, preferred_element_type=jnp.float32)
    grad_value = jnp.einsum("rd,rq->dq", act_a, grad_value_lin, preferred_element_type=jnp.float32)
    input_grad = (
        jnp.einsum("rq,dq->rd", grad_query_lin, w_query, preferred_element_type=jnp.float32)
        + jnp.einsum("rq,dq->rd", grad_key_lin, key_weight, preferred_element_type=jnp.float32)
        + jnp.einsum("rq,dq->rd", grad_value_lin, value_weight, preferred_element_type=jnp.float32)
    )
    input_part = input_grad.astype(jnp.bfloat16)

    def row_part(distance):
        place = jnp.clip(me + distance, 0, count - 1) * share_rows
        return lax.dynamic_slice_in_dim(input_part, place, share_rows, 0)

    input_grad_share = line_sum(row_part, count)
    through_attn, gain_attn_part = norm_back(input_share, gain_attn, input_grad_share)
    arrived = line_hops((res_share + through_attn).astype(jnp.bfloat16), count)
    grad_chunks = [
        picked(me, arrived, {i: c - i for i in range(count)}) for c in range(count)
    ]
    grad_input = jnp.concatenate(grad_chunks, axis=0)
    prompt_grad = grad_input[:own_rows][None]
    cont_grad = grad_input[own_rows:].reshape(1, cont_count, CONT_LENGTH, width)
    gain_own = lax.psum(
        lax.psum_scatter(
            jnp.stack([gain_attn_part, gain_mlp_part]),
            ("dp", "ctx"),
            scatter_dimension=1,
            tiled=True,
        ),
        "tensor",
    )
    mlp_sum = mlp_sum.astype(jnp.float32)
    attn_sum = lax.psum_scatter(
        jnp.concatenate([grad_query, grad_key, grad_value, grad_out], axis=1).astype(jnp.bfloat16),
        ("dp", "ctx"),
        scatter_dimension=0,
        tiled=True,
    ).astype(jnp.float32)
    ff = grad_gate.shape[1]
    qw = grad_query.shape[1]
    summed = (
        gain_own[0],
        attn_sum[:, :qw],
        attn_sum[:, qw : qw + key_width],
        attn_sum[:, qw + key_width : qw + 2 * key_width],
        attn_sum[:, qw + 2 * key_width :].T,
        gain_own[1],
        mlp_sum[:, :ff],
        mlp_sum[:, ff : 2 * ff],
        mlp_sum[:, 2 * ff :].T,
    )
    return (
        prompt_out,
        cont_out,
        prompt_grad,
        cont_grad,
        summed[0],
        summed[1],
        summed[2],
        summed[3],
        summed[4],
        summed[5],
        summed[6],
        summed[7],
        summed[8],
    )


def solution(mesh):
    in_specs = (
        P("dp", "ctx", None),
        P("dp", "ctx", None, None),
        P("dp"),
        P(),
        P(None, "tensor"),
        P(None, "tensor"),
        P(None, "tensor"),
        P("tensor", None),
        P(),
        P(None, "tensor"),
        P(None, "tensor"),
        P("tensor", None),
        P("dp", "ctx", None),
        P("dp", "ctx", None, None),
    )
    out_specs = (
        P("dp", "ctx", None),
        P("dp", "ctx", None, None),
        P("dp", "ctx", None),
        P("dp", "ctx", None, None),
        P(("dp", "ctx")),
        P(("dp", "ctx"), "tensor"),
        P(("dp", "ctx"), "tensor"),
        P(("dp", "ctx"), "tensor"),
        P("tensor", ("dp", "ctx")),
        P(("dp", "ctx")),
        P(("dp", "ctx"), "tensor"),
        P(("dp", "ctx"), "tensor"),
        P("tensor", ("dp", "ctx")),
    )
    return jax.shard_map(shards, mesh=mesh, in_specs=in_specs, out_specs=out_specs, check_vma=False)
```

```python
import functools
import math
import operator

import jax
import jax.numpy as jnp
from jax import lax
from jax.sharding import PartitionSpec as P

QUERY_HEADS = 32
KEY_VALUE_HEADS = 8
HEAD_WIDTH = 64
CONT_LENGTH = 128


norm_eps = 1e-05
rope_base = 10000000.0
score_scale = 0.015625
branch_scale = 0.22
masked_score = -1e30


def norm_rows(inputs, weight):
    return inputs * lax.rsqrt(jnp.mean(inputs * inputs, axis=-1, keepdims=True) + norm_eps) * weight


def norm_back(inputs, weight, upstream):
    factor = lax.rsqrt(jnp.mean(inputs * inputs, axis=-1, keepdims=True) + norm_eps)
    scaled = inputs * factor
    weighted = upstream * weight
    through = factor * (weighted - scaled * jnp.mean(weighted * scaled, axis=-1, keepdims=True))
    return (through, jnp.sum(upstream * scaled, axis=0))


def angle_tables(position):
    freq = jnp.exp(
        jnp.arange(HEAD_WIDTH // 2, dtype=jnp.float32) * (-2.0 * math.log(rope_base) / HEAD_WIDTH)
    )
    angle = position.astype(jnp.float32)[:, None] * freq[None, :]
    return (jnp.cos(angle), jnp.sin(angle))


def rotate(inputs, cos_table, sin_table):
    halves = inputs.reshape(inputs.shape[0], -1, 2, HEAD_WIDTH // 2)
    first_half = halves[:, :, 0]
    second_half = halves[:, :, 1]
    cos_rows = cos_table[:, None, :]
    sin_rows = sin_table[:, None, :]
    turned = jnp.stack(
        [
            first_half * cos_rows - second_half * sin_rows,
            second_half * cos_rows + first_half * sin_rows,
        ],
        axis=2,
    )
    return turned.reshape(inputs.shape)


def score_block(query_rows, joined_keys, allowed):
    query_total = query_rows.shape[0]
    key_total = joined_keys.shape[0]
    key_value_heads = joined_keys.shape[1] // HEAD_WIDTH
    query_head_rows = query_rows.reshape(
        query_total, key_value_heads, QUERY_HEADS // KEY_VALUE_HEADS, HEAD_WIDTH
    )
    key_head_rows = joined_keys.reshape(key_total, key_value_heads, HEAD_WIDTH)
    scores = (
        jnp.einsum(
            "bhgd,khd->hgbk", query_head_rows, key_head_rows, preferred_element_type=jnp.float32
        )
        * score_scale
    )
    return (jnp.where(allowed[None, None], scores, masked_score), query_head_rows, key_head_rows)


def attend_forward(query_rows, joined_keys, joined_values, allowed):
    scores, query_head_rows, key_head_rows = score_block(query_rows, joined_keys, allowed)
    highest_score = jnp.max(scores, axis=-1, keepdims=True)
    log_total = highest_score + jnp.log(
        jnp.sum(jnp.exp(scores - highest_score), axis=-1, keepdims=True)
    )
    weights = jnp.exp(scores - log_total).astype(jnp.bfloat16)
    value_head_rows = joined_values.reshape(key_head_rows.shape)
    mixed_heads = jnp.einsum(
        "hgbk,khd->bhgd", weights, value_head_rows, preferred_element_type=jnp.float32
    )
    return (mixed_heads.reshape(query_rows.shape[0], -1), log_total)


def attend_backward(query_rows, joined_keys, joined_values, allowed, log_total, upstream):
    scores, query_head_rows, key_head_rows = score_block(query_rows, joined_keys, allowed)
    weights = jnp.exp(scores - log_total)
    value_head_rows = joined_values.reshape(key_head_rows.shape)
    grad_heads = upstream.reshape(query_head_rows.shape)
    grad_weights = jnp.einsum(
        "bhgd,khd->hgbk", grad_heads, value_head_rows, preferred_element_type=jnp.float32
    )
    grad_scores = (
        weights * (grad_weights - jnp.sum(grad_weights * weights, axis=-1, keepdims=True))
    ).astype(jnp.bfloat16)
    grad_query = (
        jnp.einsum("hgbk,khd->bhgd", grad_scores, key_head_rows, preferred_element_type=jnp.float32)
        * score_scale
    )
    grad_key = (
        jnp.einsum(
            "hgbk,bhgd->khd", grad_scores, query_head_rows, preferred_element_type=jnp.float32
        )
        * score_scale
    )
    grad_value = jnp.einsum(
        "hgbk,bhgd->khd",
        weights.astype(jnp.bfloat16),
        grad_heads,
        preferred_element_type=jnp.float32,
    )
    return (
        grad_query.reshape(query_rows.shape[0], -1),
        grad_key.reshape(joined_keys.shape[0], -1),
        grad_value.reshape(joined_keys.shape[0], -1),
    )


def picked(me, arrays, keys):
    out = None
    for key in dict.fromkeys(keys.values()):
        if out is None:
            out = arrays[key]
        else:
            chosen = functools.reduce(
                operator.or_, [me == device for device, held in keys.items() if held == key]
            )
            out = jnp.where(chosen, arrays[key], out)
    return out


def slot_tables(count):
    chunk_of = []
    for device in range(count):
        near = min(device, count - 1 - device)
        far = 1 if device < count - 1 - device else -1
        order = [device]
        for slot in range(1, count):
            if slot <= 2 * near:
                distance = (slot + 1) // 2
                order.append(device - distance if slot % 2 else device + distance)
            else:
                order.append(device + far * (slot - near))
        chunk_of.append(order)
    return chunk_of


def hop_step(forward, backward, step, count):
    return (
        lax.ppermute(forward, "tensor", [(i, i + 1) for i in range(step - 1, count - 1)]),
        lax.ppermute(backward, "tensor", [(i, i - 1) for i in range(1, count - step + 1)]),
    )


def added(first, second):
    return (first.astype(jnp.float32) + second.astype(jnp.float32)).astype(jnp.bfloat16)


def sum_step(state, part_at, distance, count):
    to_right = part_at(distance)
    to_left = part_at(-distance)
    if state is not None:
        to_right = added(to_right, state[0])
        to_left = added(to_left, state[1])
    return (
        lax.ppermute(to_right, "tensor", [(i, i + 1) for i in range(0, count - distance)]),
        lax.ppermute(to_left, "tensor", [(i, i - 1) for i in range(distance, count)]),
    )


def sum_end(state, part_at):
    return sum(part.astype(jnp.float32) for part in (part_at(0), *state))


def tied(*values):
    return lax.optimization_barrier(values)


def exchanged(me, send_block, count):
    received = {0: send_block(me)}
    for shift in range(1, count):
        received[shift] = lax.ppermute(
            send_block(lax.rem(me + shift, count)),
            "tensor",
            [(i, (i + shift) % count) for i in range(count)],
        )
    return [
        picked(me, received, {i: (i - source) % count for i in range(count)})
        for source in range(count)
    ]


def shards(
    prompt_in,
    cont_in,
    prompt_len,
    norm_attn,
    w_query,
    key_weight,
    value_weight,
    w_out,
    norm_mlp,
    w_gate,
    w_up,
    w_down,
    prompt_cot,
    cont_cot,
):
    own_rows = prompt_in.shape[1]
    cont_count = cont_in.shape[1]
    width = prompt_in.shape[2]
    cont_rows = cont_count * CONT_LENGTH
    total_rows = own_rows + cont_rows
    key_width = key_weight.shape[1]
    ctx_index = lax.axis_index("ctx")
    count = lax.axis_size("tensor")
    me = lax.axis_index("tensor")
    share_rows = total_rows // count
    share_start = me * share_rows
    head_half = w_out.shape[0] // 2
    kv_heads = key_weight.shape[1] // HEAD_WIDTH
    group_width = w_out.shape[0] // kv_heads
    order = slot_tables(count)
    slot_chunks = [
        picked(me, {i: jnp.int32(i) for i in range(count)}, {i: order[i][s] for i in range(count)})
        for s in range(count)
    ]
    slot_of = [[order[i].index(c) for c in range(count)] for i in range(count)]
    token_length = prompt_len[0]
    gain_attn = norm_attn.astype(jnp.float32)
    gain_mlp = norm_mlp.astype(jnp.float32)

    def share_of(values):
        return lax.dynamic_slice_in_dim(values, share_start, share_rows, 0)

    def slot_order(values):
        return jnp.concatenate(
            [
                lax.dynamic_slice_in_dim(values, slot_chunks[s] * share_rows, share_rows, 0)
                for s in range(count)
            ],
            axis=0,
        )

    def slots_from(arrived):
        return [
            picked(me, arrived, {i: order[i][s] - i for i in range(count)}) for s in range(count)
        ]

    def slot_part(parts):
        return lambda distance: picked(
            me,
            parts,
            {i: slot_of[i][i + distance] for i in range(count) if 0 <= i + distance < count},
        )

    own_out_half = lax.dynamic_slice_in_dim(w_out, ctx_index * head_half, head_half, 0)
    full_out = lax.all_gather(own_out_half, ("tensor", "ctx"), axis=0, tiled=True)
    all_rows = jnp.concatenate([prompt_in[0], cont_in[0].reshape(cont_rows, width)], axis=0).astype(
        jnp.float32
    )
    input_share = share_of(all_rows)
    within = jnp.arange(cont_rows, dtype=jnp.int32) % CONT_LENGTH
    owner = jnp.arange(cont_rows, dtype=jnp.int32) // CONT_LENGTH
    positions = jnp.concatenate(
        [ctx_index * own_rows + jnp.arange(own_rows, dtype=jnp.int32), token_length + within]
    )
    cos_table, sin_table = angle_tables(positions)
    act_a = norm_rows(all_rows, gain_attn).astype(jnp.bfloat16)
    query_rows = rotate(
        jnp.dot(act_a, w_query, preferred_element_type=jnp.float32), cos_table, sin_table
    ).astype(jnp.bfloat16)
    joined_keys = rotate(
        jnp.dot(act_a, key_weight, preferred_element_type=jnp.float32), cos_table, sin_table
    ).astype(jnp.bfloat16)
    joined_values = jnp.dot(act_a, value_weight, preferred_element_type=jnp.float32).astype(
        jnp.bfloat16
    )
    local_pairs = jnp.concatenate([joined_keys[:own_rows], joined_values[:own_rows]], axis=1)
    prompt_pairs = lax.all_gather(local_pairs, "ctx", axis=0, tiled=True)
    prompt_total = prompt_pairs.shape[0]
    shared_prompt_keys = prompt_pairs[:, :key_width]
    shared_prompt_values = prompt_pairs[:, key_width:]
    key_place = jnp.arange(prompt_total, dtype=jnp.int32)
    key_valid = key_place < token_length
    block_rows = min(512, own_rows)
    block_index = 0
    query_place = (
        ctx_index * own_rows + block_index * block_rows + jnp.arange(block_rows, dtype=jnp.int32)
    )
    block_masks = [(key_place[None, :] <= query_place[:, None]) & key_valid[None, :]]
    cont_mask = jnp.concatenate(
        [
            jnp.broadcast_to(key_valid[None, :], (cont_rows, prompt_total)),
            (owner[:, None] == owner[None, :]) & (within[None, :] <= within[:, None]),
        ],
        axis=1,
    )
    cont_keys = jnp.concatenate([shared_prompt_keys, joined_keys[own_rows:]], axis=0)
    cont_values = jnp.concatenate([shared_prompt_values, joined_values[own_rows:]], axis=0)
    prompt_mask = block_masks[0]

    def head_inputs(head, prompt):
        wide = slice(head * group_width, (head + 1) * group_width)
        thin = slice(head * HEAD_WIDTH, (head + 1) * HEAD_WIDTH)
        if prompt:
            return (
                query_rows[:own_rows, wide],
                shared_prompt_keys[:, thin],
                shared_prompt_values[:, thin],
                prompt_mask,
            )
        return (query_rows[own_rows:, wide], cont_keys[:, thin], cont_values[:, thin], cont_mask)

    mixed_list = []
    totals = {}
    share_list = []
    for head in range(kv_heads):
        mixed_prompt, totals[head, True] = attend_forward(*head_inputs(head, True))
        mixed_cont, totals[head, False] = attend_forward(*head_inputs(head, False))
        mixed = jnp.concatenate([mixed_prompt, mixed_cont], axis=0).astype(jnp.bfloat16)
        mixed_list.append(mixed)
        share_list.append(
            exchanged(
                me,
                lambda target: lax.dynamic_slice_in_dim(mixed, target * share_rows, share_rows, 0),
                count,
            )
        )
    upstream = jnp.concatenate([prompt_cot[0], cont_cot[0].reshape(cont_rows, width)], axis=0)
    grad_mlp = slot_order((branch_scale * upstream.astype(jnp.float32)).astype(jnp.bfloat16))
    mixed_list[-1], grad_mlp = tied(mixed_list[-1], grad_mlp)
    grad_hidden = jnp.einsum("rd,fd->rf", grad_mlp, w_down, preferred_element_type=jnp.float32)
    share_list[-1], grad_hidden = tied(share_list[-1], grad_hidden)
    mixed_heads = jnp.concatenate(mixed_list, axis=1)
    mixed_share = jnp.concatenate(
        [share_list[head][source] for source in range(count) for head in range(kv_heads)], axis=1
    )
    attn_share = jnp.dot(mixed_share, full_out, preferred_element_type=jnp.float32)
    hidden_share = input_share + branch_scale * attn_share
    act_b_share = norm_rows(hidden_share, gain_mlp).astype(jnp.bfloat16)
    forward, backward = (act_b_share, act_b_share)
    arrived = {0: act_b_share}
    for step in range(1, count):
        forward, backward = hop_step(forward, backward, step, count)
        arrived[-step], arrived[step] = (forward, backward)
    act_b_slots = slots_from(arrived)
    hidden_list, gate_list, up_list, part_list = ([], [], [], [])
    for s in range(count):
        gate_proj = jnp.dot(act_b_slots[s], w_gate, preferred_element_type=jnp.float32)
        up_proj = jnp.dot(act_b_slots[s], w_up, preferred_element_type=jnp.float32)
        sigmoid_gate = jax.nn.sigmoid(gate_proj)
        silu_gate = gate_proj * sigmoid_gate
        grad_slot = grad_hidden[s * share_rows : (s + 1) * share_rows]
        hidden = (silu_gate * up_proj).astype(jnp.bfloat16)
        grad_gate_slot = (
            grad_slot * up_proj * sigmoid_gate * (1.0 + gate_proj * (1.0 - sigmoid_gate))
        ).astype(jnp.bfloat16)
        grad_up_slot = (grad_slot * silu_gate).astype(jnp.bfloat16)
        part = (
            jnp.einsum("rf,df->rd", grad_gate_slot, w_gate, preferred_element_type=jnp.float32)
            + jnp.einsum("rf,df->rd", grad_up_slot, w_up, preferred_element_type=jnp.float32)
        ).astype(jnp.bfloat16)
        if s + 1 < count:
            hidden, grad_gate_slot, grad_up_slot, part, act_b_slots[s + 1] = tied(
                hidden, grad_gate_slot, grad_up_slot, part, act_b_slots[s + 1]
            )
        hidden_list.append(hidden)
        gate_list.append(grad_gate_slot)
        up_list.append(grad_up_slot)
        part_list.append(part)
    last = count - 1
    part_list[last], hidden_list[last], gate_list[last], up_list[last] = tied(
        part_list[last], hidden_list[last], gate_list[last], up_list[last]
    )
    act_b = jnp.concatenate(act_b_slots, axis=0)
    hidden_act = jnp.concatenate(hidden_list, axis=0)
    grad_gate_act = jnp.concatenate(gate_list, axis=0)
    grad_up_act = jnp.concatenate(up_list, axis=0)

    def over_tokens(values):
        return lax.psum_scatter(
            values.astype(jnp.bfloat16), ("dp", "ctx"), scatter_dimension=0, tiled=True
        )

    fillers = [
        lambda: jnp.einsum(
            "rd,rf->df",
            act_b,
            jnp.concatenate([grad_gate_act, grad_up_act], axis=1),
            preferred_element_type=jnp.float32,
        ),
        lambda: jnp.einsum("rf,rd->df", hidden_act, grad_mlp, preferred_element_type=jnp.float32),
        lambda: jnp.dot(hidden_act, w_down, preferred_element_type=jnp.float32),
    ]
    filled = []
    state = None
    for distance in range(count - 1, 0, -1):
        state = sum_step(state, slot_part(part_list), distance, count)
        if fillers:
            filled.append(fillers.pop(0)().astype(jnp.bfloat16))
            state, filled[-1] = tied(state, filled[-1])
    filled.extend(filler().astype(jnp.bfloat16) for filler in fillers)
    wide_sum = over_tokens(filled[0])
    down_sum = over_tokens(filled[1])
    mlp_part = filled[2]
    normed_share = sum_end(state, slot_part(part_list))
    through_mlp, gain_mlp_part = norm_back(hidden_share, gain_mlp, normed_share)
    res_share = share_of(upstream).astype(jnp.float32) + through_mlp
    grad_attn_share = (branch_scale * res_share).astype(jnp.bfloat16)
    mixed_grad = jnp.einsum(
        "rd,qd->rq", grad_attn_share, full_out, preferred_element_type=jnp.float32
    ).astype(jnp.bfloat16)
    grad_list = []
    for head in range(kv_heads):
        grad_list.append(
            jnp.concatenate(
                exchanged(
                    me,
                    lambda target: lax.dynamic_slice_in_dim(
                        mixed_grad,
                        target * (kv_heads * group_width) + head * group_width,
                        group_width,
                        1,
                    ),
                    count,
                ),
                axis=0,
            )
        )
    mlp_slots = slot_part(
        [mlp_part[s * share_rows : (s + 1) * share_rows] for s in range(count)]
    )
    pieces = [(head, prompt) for head in range(kv_heads) for prompt in (True, False)]
    upstream_pieces = {
        (head, prompt): grad_list[head][:own_rows] if prompt else grad_list[head][own_rows:]
        for head, prompt in pieces
    }
    piece_grads = {}
    upstream_pieces[pieces[0]], gather_start = tied(upstream_pieces[pieces[0]], grad_attn_share)
    arrived = {0: grad_attn_share}
    forward, backward = (gather_start, gather_start)
    mlp_state = None
    for place in range(max(count, len(pieces))):
        moved = []
        if place < count - 1:
            forward, backward = hop_step(forward, backward, place + 1, count)
            moved += [forward, backward]
        if 1 <= place < count:
            mlp_state = sum_step(mlp_state, mlp_slots, count - place, count)
            moved += mlp_state
        if place < len(pieces):
            query_piece, keys_piece, values_piece, mask_piece = head_inputs(*pieces[place])
            piece_grads[pieces[place]] = attend_backward(
                query_piece,
                keys_piece,
                values_piece,
                mask_piece,
                totals[pieces[place]],
                upstream_pieces[pieces[place]],
            )
        if place + 1 < len(pieces):
            following = pieces[place + 1]
            moved, piece_grads[pieces[place]], upstream_pieces[following] = tied(
                moved, piece_grads[pieces[place]], upstream_pieces[following]
            )
        if place < count - 1:
            forward, backward, *moved = moved
            arrived[-place - 1], arrived[place + 1] = (forward, backward)
        if 1 <= place < count:
            mlp_state = tuple(moved)
    mlp_share = sum_end(mlp_state, mlp_slots)
    result_share = (hidden_share + branch_scale * mlp_share).astype(jnp.bfloat16)
    grad_attn = jnp.concatenate(slots_from(arrived), axis=0)
    grad_out = jnp.einsum(
        "rq,rd->dq", slot_order(mixed_heads), grad_attn, preferred_element_type=jnp.float32
    )
    query_grad_rows = jnp.concatenate(
        [
            jnp.concatenate([piece_grads[head, True][0], piece_grads[head, False][0]], axis=0)
            for head in range(kv_heads)
        ],
        axis=1,
    )
    prompt_pairs_grad = jnp.concatenate(
        [
            piece_grads[head, True][which] + piece_grads[head, False][which][:prompt_total]
            for which in (1, 2)
            for head in range(kv_heads)
        ],
        axis=1,
    )
    grad_key_cont, grad_value_cont = (
        jnp.concatenate([piece_grads[head, False][which] for head in range(kv_heads)], axis=1)
        for which in (1, 2)
    )
    other_pairs = lax.ppermute(
        lax.dynamic_slice_in_dim(prompt_pairs_grad, (1 - ctx_index) * own_rows, own_rows, 0),
        "ctx",
        [(0, 1), (1, 0)],
    )
    pair_grads = other_pairs + lax.dynamic_slice_in_dim(
        prompt_pairs_grad, ctx_index * own_rows, own_rows, 0
    )
    key_grad_rows = jnp.concatenate(
        [pair_grads[:, :key_width], grad_key_cont[prompt_total:]], axis=0
    )
    value_grad_rows = jnp.concatenate(
        [pair_grads[:, key_width:], grad_value_cont[prompt_total:]], axis=0
    )
    grad_query_lin = rotate(query_grad_rows, cos_table, -sin_table).astype(jnp.bfloat16)
    grad_key_lin = rotate(key_grad_rows, cos_table, -sin_table).astype(jnp.bfloat16)
    grad_value_lin = value_grad_rows.astype(jnp.bfloat16)
    grad_query = jnp.einsum("rd,rq->dq", act_a, grad_query_lin, preferred_element_type=jnp.float32)
    grad_key = jnp.einsum("rd,rq->dq", act_a, grad_key_lin, preferred_element_type=jnp.float32)
    grad_value = jnp.einsum("rd,rq->dq", act_a, grad_value_lin, preferred_element_type=jnp.float32)
    input_grad = (
        jnp.einsum("rq,dq->rd", grad_query_lin, w_query, preferred_element_type=jnp.float32)
        + jnp.einsum("rq,dq->rd", grad_key_lin, key_weight, preferred_element_type=jnp.float32)
        + jnp.einsum("rq,dq->rd", grad_value_lin, value_weight, preferred_element_type=jnp.float32)
    )
    input_part = input_grad.astype(jnp.bfloat16)

    def row_part(distance):
        place = jnp.clip(me + distance, 0, count - 1) * share_rows
        return lax.dynamic_slice_in_dim(input_part, place, share_rows, 0)

    state = None
    forward, backward = hop_step(result_share, result_share, 1, count)
    forward, backward, input_part, wide_sum = tied(forward, backward, input_part, wide_sum)
    result_arrived = {0: result_share, -1: forward, 1: backward}
    for distance in range(count - 1, 0, -1):
        state = sum_step(state, row_part, distance, count)
        step = count - distance + 1
        if step < count:
            forward, backward = hop_step(forward, backward, step, count)
            state, forward, backward, down_sum = tied(state, forward, backward, down_sum)
            result_arrived[-step], result_arrived[step] = (forward, backward)
    input_grad_share = sum_end(state, row_part)

    def rows_from(arrived):
        chunks = [picked(me, arrived, {i: c - i for i in range(count)}) for c in range(count)]
        gathered = jnp.concatenate(chunks, axis=0)
        return (
            gathered[:own_rows][None],
            gathered[own_rows:].reshape(1, cont_count, CONT_LENGTH, width),
        )

    prompt_out, cont_out = rows_from(result_arrived)
    through_attn, gain_attn_part = norm_back(input_share, gain_attn, input_grad_share)
    grad_share = (res_share + through_attn).astype(jnp.bfloat16)
    forward, backward = (grad_share, grad_share)
    arrived = {0: grad_share}
    for step in range(1, count):
        forward, backward = hop_step(forward, backward, step, count)
        arrived[-step], arrived[step] = (forward, backward)
    prompt_grad, cont_grad = rows_from(arrived)
    gain_own = lax.psum(
        lax.psum_scatter(
            jnp.stack([gain_attn_part, gain_mlp_part]),
            ("dp", "ctx"),
            scatter_dimension=1,
            tiled=True,
        ),
        "tensor",
    )
    attn_sum = lax.psum_scatter(
        jnp.concatenate([grad_query, grad_key, grad_value, grad_out], axis=1).astype(jnp.bfloat16),
        ("dp", "ctx"),
        scatter_dimension=0,
        tiled=True,
    ).astype(jnp.float32)
    qw = grad_query.shape[1]
    ff = w_gate.shape[1]
    summed = (
        gain_own[0],
        attn_sum[:, :qw],
        attn_sum[:, qw : qw + key_width],
        attn_sum[:, qw + key_width : qw + 2 * key_width],
        attn_sum[:, qw + 2 * key_width :].T,
        gain_own[1],
        wide_sum[:, :ff].astype(jnp.float32),
        wide_sum[:, ff:].astype(jnp.float32),
        down_sum.astype(jnp.float32).T,
    )
    return (
        prompt_out,
        cont_out,
        prompt_grad,
        cont_grad,
        summed[0],
        summed[1],
        summed[2],
        summed[3],
        summed[4],
        summed[5],
        summed[6],
        summed[7],
        summed[8],
    )


def solution(mesh):
    in_specs = (
        P("dp", "ctx", None),
        P("dp", "ctx", None, None),
        P("dp"),
        P(),
        P(None, "tensor"),
        P(None, "tensor"),
        P(None, "tensor"),
        P("tensor", None),
        P(),
        P(None, "tensor"),
        P(None, "tensor"),
        P("tensor", None),
        P("dp", "ctx", None),
        P("dp", "ctx", None, None),
    )
    out_specs = (
        P("dp", "ctx", None),
        P("dp", "ctx", None, None),
        P("dp", "ctx", None),
        P("dp", "ctx", None, None),
        P(("dp", "ctx")),
        P(("dp", "ctx"), "tensor"),
        P(("dp", "ctx"), "tensor"),
        P(("dp", "ctx"), "tensor"),
        P("tensor", ("dp", "ctx")),
        P(("dp", "ctx")),
        P(("dp", "ctx"), "tensor"),
        P(("dp", "ctx"), "tensor"),
        P("tensor", ("dp", "ctx")),
    )
    return jax.shard_map(shards, mesh=mesh, in_specs=in_specs, out_specs=out_specs, check_vma=False)
```

```python
import functools
import math
import operator

import jax
import jax.numpy as jnp
from jax import lax
from jax.sharding import PartitionSpec as P

QUERY_HEADS = 32
KEY_VALUE_HEADS = 8
HEAD_WIDTH = 64
CONT_LENGTH = 128


norm_eps = 1e-05
rope_base = 10000000.0
score_scale = 0.015625
branch_scale = 0.22
masked_score = -1e30


def norm_rows(inputs, weight):
    return inputs * lax.rsqrt(jnp.mean(inputs * inputs, axis=-1, keepdims=True) + norm_eps) * weight


def norm_back(inputs, weight, upstream):
    factor = lax.rsqrt(jnp.mean(inputs * inputs, axis=-1, keepdims=True) + norm_eps)
    scaled = inputs * factor
    weighted = upstream * weight
    through = factor * (weighted - scaled * jnp.mean(weighted * scaled, axis=-1, keepdims=True))
    return (through, jnp.sum(upstream * scaled, axis=0))


def angle_tables(position):
    freq = jnp.exp(
        jnp.arange(HEAD_WIDTH // 2, dtype=jnp.float32) * (-2.0 * math.log(rope_base) / HEAD_WIDTH)
    )
    angle = position.astype(jnp.float32)[:, None] * freq[None, :]
    return (jnp.cos(angle), jnp.sin(angle))


def rotate(inputs, cos_table, sin_table):
    halves = inputs.reshape(inputs.shape[0], -1, 2, HEAD_WIDTH // 2)
    first_half = halves[:, :, 0]
    second_half = halves[:, :, 1]
    cos_rows = cos_table[:, None, :]
    sin_rows = sin_table[:, None, :]
    turned = jnp.stack(
        [
            first_half * cos_rows - second_half * sin_rows,
            second_half * cos_rows + first_half * sin_rows,
        ],
        axis=2,
    )
    return turned.reshape(inputs.shape)


def score_block(query_rows, joined_keys, allowed):
    query_total = query_rows.shape[0]
    key_total = joined_keys.shape[0]
    key_value_heads = joined_keys.shape[1] // HEAD_WIDTH
    query_head_rows = query_rows.reshape(
        query_total, key_value_heads, QUERY_HEADS // KEY_VALUE_HEADS, HEAD_WIDTH
    )
    key_head_rows = joined_keys.reshape(key_total, key_value_heads, HEAD_WIDTH)
    scores = (
        jnp.einsum(
            "bhgd,khd->hgbk", query_head_rows, key_head_rows, preferred_element_type=jnp.float32
        )
        * score_scale
    )
    return (jnp.where(allowed[None, None], scores, masked_score), query_head_rows, key_head_rows)


def attend_forward(query_rows, joined_keys, joined_values, allowed):
    scores, query_head_rows, key_head_rows = score_block(query_rows, joined_keys, allowed)
    highest_score = jnp.max(scores, axis=-1, keepdims=True)
    log_total = highest_score + jnp.log(
        jnp.sum(jnp.exp(scores - highest_score), axis=-1, keepdims=True)
    )
    weights = jnp.exp(scores - log_total).astype(jnp.bfloat16)
    value_head_rows = joined_values.reshape(key_head_rows.shape)
    mixed_heads = jnp.einsum(
        "hgbk,khd->bhgd", weights, value_head_rows, preferred_element_type=jnp.float32
    )
    return (mixed_heads.reshape(query_rows.shape[0], -1), log_total)


def attend_backward(query_rows, joined_keys, joined_values, allowed, log_total, upstream):
    scores, query_head_rows, key_head_rows = score_block(query_rows, joined_keys, allowed)
    weights = jnp.exp(scores - log_total)
    value_head_rows = joined_values.reshape(key_head_rows.shape)
    grad_heads = upstream.reshape(query_head_rows.shape)
    grad_weights = jnp.einsum(
        "bhgd,khd->hgbk", grad_heads, value_head_rows, preferred_element_type=jnp.float32
    )
    grad_scores = (
        weights * (grad_weights - jnp.sum(grad_weights * weights, axis=-1, keepdims=True))
    ).astype(jnp.bfloat16)
    grad_query = (
        jnp.einsum("hgbk,khd->bhgd", grad_scores, key_head_rows, preferred_element_type=jnp.float32)
        * score_scale
    )
    grad_key = (
        jnp.einsum(
            "hgbk,bhgd->khd", grad_scores, query_head_rows, preferred_element_type=jnp.float32
        )
        * score_scale
    )
    grad_value = jnp.einsum(
        "hgbk,bhgd->khd",
        weights.astype(jnp.bfloat16),
        grad_heads,
        preferred_element_type=jnp.float32,
    )
    return (
        grad_query.reshape(query_rows.shape[0], -1),
        grad_key.reshape(joined_keys.shape[0], -1),
        grad_value.reshape(joined_keys.shape[0], -1),
    )


def picked(me, arrays, keys):
    out = None
    for key in dict.fromkeys(keys.values()):
        if out is None:
            out = arrays[key]
        else:
            chosen = functools.reduce(
                operator.or_, [me == device for device, held in keys.items() if held == key]
            )
            out = jnp.where(chosen, arrays[key], out)
    return out


def slot_tables(count):
    chunk_of = []
    for device in range(count):
        near = min(device, count - 1 - device)
        far = 1 if device < count - 1 - device else -1
        order = [device]
        for slot in range(1, count):
            if slot <= 2 * near:
                distance = (slot + 1) // 2
                order.append(device - distance if slot % 2 else device + distance)
            else:
                order.append(device + far * (slot - near))
        chunk_of.append(order)
    return chunk_of


def hop_step(forward, backward, step, count):
    return (
        lax.ppermute(forward, "tensor", [(i, i + 1) for i in range(step - 1, count - 1)]),
        lax.ppermute(backward, "tensor", [(i, i - 1) for i in range(1, count - step + 1)]),
    )


def added(first, second):
    return (first.astype(jnp.float32) + second.astype(jnp.float32)).astype(jnp.bfloat16)


def sum_step(state, part_at, distance, count):
    to_right = part_at(distance)
    to_left = part_at(-distance)
    if state is not None:
        to_right = added(to_right, state[0])
        to_left = added(to_left, state[1])
    return (
        lax.ppermute(to_right, "tensor", [(i, i + 1) for i in range(0, count - distance)]),
        lax.ppermute(to_left, "tensor", [(i, i - 1) for i in range(distance, count)]),
    )


def sum_end(state, part_at):
    return sum(part.astype(jnp.float32) for part in (part_at(0), *state))


def tied(*values):
    return lax.optimization_barrier(values)


def exchanged(me, send_block, count):
    received = {0: send_block(me)}
    for shift in range(1, count):
        received[shift] = lax.ppermute(
            send_block(lax.rem(me + shift, count)),
            "tensor",
            [(i, (i + shift) % count) for i in range(count)],
        )
    return [
        picked(me, received, {i: (i - source) % count for i in range(count)})
        for source in range(count)
    ]


def pair_stages():
    return [
        (axis, 1 << bit)
        for axis in ("ctx", "tensor", "dp")
        for bit in range(lax.axis_size(axis).bit_length() - 1)
    ]


def pair_sum(values, axis, distance):
    return values + lax.ppermute(
        values, axis, [(i, i ^ distance) for i in range(lax.axis_size(axis))]
    )


def shards(
    prompt_in,
    cont_in,
    prompt_len,
    norm_attn,
    w_query,
    key_weight,
    value_weight,
    w_out,
    norm_mlp,
    w_gate,
    w_up,
    w_down,
    prompt_cot,
    cont_cot,
):
    own_rows = prompt_in.shape[1]
    cont_count = cont_in.shape[1]
    width = prompt_in.shape[2]
    cont_rows = cont_count * CONT_LENGTH
    total_rows = own_rows + cont_rows
    key_width = key_weight.shape[1]
    ctx_index = lax.axis_index("ctx")
    count = lax.axis_size("tensor")
    me = lax.axis_index("tensor")
    share_rows = total_rows // count
    share_start = me * share_rows
    head_half = w_out.shape[0] // 2
    kv_heads = key_weight.shape[1] // HEAD_WIDTH
    group_width = w_out.shape[0] // kv_heads
    order = slot_tables(count)
    slot_chunks = [
        picked(me, {i: jnp.int32(i) for i in range(count)}, {i: order[i][s] for i in range(count)})
        for s in range(count)
    ]
    slot_of = [[order[i].index(c) for c in range(count)] for i in range(count)]
    token_length = prompt_len[0]
    gain_attn = norm_attn.astype(jnp.float32)
    gain_mlp = norm_mlp.astype(jnp.float32)

    def share_of(values):
        return lax.dynamic_slice_in_dim(values, share_start, share_rows, 0)

    def slot_order(values):
        return jnp.concatenate(
            [
                lax.dynamic_slice_in_dim(values, slot_chunks[s] * share_rows, share_rows, 0)
                for s in range(count)
            ],
            axis=0,
        )

    def slots_from(arrived):
        return [
            picked(me, arrived, {i: order[i][s] - i for i in range(count)}) for s in range(count)
        ]

    def slot_part(parts):
        return lambda distance: picked(
            me,
            parts,
            {i: slot_of[i][i + distance] for i in range(count) if 0 <= i + distance < count},
        )

    own_out_half = lax.dynamic_slice_in_dim(w_out, ctx_index * head_half, head_half, 0)
    full_out = lax.all_gather(own_out_half, ("tensor", "ctx"), axis=0, tiled=True)
    all_rows = jnp.concatenate([prompt_in[0], cont_in[0].reshape(cont_rows, width)], axis=0).astype(
        jnp.float32
    )
    input_share = share_of(all_rows)
    within = jnp.arange(cont_rows, dtype=jnp.int32) % CONT_LENGTH
    owner = jnp.arange(cont_rows, dtype=jnp.int32) // CONT_LENGTH
    positions = jnp.concatenate(
        [ctx_index * own_rows + jnp.arange(own_rows, dtype=jnp.int32), token_length + within]
    )
    cos_table, sin_table = angle_tables(positions)
    act_a = norm_rows(all_rows, gain_attn).astype(jnp.bfloat16)
    query_rows = rotate(
        jnp.dot(act_a, w_query, preferred_element_type=jnp.float32), cos_table, sin_table
    ).astype(jnp.bfloat16)
    joined_keys = rotate(
        jnp.dot(act_a, key_weight, preferred_element_type=jnp.float32), cos_table, sin_table
    ).astype(jnp.bfloat16)
    joined_values = jnp.dot(act_a, value_weight, preferred_element_type=jnp.float32).astype(
        jnp.bfloat16
    )
    local_pairs = jnp.concatenate([joined_keys[:own_rows], joined_values[:own_rows]], axis=1)
    prompt_pairs = lax.all_gather(local_pairs, "ctx", axis=0, tiled=True)
    prompt_total = prompt_pairs.shape[0]
    shared_prompt_keys = prompt_pairs[:, :key_width]
    shared_prompt_values = prompt_pairs[:, key_width:]
    key_place = jnp.arange(prompt_total, dtype=jnp.int32)
    key_valid = key_place < token_length
    block_rows = min(512, own_rows)
    block_index = 0
    query_place = (
        ctx_index * own_rows + block_index * block_rows + jnp.arange(block_rows, dtype=jnp.int32)
    )
    block_masks = [(key_place[None, :] <= query_place[:, None]) & key_valid[None, :]]
    cont_mask = jnp.concatenate(
        [
            jnp.broadcast_to(key_valid[None, :], (cont_rows, prompt_total)),
            (owner[:, None] == owner[None, :]) & (within[None, :] <= within[:, None]),
        ],
        axis=1,
    )
    cont_keys = jnp.concatenate([shared_prompt_keys, joined_keys[own_rows:]], axis=0)
    cont_values = jnp.concatenate([shared_prompt_values, joined_values[own_rows:]], axis=0)
    prompt_mask = block_masks[0]

    def head_inputs(head, prompt):
        wide = slice(head * group_width, (head + 1) * group_width)
        thin = slice(head * HEAD_WIDTH, (head + 1) * HEAD_WIDTH)
        if prompt:
            return (
                query_rows[:own_rows, wide],
                shared_prompt_keys[:, thin],
                shared_prompt_values[:, thin],
                prompt_mask,
            )
        return (query_rows[own_rows:, wide], cont_keys[:, thin], cont_values[:, thin], cont_mask)

    mixed_list = []
    totals = {}
    share_list = []
    for head in range(kv_heads):
        mixed_prompt, totals[head, True] = attend_forward(*head_inputs(head, True))
        mixed_cont, totals[head, False] = attend_forward(*head_inputs(head, False))
        mixed = jnp.concatenate([mixed_prompt, mixed_cont], axis=0).astype(jnp.bfloat16)
        mixed_list.append(mixed)
        share_list.append(
            exchanged(
                me,
                lambda target: lax.dynamic_slice_in_dim(mixed, target * share_rows, share_rows, 0),
                count,
            )
        )
    upstream = jnp.concatenate([prompt_cot[0], cont_cot[0].reshape(cont_rows, width)], axis=0)
    grad_mlp = slot_order((branch_scale * upstream.astype(jnp.float32)).astype(jnp.bfloat16))
    mixed_list[-1], grad_mlp = tied(mixed_list[-1], grad_mlp)
    grad_hidden = jnp.einsum("rd,fd->rf", grad_mlp, w_down, preferred_element_type=jnp.float32)
    share_list[-1], grad_hidden = tied(share_list[-1], grad_hidden)
    mixed_heads = jnp.concatenate(mixed_list, axis=1)
    mixed_share = jnp.concatenate(
        [share_list[head][source] for source in range(count) for head in range(kv_heads)], axis=1
    )
    attn_share = jnp.dot(mixed_share, full_out, preferred_element_type=jnp.float32)
    hidden_share = input_share + branch_scale * attn_share
    act_b_share = norm_rows(hidden_share, gain_mlp).astype(jnp.bfloat16)
    forward, backward = (act_b_share, act_b_share)
    arrived = {0: act_b_share}
    act_b_slots = []
    hidden_list, gate_list, up_list, part_list = ([], [], [], [])
    for s in range(count):
        act_b_slots.append(
            picked(me, arrived, {i: order[i][s] - i for i in range(count)})
        )
        if s + 1 < count:
            forward, backward = hop_step(forward, backward, s + 1, count)
        gate_proj = jnp.dot(act_b_slots[s], w_gate, preferred_element_type=jnp.float32)
        up_proj = jnp.dot(act_b_slots[s], w_up, preferred_element_type=jnp.float32)
        sigmoid_gate = jax.nn.sigmoid(gate_proj)
        silu_gate = gate_proj * sigmoid_gate
        grad_slot = grad_hidden[s * share_rows : (s + 1) * share_rows]
        hidden = (silu_gate * up_proj).astype(jnp.bfloat16)
        grad_gate_slot = (
            grad_slot * up_proj * sigmoid_gate * (1.0 + gate_proj * (1.0 - sigmoid_gate))
        ).astype(jnp.bfloat16)
        grad_up_slot = (grad_slot * silu_gate).astype(jnp.bfloat16)
        part = (
            jnp.einsum("rf,df->rd", grad_gate_slot, w_gate, preferred_element_type=jnp.float32)
            + jnp.einsum("rf,df->rd", grad_up_slot, w_up, preferred_element_type=jnp.float32)
        ).astype(jnp.bfloat16)
        forward, backward, hidden, grad_gate_slot, grad_up_slot, part = tied(
            forward, backward, hidden, grad_gate_slot, grad_up_slot, part
        )
        arrived[-s - 1], arrived[s + 1] = (forward, backward)
        hidden_list.append(hidden)
        gate_list.append(grad_gate_slot)
        up_list.append(grad_up_slot)
        part_list.append(part)
    act_b = jnp.concatenate(act_b_slots, axis=0)
    hidden_act = jnp.concatenate(hidden_list, axis=0)
    grad_gate_act = jnp.concatenate(gate_list, axis=0)
    grad_up_act = jnp.concatenate(up_list, axis=0)

    def over_tokens(values):
        return lax.psum_scatter(
            values.astype(jnp.bfloat16), ("dp", "ctx"), scatter_dimension=0, tiled=True
        )

    fillers = [
        lambda: jnp.einsum("rd,rf->df", act_b, grad_gate_act, preferred_element_type=jnp.float32),
        lambda: jnp.einsum("rd,rf->df", act_b, grad_up_act, preferred_element_type=jnp.float32),
        lambda: jnp.einsum("rf,rd->df", hidden_act, grad_mlp, preferred_element_type=jnp.float32),
    ]
    filled = []
    state = None
    for distance in range(count - 1, 0, -1):
        state = sum_step(state, slot_part(part_list), distance, count)
        if fillers:
            filled.append(fillers.pop(0)().astype(jnp.bfloat16))
            state, filled[-1] = tied(state, filled[-1])
    filled.extend(filler().astype(jnp.bfloat16) for filler in fillers)
    gate_sum, up_sum, down_sum = (over_tokens(product) for product in filled)
    normed_share = sum_end(state, slot_part(part_list))
    through_mlp, gain_mlp_part = norm_back(hidden_share, gain_mlp, normed_share)
    res_share = share_of(upstream).astype(jnp.float32) + through_mlp
    grad_attn_share = (branch_scale * res_share).astype(jnp.bfloat16)
    mixed_grad = jnp.einsum(
        "rd,qd->rq", grad_attn_share, full_out, preferred_element_type=jnp.float32
    ).astype(jnp.bfloat16)
    grad_mixed = jnp.concatenate(
        exchanged(
            me,
            lambda target: lax.dynamic_slice_in_dim(
                mixed_grad, target * w_out.shape[0], w_out.shape[0], 1
            ),
            count,
        ),
        axis=0,
    )
    hidden_act, mixed_grad = tied(hidden_act, mixed_grad)
    mlp_part = jnp.dot(hidden_act, w_down, preferred_element_type=jnp.float32).astype(jnp.bfloat16)
    grad_mixed, mlp_part = tied(grad_mixed, mlp_part)
    mlp_slots = slot_part(
        [mlp_part[s * share_rows : (s + 1) * share_rows] for s in range(count)]
    )
    pieces = [(head, prompt) for head in range(kv_heads) for prompt in (True, False)]
    upstream_pieces = {
        (head, prompt): grad_mixed[
            (slice(0, own_rows) if prompt else slice(own_rows, total_rows)),
            head * group_width : (head + 1) * group_width,
        ]
        for head, prompt in pieces
    }
    piece_grads = {}
    upstream_pieces[pieces[0]], gather_start = tied(upstream_pieces[pieces[0]], grad_attn_share)
    arrived = {0: grad_attn_share}
    forward, backward = (gather_start, gather_start)
    mlp_state = None
    for place in range(max(count, len(pieces))):
        moved = []
        if place < count - 1:
            forward, backward = hop_step(forward, backward, place + 1, count)
            moved += [forward, backward]
        if 1 <= place < count:
            mlp_state = sum_step(mlp_state, mlp_slots, count - place, count)
            moved += mlp_state
        if place < len(pieces):
            query_piece, keys_piece, values_piece, mask_piece = head_inputs(*pieces[place])
            piece_grads[pieces[place]] = attend_backward(
                query_piece,
                keys_piece,
                values_piece,
                mask_piece,
                totals[pieces[place]],
                upstream_pieces[pieces[place]],
            )
        if place + 1 < len(pieces):
            following = pieces[place + 1]
            moved, piece_grads[pieces[place]], upstream_pieces[following] = tied(
                moved, piece_grads[pieces[place]], upstream_pieces[following]
            )
        elif place < len(pieces):
            moved, piece_grads[pieces[place]] = tied(moved, piece_grads[pieces[place]])
        if place < count - 1:
            forward, backward, *moved = moved
            arrived[-place - 1], arrived[place + 1] = (forward, backward)
        if 1 <= place < count:
            mlp_state = tuple(moved)
    mlp_share = sum_end(mlp_state, mlp_slots)
    result_share = (hidden_share + branch_scale * mlp_share).astype(jnp.bfloat16)
    grad_attn = jnp.concatenate(slots_from(arrived), axis=0)
    grad_out = jnp.einsum(
        "rq,rd->dq", slot_order(mixed_heads), grad_attn, preferred_element_type=jnp.float32
    )
    query_grad_rows = jnp.concatenate(
        [
            jnp.concatenate([piece_grads[head, True][0], piece_grads[head, False][0]], axis=0)
            for head in range(kv_heads)
        ],
        axis=1,
    )
    prompt_pairs_grad = jnp.concatenate(
        [
            piece_grads[head, True][which] + piece_grads[head, False][which][:prompt_total]
            for which in (1, 2)
            for head in range(kv_heads)
        ],
        axis=1,
    )
    grad_key_cont, grad_value_cont = (
        jnp.concatenate([piece_grads[head, False][which] for head in range(kv_heads)], axis=1)
        for which in (1, 2)
    )
    other_pairs = lax.ppermute(
        lax.dynamic_slice_in_dim(prompt_pairs_grad, (1 - ctx_index) * own_rows, own_rows, 0),
        "ctx",
        [(0, 1), (1, 0)],
    )
    pair_grads = other_pairs + lax.dynamic_slice_in_dim(
        prompt_pairs_grad, ctx_index * own_rows, own_rows, 0
    )
    key_grad_rows = jnp.concatenate(
        [pair_grads[:, :key_width], grad_key_cont[prompt_total:]], axis=0
    )
    value_grad_rows = jnp.concatenate(
        [pair_grads[:, key_width:], grad_value_cont[prompt_total:]], axis=0
    )
    grad_query_lin = rotate(query_grad_rows, cos_table, -sin_table).astype(jnp.bfloat16)
    grad_key_lin = rotate(key_grad_rows, cos_table, -sin_table).astype(jnp.bfloat16)
    grad_value_lin = value_grad_rows.astype(jnp.bfloat16)
    grad_query = jnp.einsum("rd,rq->dq", act_a, grad_query_lin, preferred_element_type=jnp.float32)
    grad_key = jnp.einsum("rd,rq->dq", act_a, grad_key_lin, preferred_element_type=jnp.float32)
    grad_value = jnp.einsum("rd,rq->dq", act_a, grad_value_lin, preferred_element_type=jnp.float32)
    input_grad = (
        jnp.einsum("rq,dq->rd", grad_query_lin, w_query, preferred_element_type=jnp.float32)
        + jnp.einsum("rq,dq->rd", grad_key_lin, key_weight, preferred_element_type=jnp.float32)
        + jnp.einsum("rq,dq->rd", grad_value_lin, value_weight, preferred_element_type=jnp.float32)
    )
    input_part = input_grad.astype(jnp.bfloat16)

    def row_part(distance):
        place = jnp.clip(me + distance, 0, count - 1) * share_rows
        return lax.dynamic_slice_in_dim(input_part, place, share_rows, 0)

    state = None
    forward, backward = hop_step(result_share, result_share, 1, count)
    forward, backward, input_part, gate_sum, up_sum = tied(
        forward, backward, input_part, gate_sum, up_sum
    )
    result_arrived = {0: result_share, -1: forward, 1: backward}
    for distance in range(count - 1, 0, -1):
        state = sum_step(state, row_part, distance, count)
        step = count - distance + 1
        if step < count:
            forward, backward = hop_step(forward, backward, step, count)
            state, forward, backward, down_sum = tied(state, forward, backward, down_sum)
            result_arrived[-step], result_arrived[step] = (forward, backward)
    input_grad_share = sum_end(state, row_part)

    def rows_from(arrived):
        chunks = [picked(me, arrived, {i: c - i for i in range(count)}) for c in range(count)]
        gathered = jnp.concatenate(chunks, axis=0)
        return (
            gathered[:own_rows][None],
            gathered[own_rows:].reshape(1, cont_count, CONT_LENGTH, width),
        )

    prompt_out, cont_out = rows_from(result_arrived)
    through_attn, gain_attn_part = norm_back(input_share, gain_attn, input_grad_share)
    grad_share = (res_share + through_attn).astype(jnp.bfloat16)
    forward, backward = (grad_share, grad_share)
    arrived = {0: grad_share}
    gain_parts = jnp.stack([gain_attn_part, gain_mlp_part])
    stages = pair_stages()
    per_hop = -(-len(stages) // (count - 1))
    for step in range(1, count):
        forward, backward = hop_step(forward, backward, step, count)
        for axis, distance in stages[(step - 1) * per_hop : step * per_hop]:
            gain_parts = pair_sum(gain_parts, axis, distance)
        forward, backward, gain_parts = tied(forward, backward, gain_parts)
        arrived[-step], arrived[step] = (forward, backward)
    prompt_grad, cont_grad = rows_from(arrived)
    gain_rows = width // (lax.axis_size("dp") * lax.axis_size("ctx"))
    gain_place = (lax.axis_index("dp") * lax.axis_size("ctx") + ctx_index) * gain_rows
    gain_own = lax.dynamic_slice_in_dim(gain_parts, gain_place, gain_rows, 1)
    attn_sum = lax.psum_scatter(
        jnp.concatenate([grad_query, grad_key, grad_value, grad_out], axis=1).astype(jnp.bfloat16),
        ("dp", "ctx"),
        scatter_dimension=0,
        tiled=True,
    ).astype(jnp.float32)
    qw = grad_query.shape[1]
    summed = (
        gain_own[0],
        attn_sum[:, :qw],
        attn_sum[:, qw : qw + key_width],
        attn_sum[:, qw + key_width : qw + 2 * key_width],
        attn_sum[:, qw + 2 * key_width :].T,
        gain_own[1],
        gate_sum.astype(jnp.float32),
        up_sum.astype(jnp.float32),
        down_sum.astype(jnp.float32).T,
    )
    return (
        prompt_out,
        cont_out,
        prompt_grad,
        cont_grad,
        summed[0],
        summed[1],
        summed[2],
        summed[3],
        summed[4],
        summed[5],
        summed[6],
        summed[7],
        summed[8],
    )


def solution(mesh):
    in_specs = (
        P("dp", "ctx", None),
        P("dp", "ctx", None, None),
        P("dp"),
        P(),
        P(None, "tensor"),
        P(None, "tensor"),
        P(None, "tensor"),
        P("tensor", None),
        P(),
        P(None, "tensor"),
        P(None, "tensor"),
        P("tensor", None),
        P("dp", "ctx", None),
        P("dp", "ctx", None, None),
    )
    out_specs = (
        P("dp", "ctx", None),
        P("dp", "ctx", None, None),
        P("dp", "ctx", None),
        P("dp", "ctx", None, None),
        P(("dp", "ctx")),
        P(("dp", "ctx"), "tensor"),
        P(("dp", "ctx"), "tensor"),
        P(("dp", "ctx"), "tensor"),
        P("tensor", ("dp", "ctx")),
        P(("dp", "ctx")),
        P(("dp", "ctx"), "tensor"),
        P(("dp", "ctx"), "tensor"),
        P("tensor", ("dp", "ctx")),
    )
    return jax.shard_map(shards, mesh=mesh, in_specs=in_specs, out_specs=out_specs, check_vma=False)
```

```python
import functools
import math
import operator

import jax
import jax.numpy as jnp
from jax import lax
from jax.experimental import pallas as pl
from jax.experimental.pallas import tpu as pltpu
from jax.sharding import PartitionSpec as P

QUERY_HEADS = 32
KEY_VALUE_HEADS = 8
HEAD_WIDTH = 64
CONT_LENGTH = 128


norm_eps = 1e-05
rope_base = 10000000.0
score_scale = 0.015625
branch_scale = 0.22
masked_score = -1e30


def norm_rows(inputs, weight):
    return inputs * lax.rsqrt(jnp.mean(inputs * inputs, axis=-1, keepdims=True) + norm_eps) * weight


def norm_back(inputs, weight, upstream):
    factor = lax.rsqrt(jnp.mean(inputs * inputs, axis=-1, keepdims=True) + norm_eps)
    scaled = inputs * factor
    weighted = upstream * weight
    through = factor * (weighted - scaled * jnp.mean(weighted * scaled, axis=-1, keepdims=True))
    return (through, jnp.sum(upstream * scaled, axis=0))


def angle_tables(position):
    freq = jnp.exp(
        jnp.arange(HEAD_WIDTH // 2, dtype=jnp.float32) * (-2.0 * math.log(rope_base) / HEAD_WIDTH)
    )
    angle = position.astype(jnp.float32)[:, None] * freq[None, :]
    return (jnp.cos(angle), jnp.sin(angle))


def rotate(inputs, cos_table, sin_table):
    rows = inputs.shape[1]
    halves = inputs.reshape(-1, 2, HEAD_WIDTH // 2, rows)
    first_half = halves[:, 0]
    second_half = halves[:, 1]
    turned = jnp.stack(
        [
            first_half * cos_table[None] - second_half * sin_table[None],
            second_half * cos_table[None] + first_half * sin_table[None],
        ],
        axis=1,
    )
    return turned.reshape(inputs.shape)


HEAD_GROUP = QUERY_HEADS // KEY_VALUE_HEADS
BLOCK = CONT_LENGTH


def lanes_from_heads(block):
    return jnp.concatenate(
        [block[g * HEAD_WIDTH : (g + 1) * HEAD_WIDTH] for g in range(HEAD_GROUP)], axis=1
    )


def heads_from_lanes(block):
    return jnp.concatenate(
        [block[:, g * BLOCK : (g + 1) * BLOCK] for g in range(HEAD_GROUP)], axis=0
    )


def inner(first, second):
    return jnp.dot(first, second, preferred_element_type=jnp.float32)


def across(first, second):
    return lax.dot_general(
        first, second, (((1,), (1,)), ((), ())), preferred_element_type=jnp.float32
    )


def scaled_queries(query_ref):
    return lanes_from_heads(query_ref[...].astype(jnp.float32) * score_scale).astype(jnp.bfloat16)


def block_scores(meta_ref, keys, own_keys, queries):
    lanes = HEAD_GROUP * BLOCK
    scores = inner(keys, queries)
    place = lax.broadcasted_iota(jnp.int32, scores.shape, 0)
    if own_keys is None:
        row = lax.broadcasted_iota(jnp.int32, (1, lanes), 1) % BLOCK
        limit = jnp.minimum(row + (meta_ref[1] + pl.program_id(0) * BLOCK + 1), meta_ref[0])
        return [jnp.where(place < limit, scores, masked_score)]
    own = inner(own_keys, queries)
    own_place = lax.broadcasted_iota(jnp.int32, own.shape, 0)
    own_row = lax.broadcasted_iota(jnp.int32, own.shape, 1) % BLOCK
    return [
        jnp.where(place < meta_ref[0], scores, masked_score),
        jnp.where(own_place <= own_row, own, masked_score),
    ]


def forward_kernel(meta_ref, query_ref, *refs):
    *key_refs, mixed_ref, total_ref = refs
    keys, values_t = key_refs[:2]
    own_keys, own_values_t = key_refs[2:] if len(key_refs) > 2 else (None, None)
    queries = scaled_queries(query_ref)
    parts = block_scores(
        meta_ref, keys[...], None if own_keys is None else own_keys[...], queries
    )
    highest = functools.reduce(
        jnp.maximum, [jnp.max(part, axis=0, keepdims=True) for part in parts]
    )
    weights = [jnp.exp(part - highest) for part in parts]
    total = sum(jnp.sum(weight, axis=0, keepdims=True) for weight in weights)
    mixed = sum(
        inner(ref[...], weight.astype(jnp.bfloat16))
        for ref, weight in zip((values_t, own_values_t), weights)
    )
    mixed_ref[...] = heads_from_lanes(mixed * (1.0 / total)).astype(jnp.bfloat16)
    total_ref[0] = highest + jnp.log(total)


def backward_kernel(meta_ref, query_ref, grad_ref, total_ref, *refs):
    own = len(refs) > 6
    keys, keys_t, values = refs[:3]
    own_keys, own_keys_t, own_values = refs[3:6] if own else (None, None, None)
    query_out, key_out, value_out, *own_out = refs[6:] if own else refs[3:]
    queries = scaled_queries(query_ref)
    grads = lanes_from_heads(grad_ref[...].astype(jnp.float32)).astype(jnp.bfloat16)
    parts = block_scores(meta_ref, keys[...], own_keys[...] if own else None, queries)
    weights = [jnp.exp(part - total_ref[0]) for part in parts]
    grad_weights = [inner(ref[...], grads) for ref, _ in zip((values, own_values), parts)]
    mean = sum(
        jnp.sum(weight * grad, axis=0, keepdims=True)
        for weight, grad in zip(weights, grad_weights)
    )
    grad_scores = [
        (weight * (grad - mean)).astype(jnp.bfloat16)
        for weight, grad in zip(weights, grad_weights)
    ]
    query_grad = sum(inner(ref[...], part) for ref, part in zip((keys_t, own_keys_t), grad_scores))
    query_out[...] = heads_from_lanes(query_grad * score_scale)

    @pl.when(pl.program_id(0) == 0)
    def _():
        key_out[...] = jnp.zeros_like(key_out)
        value_out[...] = jnp.zeros_like(value_out)

    key_out[...] += across(grad_scores[0], queries)
    value_out[...] += across(weights[0].astype(jnp.bfloat16), grads)
    if own:
        own_out[0][...] = across(grad_scores[1], queries)
        own_out[1][...] = across(weights[1].astype(jnp.bfloat16), grads)


def attention_call(kernel, meta, moving, keys, own, outs, products):
    rows = moving[0].shape[1]
    lanes = HEAD_GROUP * BLOCK
    tall = HEAD_GROUP * HEAD_WIDTH
    kinds = {
        "rows": pl.BlockSpec((tall, BLOCK), lambda i, meta: (0, i)),
        "total": pl.BlockSpec((1, 1, lanes), lambda i, meta: (i, 0, 0)),
        "own": pl.BlockSpec((BLOCK, HEAD_WIDTH), lambda i, meta: (i, 0)),
        "own_t": pl.BlockSpec((HEAD_WIDTH, BLOCK), lambda i, meta: (0, i)),
    }

    def whole(shape):
        return pl.BlockSpec(shape, lambda i, meta: (0, 0))

    in_specs = [kinds["total"] if array.ndim == 3 else kinds["rows"] for array in moving]
    in_specs += [whole(array.shape) for array in keys]
    in_specs += [kinds["own" if array.shape[1] == HEAD_WIDTH else "own_t"] for array in own]
    out_specs = [
        whole(out.shape) if kind == "whole" else kinds[kind] for kind, out in outs
    ]
    key_total = keys[0].shape[0] + (BLOCK if own else 0)
    work = HEAD_GROUP * rows * key_total
    return pl.pallas_call(
        kernel,
        out_shape=[out for _, out in outs],
        grid_spec=pltpu.PrefetchScalarGridSpec(
            num_scalar_prefetch=1,
            grid=(rows // BLOCK,),
            in_specs=in_specs,
            out_specs=out_specs,
        ),
        compiler_params=pltpu.CompilerParams(
            dimension_semantics=("arbitrary",), vmem_limit_bytes=40 * 1024 * 1024
        ),
        cost_estimate=pl.CostEstimate(
            flops=2 * products * work * HEAD_WIDTH,
            bytes_accessed=2 * (sum(array.size for array in moving) + 4 * keys[0].size),
            transcendentals=work,
        ),
    )(meta, *moving, *keys, *own)


def attend_forward(meta, queries, keys, values, own_keys, own_values):
    rows = queries.shape[1]
    own = [] if own_keys is None else [own_keys, own_values.T]
    return attention_call(
        forward_kernel,
        meta,
        [queries],
        [keys, values.T],
        own,
        [
            ("rows", jax.ShapeDtypeStruct(queries.shape, jnp.bfloat16)),
            (
                "total",
                jax.ShapeDtypeStruct((rows // BLOCK, 1, HEAD_GROUP * BLOCK), jnp.float32),
            ),
        ],
        2,
    )


def attend_backward(meta, queries, keys, values, own_keys, own_values, totals, upstream):
    own = [] if own_keys is None else [own_keys, own_keys.T, own_values]
    key_shape = jax.ShapeDtypeStruct(keys.shape, jnp.float32)
    outs = [("rows", jax.ShapeDtypeStruct(queries.shape, jnp.float32))]
    outs += [("whole", key_shape), ("whole", key_shape)]
    if own:
        outs += [("own", jax.ShapeDtypeStruct(own_keys.shape, jnp.float32))] * 2
    return attention_call(
        backward_kernel,
        meta,
        [queries, upstream, totals],
        [keys, keys.T, values],
        own,
        outs,
        5,
    )


def picked(me, arrays, keys):
    out = None
    for key in dict.fromkeys(keys.values()):
        if out is None:
            out = arrays[key]
        else:
            chosen = functools.reduce(
                operator.or_, [me == device for device, held in keys.items() if held == key]
            )
            out = jnp.where(chosen, arrays[key], out)
    return out


def slot_tables(count):
    chunk_of = []
    for device in range(count):
        near = min(device, count - 1 - device)
        far = 1 if device < count - 1 - device else -1
        order = [device]
        for slot in range(1, count):
            if slot <= 2 * near:
                distance = (slot + 1) // 2
                order.append(device - distance if slot % 2 else device + distance)
            else:
                order.append(device + far * (slot - near))
        chunk_of.append(order)
    return chunk_of


def hop_step(forward, backward, step, count):
    return (
        lax.ppermute(forward, "tensor", [(i, i + 1) for i in range(step - 1, count - 1)]),
        lax.ppermute(backward, "tensor", [(i, i - 1) for i in range(1, count - step + 1)]),
    )


def added(first, second):
    return (first.astype(jnp.float32) + second.astype(jnp.float32)).astype(jnp.bfloat16)


def sum_step(state, part_at, distance, count):
    to_right = part_at(distance)
    to_left = part_at(-distance)
    if state is not None:
        to_right = added(to_right, state[0])
        to_left = added(to_left, state[1])
    return (
        lax.ppermute(to_right, "tensor", [(i, i + 1) for i in range(0, count - distance)]),
        lax.ppermute(to_left, "tensor", [(i, i - 1) for i in range(distance, count)]),
    )


def sum_end(state, part_at):
    return sum(part.astype(jnp.float32) for part in (part_at(0), *state))


def tied(*values):
    return lax.optimization_barrier(values)


def exchanged(me, send_block, count):
    received = {0: send_block(me)}
    for shift in range(1, count):
        received[shift] = lax.ppermute(
            send_block(lax.rem(me + shift, count)),
            "tensor",
            [(i, (i + shift) % count) for i in range(count)],
        )
    return [
        picked(me, received, {i: (i - source) % count for i in range(count)})
        for source in range(count)
    ]


def pair_stages():
    return [
        (axis, 1 << bit)
        for axis in ("ctx", "tensor", "dp")
        for bit in range(lax.axis_size(axis).bit_length() - 1)
    ]


def pair_sum(values, axis, distance):
    return values + lax.ppermute(
        values, axis, [(i, i ^ distance) for i in range(lax.axis_size(axis))]
    )


def shards(
    prompt_in,
    cont_in,
    prompt_len,
    norm_attn,
    w_query,
    key_weight,
    value_weight,
    w_out,
    norm_mlp,
    w_gate,
    w_up,
    w_down,
    prompt_cot,
    cont_cot,
):
    own_rows = prompt_in.shape[1]
    cont_count = cont_in.shape[1]
    width = prompt_in.shape[2]
    cont_rows = cont_count * CONT_LENGTH
    total_rows = own_rows + cont_rows
    key_width = key_weight.shape[1]
    ctx_index = lax.axis_index("ctx")
    count = lax.axis_size("tensor")
    me = lax.axis_index("tensor")
    share_rows = total_rows // count
    share_start = me * share_rows
    head_half = w_out.shape[0] // 2
    kv_heads = key_weight.shape[1] // HEAD_WIDTH
    group_width = w_out.shape[0] // kv_heads
    order = slot_tables(count)
    slot_chunks = [
        picked(me, {i: jnp.int32(i) for i in range(count)}, {i: order[i][s] for i in range(count)})
        for s in range(count)
    ]
    slot_of = [[order[i].index(c) for c in range(count)] for i in range(count)]
    token_length = prompt_len[0]
    gain_attn = norm_attn.astype(jnp.float32)
    gain_mlp = norm_mlp.astype(jnp.float32)

    def share_of(values):
        return lax.dynamic_slice_in_dim(values, share_start, share_rows, 0)

    def slot_order(values):
        return jnp.concatenate(
            [
                lax.dynamic_slice_in_dim(values, slot_chunks[s] * share_rows, share_rows, 0)
                for s in range(count)
            ],
            axis=0,
        )

    def slots_from(arrived):
        return [
            picked(me, arrived, {i: order[i][s] - i for i in range(count)}) for s in range(count)
        ]

    def slot_part(parts):
        return lambda distance: picked(
            me,
            parts,
            {i: slot_of[i][i + distance] for i in range(count) if 0 <= i + distance < count},
        )

    own_out_half = lax.dynamic_slice_in_dim(w_out, ctx_index * head_half, head_half, 0)
    full_out = lax.all_gather(own_out_half, ("tensor", "ctx"), axis=0, tiled=True)
    all_rows = jnp.concatenate([prompt_in[0], cont_in[0].reshape(cont_rows, width)], axis=0).astype(
        jnp.float32
    )
    input_share = share_of(all_rows)
    within = jnp.arange(cont_rows, dtype=jnp.int32) % CONT_LENGTH
    positions = jnp.concatenate(
        [ctx_index * own_rows + jnp.arange(own_rows, dtype=jnp.int32), token_length + within]
    )
    cos_table, sin_table = (table.T for table in angle_tables(positions))
    act_a = norm_rows(all_rows, gain_attn).astype(jnp.bfloat16)
    query_rows = rotate(
        jnp.einsum("rd,dq->qr", act_a, w_query, preferred_element_type=jnp.float32),
        cos_table,
        sin_table,
    ).astype(jnp.bfloat16)
    joined_keys = (
        rotate(
            jnp.einsum("rd,dq->qr", act_a, key_weight, preferred_element_type=jnp.float32),
            cos_table,
            sin_table,
        )
        .astype(jnp.bfloat16)
        .T
    )
    joined_values = jnp.dot(act_a, value_weight, preferred_element_type=jnp.float32).astype(
        jnp.bfloat16
    )
    local_pairs = jnp.concatenate([joined_keys[:own_rows], joined_values[:own_rows]], axis=1)
    prompt_pairs = lax.all_gather(local_pairs, "ctx", axis=0, tiled=True)
    shared_prompt_keys = prompt_pairs[:, :key_width]
    shared_prompt_values = prompt_pairs[:, key_width:]
    meta = jnp.stack([token_length, ctx_index * own_rows]).astype(jnp.int32)

    def head_inputs(head, prompt):
        wide = slice(head * group_width, (head + 1) * group_width)
        thin = slice(head * HEAD_WIDTH, (head + 1) * HEAD_WIDTH)
        shared = (shared_prompt_keys[:, thin], shared_prompt_values[:, thin])
        if prompt:
            return (meta, query_rows[wide, :own_rows], *shared, None, None)
        return (
            meta,
            query_rows[wide, own_rows:],
            *shared,
            joined_keys[own_rows:, thin],
            joined_values[own_rows:, thin],
        )

    mixed_list = []
    totals = {}
    share_list = []
    for head in range(kv_heads):
        mixed_prompt, totals[head, True] = attend_forward(*head_inputs(head, True))
        mixed_cont, totals[head, False] = attend_forward(*head_inputs(head, False))
        mixed = jnp.concatenate([mixed_prompt, mixed_cont], axis=1).T
        mixed_list.append(mixed)
        share_list.append(
            exchanged(
                me,
                lambda target: lax.dynamic_slice_in_dim(mixed, target * share_rows, share_rows, 0),
                count,
            )
        )
    upstream = jnp.concatenate([prompt_cot[0], cont_cot[0].reshape(cont_rows, width)], axis=0)
    grad_mlp = slot_order((branch_scale * upstream.astype(jnp.float32)).astype(jnp.bfloat16))
    mixed_list[-1], grad_mlp = tied(mixed_list[-1], grad_mlp)
    grad_hidden = jnp.einsum("rd,fd->rf", grad_mlp, w_down, preferred_element_type=jnp.float32)
    share_list[-1], grad_hidden = tied(share_list[-1], grad_hidden)
    mixed_heads = jnp.concatenate(mixed_list, axis=1)
    mixed_share = jnp.concatenate(
        [share_list[head][source] for source in range(count) for head in range(kv_heads)], axis=1
    )
    attn_share = jnp.dot(mixed_share, full_out, preferred_element_type=jnp.float32)
    hidden_share = input_share + branch_scale * attn_share
    act_b_share = norm_rows(hidden_share, gain_mlp).astype(jnp.bfloat16)
    forward, backward = (act_b_share, act_b_share)
    arrived = {0: act_b_share}
    act_b_slots = []
    hidden_list, gate_list, up_list, part_list = ([], [], [], [])
    for s in range(count):
        act_b_slots.append(
            picked(me, arrived, {i: order[i][s] - i for i in range(count)})
        )
        if s + 1 < count:
            forward, backward = hop_step(forward, backward, s + 1, count)
        gate_proj = jnp.dot(act_b_slots[s], w_gate, preferred_element_type=jnp.float32)
        up_proj = jnp.dot(act_b_slots[s], w_up, preferred_element_type=jnp.float32)
        sigmoid_gate = jax.nn.sigmoid(gate_proj)
        silu_gate = gate_proj * sigmoid_gate
        grad_slot = grad_hidden[s * share_rows : (s + 1) * share_rows]
        hidden = (silu_gate * up_proj).astype(jnp.bfloat16)
        grad_gate_slot = (
            grad_slot * up_proj * sigmoid_gate * (1.0 + gate_proj * (1.0 - sigmoid_gate))
        ).astype(jnp.bfloat16)
        grad_up_slot = (grad_slot * silu_gate).astype(jnp.bfloat16)
        part = (
            jnp.einsum("rf,df->rd", grad_gate_slot, w_gate, preferred_element_type=jnp.float32)
            + jnp.einsum("rf,df->rd", grad_up_slot, w_up, preferred_element_type=jnp.float32)
        ).astype(jnp.bfloat16)
        forward, backward, hidden, grad_gate_slot, grad_up_slot, part = tied(
            forward, backward, hidden, grad_gate_slot, grad_up_slot, part
        )
        arrived[-s - 1], arrived[s + 1] = (forward, backward)
        hidden_list.append(hidden)
        gate_list.append(grad_gate_slot)
        up_list.append(grad_up_slot)
        part_list.append(part)
    act_b = jnp.concatenate(act_b_slots, axis=0)
    hidden_act = jnp.concatenate(hidden_list, axis=0)
    grad_gate_act = jnp.concatenate(gate_list, axis=0)
    grad_up_act = jnp.concatenate(up_list, axis=0)

    def over_tokens(values):
        return lax.psum_scatter(
            values.astype(jnp.bfloat16), ("dp", "ctx"), scatter_dimension=0, tiled=True
        )

    fillers = [
        lambda: jnp.einsum("rd,rf->df", act_b, grad_gate_act, preferred_element_type=jnp.float32),
        lambda: jnp.einsum("rd,rf->df", act_b, grad_up_act, preferred_element_type=jnp.float32),
        lambda: jnp.einsum("rf,rd->df", hidden_act, grad_mlp, preferred_element_type=jnp.float32),
    ]
    filled = []
    state = None
    for distance in range(count - 1, 0, -1):
        state = sum_step(state, slot_part(part_list), distance, count)
        if fillers:
            filled.append(fillers.pop(0)().astype(jnp.bfloat16))
            state, filled[-1] = tied(state, filled[-1])
    filled.extend(filler().astype(jnp.bfloat16) for filler in fillers)
    gate_sum, up_sum, down_sum = (over_tokens(product) for product in filled)
    normed_share = sum_end(state, slot_part(part_list))
    through_mlp, gain_mlp_part = norm_back(hidden_share, gain_mlp, normed_share)
    res_share = share_of(upstream).astype(jnp.float32) + through_mlp
    grad_attn_share = (branch_scale * res_share).astype(jnp.bfloat16)
    mixed_grad = jnp.einsum(
        "rd,qd->rq", grad_attn_share, full_out, preferred_element_type=jnp.float32
    ).astype(jnp.bfloat16)
    grad_mixed = jnp.concatenate(
        exchanged(
            me,
            lambda target: lax.dynamic_slice_in_dim(
                mixed_grad, target * w_out.shape[0], w_out.shape[0], 1
            ),
            count,
        ),
        axis=0,
    )
    hidden_act, mixed_grad = tied(hidden_act, mixed_grad)
    mlp_part = jnp.dot(hidden_act, w_down, preferred_element_type=jnp.float32).astype(jnp.bfloat16)
    grad_mixed, mlp_part = tied(grad_mixed, mlp_part)
    mlp_parts = [mlp_part[s * share_rows : (s + 1) * share_rows] for s in range(count)]
    pieces = [(head, prompt) for head in range(kv_heads) for prompt in (True, False)]
    upstream_pieces = {
        (head, prompt): grad_mixed[
            (slice(0, own_rows) if prompt else slice(own_rows, total_rows)),
            head * group_width : (head + 1) * group_width,
        ].T
        for head, prompt in pieces
    }
    piece_grads = {}
    upstream_pieces[pieces[0]], gather_start = tied(upstream_pieces[pieces[0]], grad_attn_share)
    arrived = {0: grad_attn_share}
    forward, backward = (gather_start, gather_start)
    mlp_state = None
    for place in range(max(count, len(pieces))):
        moved = []
        if place < count - 1:
            forward, backward = hop_step(forward, backward, place + 1, count)
            moved += [forward, backward]
        if 1 <= place < count:
            mlp_state = sum_step(mlp_state, slot_part(mlp_parts), count - place, count)
            moved += mlp_state
        if place < len(pieces):
            piece_grads[pieces[place]] = attend_backward(
                *head_inputs(*pieces[place]), totals[pieces[place]], upstream_pieces[pieces[place]]
            )
        if place + 1 < len(pieces):
            following = pieces[place + 1]
            moved, piece_grads[pieces[place]], upstream_pieces[following], mlp_parts = tied(
                moved, piece_grads[pieces[place]], upstream_pieces[following], mlp_parts
            )
        elif place < len(pieces):
            moved, piece_grads[pieces[place]] = tied(moved, piece_grads[pieces[place]])
        if place < count - 1:
            forward, backward, *moved = moved
            arrived[-place - 1], arrived[place + 1] = (forward, backward)
        if 1 <= place < count:
            mlp_state = tuple(moved)
    mlp_share = sum_end(mlp_state, slot_part(mlp_parts))
    result_share = (hidden_share + branch_scale * mlp_share).astype(jnp.bfloat16)
    grad_attn = jnp.concatenate(slots_from(arrived), axis=0)
    grad_out = jnp.einsum(
        "rq,rd->dq", slot_order(mixed_heads), grad_attn, preferred_element_type=jnp.float32
    )
    query_grad_rows = jnp.concatenate(
        [
            jnp.concatenate([piece_grads[head, True][0], piece_grads[head, False][0]], axis=1)
            for head in range(kv_heads)
        ],
        axis=0,
    )
    prompt_pairs_grad = jnp.concatenate(
        [
            piece_grads[head, True][which] + piece_grads[head, False][which]
            for which in (1, 2)
            for head in range(kv_heads)
        ],
        axis=1,
    )
    grad_key_cont, grad_value_cont = (
        jnp.concatenate([piece_grads[head, False][which] for head in range(kv_heads)], axis=1)
        for which in (3, 4)
    )
    other_pairs = lax.ppermute(
        lax.dynamic_slice_in_dim(prompt_pairs_grad, (1 - ctx_index) * own_rows, own_rows, 0),
        "ctx",
        [(0, 1), (1, 0)],
    )
    pair_grads = other_pairs + lax.dynamic_slice_in_dim(
        prompt_pairs_grad, ctx_index * own_rows, own_rows, 0
    )
    key_grad_rows = jnp.concatenate(
        [pair_grads[:, :key_width], grad_key_cont], axis=0
    )
    value_grad_rows = jnp.concatenate(
        [pair_grads[:, key_width:], grad_value_cont], axis=0
    )
    grad_query_lin = rotate(query_grad_rows, cos_table, -sin_table).astype(jnp.bfloat16)
    grad_key_lin = rotate(key_grad_rows.T, cos_table, -sin_table).astype(jnp.bfloat16)
    grad_value_lin = value_grad_rows.astype(jnp.bfloat16)
    grad_query = jnp.einsum("rd,qr->dq", act_a, grad_query_lin, preferred_element_type=jnp.float32)
    grad_key = jnp.einsum("rd,qr->dq", act_a, grad_key_lin, preferred_element_type=jnp.float32)
    grad_value = jnp.einsum("rd,rq->dq", act_a, grad_value_lin, preferred_element_type=jnp.float32)
    input_grad = (
        jnp.einsum("qr,dq->rd", grad_query_lin, w_query, preferred_element_type=jnp.float32)
        + jnp.einsum("qr,dq->rd", grad_key_lin, key_weight, preferred_element_type=jnp.float32)
        + jnp.einsum("rq,dq->rd", grad_value_lin, value_weight, preferred_element_type=jnp.float32)
    )
    input_part = input_grad.astype(jnp.bfloat16)

    def row_part(distance):
        place = jnp.clip(me + distance, 0, count - 1) * share_rows
        return lax.dynamic_slice_in_dim(input_part, place, share_rows, 0)

    state = None
    forward, backward = hop_step(result_share, result_share, 1, count)
    forward, backward, input_part, gate_sum, up_sum = tied(
        forward, backward, input_part, gate_sum, up_sum
    )
    result_arrived = {0: result_share, -1: forward, 1: backward}
    for distance in range(count - 1, 0, -1):
        state = sum_step(state, row_part, distance, count)
        step = count - distance + 1
        if step < count:
            forward, backward = hop_step(forward, backward, step, count)
            state, forward, backward, down_sum = tied(state, forward, backward, down_sum)
            result_arrived[-step], result_arrived[step] = (forward, backward)
    input_grad_share = sum_end(state, row_part)

    def rows_from(arrived):
        chunks = [picked(me, arrived, {i: c - i for i in range(count)}) for c in range(count)]
        gathered = jnp.concatenate(chunks, axis=0)
        return (
            gathered[:own_rows][None],
            gathered[own_rows:].reshape(1, cont_count, CONT_LENGTH, width),
        )

    prompt_out, cont_out = rows_from(result_arrived)
    through_attn, gain_attn_part = norm_back(input_share, gain_attn, input_grad_share)
    grad_share = (res_share + through_attn).astype(jnp.bfloat16)
    forward, backward = (grad_share, grad_share)
    arrived = {0: grad_share}
    gain_parts = jnp.stack([gain_attn_part, gain_mlp_part])
    stages = pair_stages()
    per_hop = -(-len(stages) // (count - 1))
    for step in range(1, count):
        forward, backward = hop_step(forward, backward, step, count)
        for axis, distance in stages[(step - 1) * per_hop : step * per_hop]:
            gain_parts = pair_sum(gain_parts, axis, distance)
        forward, backward, gain_parts = tied(forward, backward, gain_parts)
        arrived[-step], arrived[step] = (forward, backward)
    prompt_grad, cont_grad = rows_from(arrived)
    gain_rows = width // (lax.axis_size("dp") * lax.axis_size("ctx"))
    gain_place = (lax.axis_index("dp") * lax.axis_size("ctx") + ctx_index) * gain_rows
    gain_own = lax.dynamic_slice_in_dim(gain_parts, gain_place, gain_rows, 1)
    attn_sum = lax.psum_scatter(
        jnp.concatenate([grad_query, grad_key, grad_value, grad_out], axis=1).astype(jnp.bfloat16),
        ("dp", "ctx"),
        scatter_dimension=0,
        tiled=True,
    ).astype(jnp.float32)
    qw = grad_query.shape[1]
    summed = (
        gain_own[0],
        attn_sum[:, :qw],
        attn_sum[:, qw : qw + key_width],
        attn_sum[:, qw + key_width : qw + 2 * key_width],
        attn_sum[:, qw + 2 * key_width :].T,
        gain_own[1],
        gate_sum.astype(jnp.float32),
        up_sum.astype(jnp.float32),
        down_sum.astype(jnp.float32).T,
    )
    return (
        prompt_out,
        cont_out,
        prompt_grad,
        cont_grad,
        summed[0],
        summed[1],
        summed[2],
        summed[3],
        summed[4],
        summed[5],
        summed[6],
        summed[7],
        summed[8],
    )


def solution(mesh):
    in_specs = (
        P("dp", "ctx", None),
        P("dp", "ctx", None, None),
        P("dp"),
        P(),
        P(None, "tensor"),
        P(None, "tensor"),
        P(None, "tensor"),
        P("tensor", None),
        P(),
        P(None, "tensor"),
        P(None, "tensor"),
        P("tensor", None),
        P("dp", "ctx", None),
        P("dp", "ctx", None, None),
    )
    out_specs = (
        P("dp", "ctx", None),
        P("dp", "ctx", None, None),
        P("dp", "ctx", None),
        P("dp", "ctx", None, None),
        P(("dp", "ctx")),
        P(("dp", "ctx"), "tensor"),
        P(("dp", "ctx"), "tensor"),
        P(("dp", "ctx"), "tensor"),
        P("tensor", ("dp", "ctx")),
        P(("dp", "ctx")),
        P(("dp", "ctx"), "tensor"),
        P(("dp", "ctx"), "tensor"),
        P("tensor", ("dp", "ctx")),
    )
    return jax.shard_map(shards, mesh=mesh, in_specs=in_specs, out_specs=out_specs, check_vma=False)
```

```python
import functools
import math
import operator

import jax
import jax.numpy as jnp
from jax import lax
from jax.experimental import pallas as pl
from jax.experimental.pallas import tpu as pltpu
from jax.sharding import PartitionSpec as P

QUERY_HEADS = 32
KEY_VALUE_HEADS = 8
HEAD_WIDTH = 64
CONT_LENGTH = 128


norm_eps = 1e-05
rope_base = 10000000.0
score_scale = 0.015625
branch_scale = 0.22
masked_score = -1e30


def norm_rows(inputs, weight):
    return inputs * lax.rsqrt(jnp.mean(inputs * inputs, axis=-1, keepdims=True) + norm_eps) * weight


def norm_back(inputs, weight, upstream):
    factor = lax.rsqrt(jnp.mean(inputs * inputs, axis=-1, keepdims=True) + norm_eps)
    scaled = inputs * factor
    weighted = upstream * weight
    through = factor * (weighted - scaled * jnp.mean(weighted * scaled, axis=-1, keepdims=True))
    return (through, jnp.sum(upstream * scaled, axis=0))


def angle_tables(position):
    freq = jnp.exp(
        jnp.arange(HEAD_WIDTH // 2, dtype=jnp.float32) * (-2.0 * math.log(rope_base) / HEAD_WIDTH)
    )
    angle = position.astype(jnp.float32)[:, None] * freq[None, :]
    return (jnp.cos(angle), jnp.sin(angle))


def rotate(inputs, cos_table, sin_table):
    rows = inputs.shape[1]
    halves = inputs.reshape(-1, 2, HEAD_WIDTH // 2, rows)
    first_half = halves[:, 0]
    second_half = halves[:, 1]
    turned = jnp.stack(
        [
            first_half * cos_table[None] - second_half * sin_table[None],
            second_half * cos_table[None] + first_half * sin_table[None],
        ],
        axis=1,
    )
    return turned.reshape(inputs.shape)


HEAD_GROUP = QUERY_HEADS // KEY_VALUE_HEADS
BLOCK = CONT_LENGTH


def lanes_from_heads(block):
    return jnp.concatenate(
        [block[g * HEAD_WIDTH : (g + 1) * HEAD_WIDTH] for g in range(HEAD_GROUP)], axis=1
    )


def heads_from_lanes(block):
    return jnp.concatenate(
        [block[:, g * BLOCK : (g + 1) * BLOCK] for g in range(HEAD_GROUP)], axis=0
    )


def inner(first, second):
    return jnp.dot(first, second, preferred_element_type=jnp.float32)


def across(first, second):
    return lax.dot_general(
        first, second, (((1,), (1,)), ((), ())), preferred_element_type=jnp.float32
    )


def scaled_queries(query_ref):
    return lanes_from_heads(query_ref[...].astype(jnp.float32) * score_scale).astype(jnp.bfloat16)


def block_scores(meta_ref, keys, own_keys, queries):
    lanes = HEAD_GROUP * BLOCK
    scores = inner(keys, queries)
    place = lax.broadcasted_iota(jnp.int32, scores.shape, 0)
    if own_keys is None:
        row = lax.broadcasted_iota(jnp.int32, (1, lanes), 1) % BLOCK
        limit = jnp.minimum(row + (meta_ref[1] + pl.program_id(0) * BLOCK + 1), meta_ref[0])
        return [jnp.where(place < limit, scores, masked_score)]
    own = inner(own_keys, queries)
    own_place = lax.broadcasted_iota(jnp.int32, own.shape, 0)
    own_row = lax.broadcasted_iota(jnp.int32, own.shape, 1) % BLOCK
    return [
        jnp.where(place < meta_ref[0], scores, masked_score),
        jnp.where(own_place <= own_row, own, masked_score),
    ]


def forward_kernel(meta_ref, query_ref, *refs):
    *key_refs, mixed_ref, total_ref = refs
    keys, values_t = key_refs[:2]
    own_keys, own_values_t = key_refs[2:] if len(key_refs) > 2 else (None, None)
    queries = scaled_queries(query_ref)
    parts = block_scores(
        meta_ref, keys[...], None if own_keys is None else own_keys[...], queries
    )
    highest = functools.reduce(
        jnp.maximum, [jnp.max(part, axis=0, keepdims=True) for part in parts]
    )
    weights = [jnp.exp(part - highest) for part in parts]
    total = sum(jnp.sum(weight, axis=0, keepdims=True) for weight in weights)
    mixed = sum(
        inner(ref[...], weight.astype(jnp.bfloat16))
        for ref, weight in zip((values_t, own_values_t), weights)
    )
    mixed_ref[...] = heads_from_lanes(mixed * (1.0 / total)).astype(jnp.bfloat16)
    total_ref[0] = highest + jnp.log(total)


def backward_kernel(meta_ref, query_ref, grad_ref, total_ref, *refs):
    own = len(refs) > 6
    keys, keys_t, values = refs[:3]
    own_keys, own_keys_t, own_values = refs[3:6] if own else (None, None, None)
    query_out, key_out, value_out, *own_out = refs[6:] if own else refs[3:]
    queries = scaled_queries(query_ref)
    grads = lanes_from_heads(grad_ref[...].astype(jnp.float32)).astype(jnp.bfloat16)
    parts = block_scores(meta_ref, keys[...], own_keys[...] if own else None, queries)
    weights = [jnp.exp(part - total_ref[0]) for part in parts]
    grad_weights = [inner(ref[...], grads) for ref, _ in zip((values, own_values), parts)]
    mean = sum(
        jnp.sum(weight * grad, axis=0, keepdims=True)
        for weight, grad in zip(weights, grad_weights)
    )
    grad_scores = [
        (weight * (grad - mean)).astype(jnp.bfloat16)
        for weight, grad in zip(weights, grad_weights)
    ]
    query_grad = sum(inner(ref[...], part) for ref, part in zip((keys_t, own_keys_t), grad_scores))
    query_out[...] = heads_from_lanes(query_grad * score_scale)

    @pl.when(pl.program_id(0) == 0)
    def _():
        key_out[...] = jnp.zeros_like(key_out)
        value_out[...] = jnp.zeros_like(value_out)

    key_out[...] += across(grad_scores[0], queries)
    value_out[...] += across(weights[0].astype(jnp.bfloat16), grads)
    if own:
        own_out[0][...] = across(grad_scores[1], queries)
        own_out[1][...] = across(weights[1].astype(jnp.bfloat16), grads)


def attention_call(kernel, meta, moving, keys, own, outs, products):
    rows = moving[0].shape[1]
    lanes = HEAD_GROUP * BLOCK
    tall = HEAD_GROUP * HEAD_WIDTH
    kinds = {
        "rows": pl.BlockSpec((tall, BLOCK), lambda i, meta: (0, i)),
        "total": pl.BlockSpec((1, 1, lanes), lambda i, meta: (i, 0, 0)),
        "own": pl.BlockSpec((BLOCK, HEAD_WIDTH), lambda i, meta: (i, 0)),
        "own_t": pl.BlockSpec((HEAD_WIDTH, BLOCK), lambda i, meta: (0, i)),
    }

    def whole(shape):
        return pl.BlockSpec(shape, lambda i, meta: (0, 0))

    in_specs = [kinds["total"] if array.ndim == 3 else kinds["rows"] for array in moving]
    in_specs += [whole(array.shape) for array in keys]
    in_specs += [kinds["own" if array.shape[1] == HEAD_WIDTH else "own_t"] for array in own]
    out_specs = [
        whole(out.shape) if kind == "whole" else kinds[kind] for kind, out in outs
    ]
    key_total = keys[0].shape[0] + (BLOCK if own else 0)
    work = HEAD_GROUP * rows * key_total
    return pl.pallas_call(
        kernel,
        out_shape=[out for _, out in outs],
        grid_spec=pltpu.PrefetchScalarGridSpec(
            num_scalar_prefetch=1,
            grid=(rows // BLOCK,),
            in_specs=in_specs,
            out_specs=out_specs,
        ),
        compiler_params=pltpu.CompilerParams(
            dimension_semantics=("arbitrary",), vmem_limit_bytes=40 * 1024 * 1024
        ),
        cost_estimate=pl.CostEstimate(
            flops=2 * products * work * HEAD_WIDTH,
            bytes_accessed=2 * (sum(array.size for array in moving) + 4 * keys[0].size),
            transcendentals=work,
        ),
    )(meta, *moving, *keys, *own)


def attend_forward(meta, queries, keys, values, own_keys, own_values):
    rows = queries.shape[1]
    own = [] if own_keys is None else [own_keys, own_values.T]
    return attention_call(
        forward_kernel,
        meta,
        [queries],
        [keys, values.T],
        own,
        [
            ("rows", jax.ShapeDtypeStruct(queries.shape, jnp.bfloat16)),
            (
                "total",
                jax.ShapeDtypeStruct((rows // BLOCK, 1, HEAD_GROUP * BLOCK), jnp.float32),
            ),
        ],
        2,
    )


def attend_backward(meta, queries, keys, values, own_keys, own_values, totals, upstream):
    own = [] if own_keys is None else [own_keys, own_keys.T, own_values]
    key_shape = jax.ShapeDtypeStruct(keys.shape, jnp.float32)
    outs = [("rows", jax.ShapeDtypeStruct(queries.shape, jnp.float32))]
    outs += [("whole", key_shape), ("whole", key_shape)]
    if own:
        outs += [("own", jax.ShapeDtypeStruct(own_keys.shape, jnp.float32))] * 2
    return attention_call(
        backward_kernel,
        meta,
        [queries, upstream, totals],
        [keys, keys.T, values],
        own,
        outs,
        5,
    )


def picked(me, arrays, keys):
    out = None
    for key in dict.fromkeys(keys.values()):
        if out is None:
            out = arrays[key]
        else:
            chosen = functools.reduce(
                operator.or_, [me == device for device, held in keys.items() if held == key]
            )
            out = jnp.where(chosen, arrays[key], out)
    return out


def slot_tables(count):
    chunk_of = []
    for device in range(count):
        near = min(device, count - 1 - device)
        far = 1 if device < count - 1 - device else -1
        order = [device]
        for slot in range(1, count):
            if slot <= 2 * near:
                distance = (slot + 1) // 2
                order.append(device - distance if slot % 2 else device + distance)
            else:
                order.append(device + far * (slot - near))
        chunk_of.append(order)
    return chunk_of


def hop_step(forward, backward, step, count):
    return (
        lax.ppermute(forward, "tensor", [(i, i + 1) for i in range(step - 1, count - 1)]),
        lax.ppermute(backward, "tensor", [(i, i - 1) for i in range(1, count - step + 1)]),
    )


def added(first, second):
    return (first.astype(jnp.float32) + second.astype(jnp.float32)).astype(jnp.bfloat16)


def sum_step(state, part_at, distance, count):
    to_right = part_at(distance)
    to_left = part_at(-distance)
    if state is not None:
        to_right = added(to_right, state[0])
        to_left = added(to_left, state[1])
    return (
        lax.ppermute(to_right, "tensor", [(i, i + 1) for i in range(0, count - distance)]),
        lax.ppermute(to_left, "tensor", [(i, i - 1) for i in range(distance, count)]),
    )


def stream_step(states, parts, part_of, distance, count, waiting=()):
    moved = []
    for stream, state in enumerate(states):
        part_at = part_of(parts, stream)
        to_right = part_at(distance)
        to_left = part_at(-distance)
        if state is not None:
            to_right = added(to_right, state[0])
            to_left = added(to_left, state[1])
        if stream == 0:
            to_right, to_left, parts, waiting = tied(to_right, to_left, parts, waiting)
        else:
            to_right, to_left, parts = tied(to_right, to_left, parts)
        moved.append(
            (
                lax.ppermute(to_right, "tensor", [(i, i + 1) for i in range(0, count - distance)]),
                lax.ppermute(to_left, "tensor", [(i, i - 1) for i in range(distance, count)]),
            )
        )
    return (moved, parts, waiting)


def sum_end(state, part_at):
    return sum(part.astype(jnp.float32) for part in (part_at(0), *state))


def tied(*values):
    return lax.optimization_barrier(values)


def exchanged(me, send_block, count):
    received = {0: send_block(me)}
    for shift in range(1, count):
        received[shift] = lax.ppermute(
            send_block(lax.rem(me + shift, count)),
            "tensor",
            [(i, (i + shift) % count) for i in range(count)],
        )
    return [
        picked(me, received, {i: (i - source) % count for i in range(count)})
        for source in range(count)
    ]


def pair_stages():
    return [
        (axis, 1 << bit)
        for axis in ("ctx", "tensor", "dp")
        for bit in range(lax.axis_size(axis).bit_length() - 1)
    ]


def pair_sum(values, axis, distance):
    return values + lax.ppermute(
        values, axis, [(i, i ^ distance) for i in range(lax.axis_size(axis))]
    )


def shards(
    prompt_in,
    cont_in,
    prompt_len,
    norm_attn,
    w_query,
    key_weight,
    value_weight,
    w_out,
    norm_mlp,
    w_gate,
    w_up,
    w_down,
    prompt_cot,
    cont_cot,
):
    own_rows = prompt_in.shape[1]
    cont_count = cont_in.shape[1]
    width = prompt_in.shape[2]
    cont_rows = cont_count * CONT_LENGTH
    total_rows = own_rows + cont_rows
    key_width = key_weight.shape[1]
    ctx_index = lax.axis_index("ctx")
    count = lax.axis_size("tensor")
    me = lax.axis_index("tensor")
    share_rows = total_rows // count
    share_start = me * share_rows
    head_half = w_out.shape[0] // 2
    kv_heads = key_weight.shape[1] // HEAD_WIDTH
    group_width = w_out.shape[0] // kv_heads
    order = slot_tables(count)
    slot_chunks = [
        picked(me, {i: jnp.int32(i) for i in range(count)}, {i: order[i][s] for i in range(count)})
        for s in range(count)
    ]
    slot_of = [[order[i].index(c) for c in range(count)] for i in range(count)]
    token_length = prompt_len[0]
    gain_attn = norm_attn.astype(jnp.float32)
    gain_mlp = norm_mlp.astype(jnp.float32)

    def share_of(values):
        return lax.dynamic_slice_in_dim(values, share_start, share_rows, 0)

    def slot_order(values):
        return jnp.concatenate(
            [
                lax.dynamic_slice_in_dim(values, slot_chunks[s] * share_rows, share_rows, 0)
                for s in range(count)
            ],
            axis=0,
        )

    def slots_from(arrived):
        return [
            picked(me, arrived, {i: order[i][s] - i for i in range(count)}) for s in range(count)
        ]

    def slot_part(parts):
        return lambda distance: picked(
            me,
            parts,
            {i: slot_of[i][i + distance] for i in range(count) if 0 <= i + distance < count},
        )

    own_out_half = lax.dynamic_slice_in_dim(w_out, ctx_index * head_half, head_half, 0)
    full_out = lax.all_gather(own_out_half, ("tensor", "ctx"), axis=0, tiled=True)
    token_rows = jnp.concatenate([prompt_in[0], cont_in[0].reshape(cont_rows, width)], axis=0)
    all_rows = token_rows.astype(jnp.float32)
    input_share = share_of(token_rows).astype(jnp.float32)
    within = jnp.arange(cont_rows, dtype=jnp.int32) % CONT_LENGTH
    positions = jnp.concatenate(
        [ctx_index * own_rows + jnp.arange(own_rows, dtype=jnp.int32), token_length + within]
    )
    cos_table, sin_table = (table.T for table in angle_tables(positions))
    act_a = norm_rows(all_rows, gain_attn).astype(jnp.bfloat16)
    query_rows = rotate(
        jnp.einsum("rd,dq->qr", act_a, w_query, preferred_element_type=jnp.float32),
        cos_table,
        sin_table,
    ).astype(jnp.bfloat16)
    joined_keys = (
        rotate(
            jnp.einsum("rd,dq->qr", act_a, key_weight, preferred_element_type=jnp.float32),
            cos_table,
            sin_table,
        )
        .astype(jnp.bfloat16)
        .T
    )
    joined_values = jnp.dot(act_a, value_weight, preferred_element_type=jnp.float32).astype(
        jnp.bfloat16
    )
    local_pairs = jnp.concatenate([joined_keys[:own_rows], joined_values[:own_rows]], axis=1)
    prompt_pairs = lax.all_gather(local_pairs, "ctx", axis=0, tiled=True)
    shared_prompt_keys = prompt_pairs[:, :key_width]
    shared_prompt_values = prompt_pairs[:, key_width:]
    meta = jnp.stack([token_length, ctx_index * own_rows]).astype(jnp.int32)

    def head_inputs(head, prompt):
        wide = slice(head * group_width, (head + 1) * group_width)
        thin = slice(head * HEAD_WIDTH, (head + 1) * HEAD_WIDTH)
        shared = (shared_prompt_keys[:, thin], shared_prompt_values[:, thin])
        if prompt:
            return (meta, query_rows[wide, :own_rows], *shared, None, None)
        return (
            meta,
            query_rows[wide, own_rows:],
            *shared,
            joined_keys[own_rows:, thin],
            joined_values[own_rows:, thin],
        )

    mixed_list = []
    totals = {}
    share_list = []
    for head in range(kv_heads):
        mixed_prompt, totals[head, True] = attend_forward(*head_inputs(head, True))
        mixed_cont, totals[head, False] = attend_forward(*head_inputs(head, False))
        mixed = jnp.concatenate([mixed_prompt, mixed_cont], axis=1).T
        mixed_list.append(mixed)
        share_list.append(
            exchanged(
                me,
                lambda target: lax.dynamic_slice_in_dim(mixed, target * share_rows, share_rows, 0),
                count,
            )
        )
    upstream = jnp.concatenate([prompt_cot[0], cont_cot[0].reshape(cont_rows, width)], axis=0)
    grad_mlp = slot_order((branch_scale * upstream.astype(jnp.float32)).astype(jnp.bfloat16))
    mixed_list[-1], grad_mlp = tied(mixed_list[-1], grad_mlp)
    grad_hidden = jnp.einsum("rd,fd->rf", grad_mlp, w_down, preferred_element_type=jnp.float32)
    share_list[-1], grad_hidden = tied(share_list[-1], grad_hidden)
    mixed_heads = jnp.concatenate(mixed_list, axis=1)
    mixed_share = jnp.concatenate(
        [share_list[head][source] for source in range(count) for head in range(kv_heads)], axis=1
    )
    attn_share = jnp.dot(mixed_share, full_out, preferred_element_type=jnp.float32)
    hidden_share = input_share + branch_scale * attn_share
    act_b_share = norm_rows(hidden_share, gain_mlp).astype(jnp.bfloat16)
    forward, backward = (act_b_share, act_b_share)
    arrived = {0: act_b_share}
    act_b_slots = []
    hidden_list, gate_list, up_list, part_list = ([], [], [], [])
    for s in range(count):
        act_b_slots.append(
            picked(me, arrived, {i: order[i][s] - i for i in range(count)})
        )
        if s + 1 < count:
            forward, backward = hop_step(forward, backward, s + 1, count)
        gate_proj = jnp.dot(act_b_slots[s], w_gate, preferred_element_type=jnp.float32)
        up_proj = jnp.dot(act_b_slots[s], w_up, preferred_element_type=jnp.float32)
        sigmoid_gate = jax.nn.sigmoid(gate_proj)
        silu_gate = gate_proj * sigmoid_gate
        grad_slot = grad_hidden[s * share_rows : (s + 1) * share_rows]
        hidden = (silu_gate * up_proj).astype(jnp.bfloat16)
        grad_gate_slot = (
            grad_slot * up_proj * sigmoid_gate * (1.0 + gate_proj * (1.0 - sigmoid_gate))
        ).astype(jnp.bfloat16)
        grad_up_slot = (grad_slot * silu_gate).astype(jnp.bfloat16)
        part = (
            jnp.einsum("rf,df->rd", grad_gate_slot, w_gate, preferred_element_type=jnp.float32)
            + jnp.einsum("rf,df->rd", grad_up_slot, w_up, preferred_element_type=jnp.float32)
        ).astype(jnp.bfloat16)
        forward, backward, hidden, grad_gate_slot, grad_up_slot, part = tied(
            forward, backward, hidden, grad_gate_slot, grad_up_slot, part
        )
        arrived[-s - 1], arrived[s + 1] = (forward, backward)
        hidden_list.append(hidden)
        gate_list.append(grad_gate_slot)
        up_list.append(grad_up_slot)
        part_list.append(part)
    act_b = jnp.concatenate(act_b_slots, axis=0)
    hidden_act = jnp.concatenate(hidden_list, axis=0)
    grad_gate_act = jnp.concatenate(gate_list, axis=0)
    grad_up_act = jnp.concatenate(up_list, axis=0)

    def over_tokens(values):
        return lax.psum_scatter(
            values.astype(jnp.bfloat16), ("dp", "ctx"), scatter_dimension=0, tiled=True
        )

    streams = (0, 1)
    half_rows = share_rows // len(streams)

    def half(values, stream):
        return values[stream * half_rows : (stream + 1) * half_rows]

    fillers = [
        lambda act, hidden: jnp.einsum(
            "rd,rf->df", act, grad_gate_act, preferred_element_type=jnp.float32
        ),
        lambda act, hidden: jnp.einsum(
            "rd,rf->df", act, grad_up_act, preferred_element_type=jnp.float32
        ),
        lambda act, hidden: jnp.einsum(
            "rf,rd->df", hidden, grad_mlp, preferred_element_type=jnp.float32
        ),
    ]

    def half_part(parts, stream):
        return slot_part([half(part, stream) for part in parts])

    filled = []
    states = [None, None]
    for distance in range(count - 1, 0, -1):
        states, part_list, (act_b, hidden_act) = stream_step(
            states, part_list, half_part, distance, count, (act_b, hidden_act)
        )
        if fillers:
            filled.append(fillers.pop(0)(act_b, hidden_act).astype(jnp.bfloat16))
            states[1], filled[-1] = tied(states[1], filled[-1])
    filled.extend(filler(act_b, hidden_act).astype(jnp.bfloat16) for filler in fillers)
    gate_sum, up_sum, down_sum = (over_tokens(product) for product in filled)
    normed_share = jnp.concatenate(
        [sum_end(states[stream], half_part(part_list, stream)) for stream in streams], axis=0
    )
    through_mlp, gain_mlp_part = norm_back(hidden_share, gain_mlp, normed_share)
    res_share = share_of(upstream).astype(jnp.float32) + through_mlp
    grad_attn_share = (branch_scale * res_share).astype(jnp.bfloat16)
    mixed_grad = jnp.einsum(
        "rd,qd->rq", grad_attn_share, full_out, preferred_element_type=jnp.float32
    ).astype(jnp.bfloat16)
    grad_mixed = jnp.concatenate(
        exchanged(
            me,
            lambda target: lax.dynamic_slice_in_dim(
                mixed_grad, target * w_out.shape[0], w_out.shape[0], 1
            ),
            count,
        ),
        axis=0,
    )
    hidden_act, mixed_grad = tied(hidden_act, mixed_grad)
    mlp_part = jnp.dot(hidden_act, w_down, preferred_element_type=jnp.float32).astype(jnp.bfloat16)
    grad_mixed, mlp_part = tied(grad_mixed, mlp_part)
    mlp_parts = [mlp_part[s * share_rows : (s + 1) * share_rows] for s in range(count)]
    pieces = [(head, prompt) for head in range(kv_heads) for prompt in (True, False)]
    upstream_pieces = {
        (head, prompt): grad_mixed[
            (slice(0, own_rows) if prompt else slice(own_rows, total_rows)),
            head * group_width : (head + 1) * group_width,
        ].T
        for head, prompt in pieces
    }
    piece_grads = {}
    upstream_pieces[pieces[0]], gather_start = tied(upstream_pieces[pieces[0]], grad_attn_share)
    arrived = {0: grad_attn_share}
    forward, backward = (gather_start, gather_start)
    mlp_state = None
    for place in range(max(count, len(pieces))):
        moved = []
        if place < count - 1:
            forward, backward = hop_step(forward, backward, place + 1, count)
            moved += [forward, backward]
        if 1 <= place < count:
            mlp_state = sum_step(mlp_state, slot_part(mlp_parts), count - place, count)
            moved += mlp_state
        if place < len(pieces):
            piece_grads[pieces[place]] = attend_backward(
                *head_inputs(*pieces[place]), totals[pieces[place]], upstream_pieces[pieces[place]]
            )
        if place + 1 < len(pieces):
            following = pieces[place + 1]
            moved, piece_grads[pieces[place]], upstream_pieces[following], mlp_parts = tied(
                moved, piece_grads[pieces[place]], upstream_pieces[following], mlp_parts
            )
        elif place < len(pieces):
            moved, piece_grads[pieces[place]] = tied(moved, piece_grads[pieces[place]])
        if place < count - 1:
            forward, backward, *moved = moved
            arrived[-place - 1], arrived[place + 1] = (forward, backward)
        if 1 <= place < count:
            mlp_state = tuple(moved)
    mlp_share = sum_end(mlp_state, slot_part(mlp_parts))
    result_share = (hidden_share + branch_scale * mlp_share).astype(jnp.bfloat16)
    grad_attn = jnp.concatenate(slots_from(arrived), axis=0)
    query_grad_rows = jnp.concatenate(
        [
            jnp.concatenate([piece_grads[head, True][0], piece_grads[head, False][0]], axis=1)
            for head in range(kv_heads)
        ],
        axis=0,
    )
    query_grad_rows, result_share = tied(query_grad_rows, result_share)
    prompt_pairs_grad = jnp.concatenate(
        [
            piece_grads[head, True][which] + piece_grads[head, False][which]
            for which in (1, 2)
            for head in range(kv_heads)
        ],
        axis=1,
    )
    grad_key_cont, grad_value_cont = (
        jnp.concatenate([piece_grads[head, False][which] for head in range(kv_heads)], axis=1)
        for which in (3, 4)
    )
    other_pairs = lax.ppermute(
        lax.dynamic_slice_in_dim(prompt_pairs_grad, (1 - ctx_index) * own_rows, own_rows, 0),
        "ctx",
        [(0, 1), (1, 0)],
    )
    pair_grads = other_pairs + lax.dynamic_slice_in_dim(
        prompt_pairs_grad, ctx_index * own_rows, own_rows, 0
    )
    key_grad_rows = jnp.concatenate(
        [pair_grads[:, :key_width], grad_key_cont], axis=0
    )
    value_grad_rows = jnp.concatenate(
        [pair_grads[:, key_width:], grad_value_cont], axis=0
    )
    grad_query_lin = rotate(query_grad_rows, cos_table, -sin_table).astype(jnp.bfloat16)
    grad_key_lin = rotate(key_grad_rows.T, cos_table, -sin_table).astype(jnp.bfloat16)
    grad_value_lin = value_grad_rows.astype(jnp.bfloat16)
    input_grad = (
        jnp.einsum("qr,dq->rd", grad_query_lin, w_query, preferred_element_type=jnp.float32)
        + jnp.einsum("qr,dq->rd", grad_key_lin, key_weight, preferred_element_type=jnp.float32)
        + jnp.einsum("rq,dq->rd", grad_value_lin, value_weight, preferred_element_type=jnp.float32)
    )
    input_part = input_grad.astype(jnp.bfloat16)

    def row_part(rows, stream):
        def part_at(distance):
            place = jnp.clip(me + distance, 0, count - 1) * share_rows + stream * half_rows
            return lax.dynamic_slice_in_dim(rows, place, half_rows, 0)

        return part_at

    states = [None, None]
    forward, backward = hop_step(result_share, result_share, 1, count)
    forward, backward, input_part, gate_sum, up_sum = tied(
        forward, backward, input_part, gate_sum, up_sum
    )
    result_arrived = {0: result_share, -1: forward, 1: backward}
    for distance in range(count - 1, 0, -1):
        states, input_part, _ = stream_step(states, input_part, row_part, distance, count)
        step = count - distance + 1
        if step < count:
            forward, backward = hop_step(forward, backward, step, count)
            states[1], forward, backward, down_sum = tied(states[1], forward, backward, down_sum)
            if step == 2:
                states[0], act_a, mixed_heads, grad_attn = tied(
                    states[0], act_a, mixed_heads, grad_attn
                )
            result_arrived[-step], result_arrived[step] = (forward, backward)

    grad_query = jnp.einsum("rd,qr->dq", act_a, grad_query_lin, preferred_element_type=jnp.float32)
    grad_key = jnp.einsum("rd,qr->dq", act_a, grad_key_lin, preferred_element_type=jnp.float32)
    grad_value = jnp.einsum("rd,rq->dq", act_a, grad_value_lin, preferred_element_type=jnp.float32)
    grad_out = jnp.einsum(
        "rq,rd->dq", slot_order(mixed_heads), grad_attn, preferred_element_type=jnp.float32
    )

    def rows_from(arrived):
        chunks = [
            picked(me, stream, {i: c - i for i in range(count)})
            for c in range(count)
            for stream in arrived
        ]
        gathered = jnp.concatenate(chunks, axis=0)
        return (
            gathered[:own_rows][None],
            gathered[own_rows:].reshape(1, cont_count, CONT_LENGTH, width),
        )

    prompt_out, cont_out = rows_from([result_arrived])
    travelling = []
    arrived = []
    gain_attn_part = 0.0
    for stream in streams:
        through_attn, gain_half = norm_back(
            half(input_share, stream), gain_attn, sum_end(states[stream], row_part(input_part, stream))
        )
        gain_attn_part = gain_attn_part + gain_half
        grad_share = (half(res_share, stream) + through_attn).astype(jnp.bfloat16)
        travelling.append((grad_share, grad_share))
        arrived.append({0: grad_share})
    gain_parts = jnp.stack([gain_attn_part, gain_mlp_part])
    stages = pair_stages()
    per_hop = -(-len(stages) // (count - 1))
    for step in range(1, count):
        travelling = [hop_step(*travelling[stream], step, count) for stream in streams]
        for axis, distance in stages[(step - 1) * per_hop : step * per_hop]:
            gain_parts = pair_sum(gain_parts, axis, distance)
        *travelling[1], gain_parts = tied(*travelling[1], gain_parts)
        for stream in streams:
            arrived[stream][-step], arrived[stream][step] = travelling[stream]
    prompt_grad, cont_grad = rows_from(arrived)
    gain_rows = width // (lax.axis_size("dp") * lax.axis_size("ctx"))
    gain_place = (lax.axis_index("dp") * lax.axis_size("ctx") + ctx_index) * gain_rows
    gain_own = lax.dynamic_slice_in_dim(gain_parts, gain_place, gain_rows, 1)
    attn_sum = lax.psum_scatter(
        jnp.concatenate([grad_query, grad_key, grad_value, grad_out], axis=1).astype(jnp.bfloat16),
        ("dp", "ctx"),
        scatter_dimension=0,
        tiled=True,
    ).astype(jnp.float32)
    qw = grad_query.shape[1]
    summed = (
        gain_own[0],
        attn_sum[:, :qw],
        attn_sum[:, qw : qw + key_width],
        attn_sum[:, qw + key_width : qw + 2 * key_width],
        attn_sum[:, qw + 2 * key_width :].T,
        gain_own[1],
        gate_sum.astype(jnp.float32),
        up_sum.astype(jnp.float32),
        down_sum.astype(jnp.float32).T,
    )
    return (
        prompt_out,
        cont_out,
        prompt_grad,
        cont_grad,
        summed[0],
        summed[1],
        summed[2],
        summed[3],
        summed[4],
        summed[5],
        summed[6],
        summed[7],
        summed[8],
    )


def solution(mesh):
    in_specs = (
        P("dp", "ctx", None),
        P("dp", "ctx", None, None),
        P("dp"),
        P(),
        P(None, "tensor"),
        P(None, "tensor"),
        P(None, "tensor"),
        P("tensor", None),
        P(),
        P(None, "tensor"),
        P(None, "tensor"),
        P("tensor", None),
        P("dp", "ctx", None),
        P("dp", "ctx", None, None),
    )
    out_specs = (
        P("dp", "ctx", None),
        P("dp", "ctx", None, None),
        P("dp", "ctx", None),
        P("dp", "ctx", None, None),
        P(("dp", "ctx")),
        P(("dp", "ctx"), "tensor"),
        P(("dp", "ctx"), "tensor"),
        P(("dp", "ctx"), "tensor"),
        P("tensor", ("dp", "ctx")),
        P(("dp", "ctx")),
        P(("dp", "ctx"), "tensor"),
        P(("dp", "ctx"), "tensor"),
        P("tensor", ("dp", "ctx")),
    )
    return jax.shard_map(shards, mesh=mesh, in_specs=in_specs, out_specs=out_specs, check_vma=False)
```

```python
import functools
import math
import operator

import jax
import jax.numpy as jnp
from jax import lax
from jax.experimental import pallas as pl
from jax.experimental.pallas import tpu as pltpu
from jax.sharding import PartitionSpec as P

QUERY_HEADS = 32
KEY_VALUE_HEADS = 8
HEAD_WIDTH = 64
CONT_LENGTH = 128


norm_eps = 1e-05
rope_base = 10000000.0
score_scale = 0.015625
branch_scale = 0.22
masked_score = -1e30


def norm_rows(inputs, weight):
    return inputs * lax.rsqrt(jnp.mean(inputs * inputs, axis=-1, keepdims=True) + norm_eps) * weight


def norm_back(inputs, weight, upstream):
    factor = lax.rsqrt(jnp.mean(inputs * inputs, axis=-1, keepdims=True) + norm_eps)
    scaled = inputs * factor
    weighted = upstream * weight
    through = factor * (weighted - scaled * jnp.mean(weighted * scaled, axis=-1, keepdims=True))
    return (through, jnp.sum(upstream * scaled, axis=0))


def angle_tables(position):
    freq = jnp.exp(
        jnp.arange(HEAD_WIDTH // 2, dtype=jnp.float32) * (-2.0 * math.log(rope_base) / HEAD_WIDTH)
    )
    angle = position.astype(jnp.float32)[:, None] * freq[None, :]
    return (jnp.cos(angle), jnp.sin(angle))


def rotate(inputs, cos_table, sin_table):
    rows = inputs.shape[1]
    halves = inputs.reshape(-1, 2, HEAD_WIDTH // 2, rows)
    first_half = halves[:, 0]
    second_half = halves[:, 1]
    turned = jnp.stack(
        [
            first_half * cos_table[None] - second_half * sin_table[None],
            second_half * cos_table[None] + first_half * sin_table[None],
        ],
        axis=1,
    )
    return turned.reshape(inputs.shape)


HEAD_GROUP = QUERY_HEADS // KEY_VALUE_HEADS
BLOCK = CONT_LENGTH


def lanes_from_heads(block):
    return jnp.concatenate(
        [block[g * HEAD_WIDTH : (g + 1) * HEAD_WIDTH] for g in range(HEAD_GROUP)], axis=1
    )


def heads_from_lanes(block):
    return jnp.concatenate(
        [block[:, g * BLOCK : (g + 1) * BLOCK] for g in range(HEAD_GROUP)], axis=0
    )


def inner(first, second):
    return jnp.dot(first, second, preferred_element_type=jnp.float32)


def across(first, second):
    return lax.dot_general(
        first, second, (((1,), (1,)), ((), ())), preferred_element_type=jnp.float32
    )


def scaled_queries(query_ref):
    return lanes_from_heads(query_ref[...].astype(jnp.float32) * score_scale).astype(jnp.bfloat16)


def block_scores(meta_ref, keys, own_keys, queries):
    lanes = HEAD_GROUP * BLOCK
    scores = inner(keys, queries)
    place = lax.broadcasted_iota(jnp.int32, scores.shape, 0)
    if own_keys is None:
        row = lax.broadcasted_iota(jnp.int32, (1, lanes), 1) % BLOCK
        limit = jnp.minimum(row + (meta_ref[1] + pl.program_id(0) * BLOCK + 1), meta_ref[0])
        return [jnp.where(place < limit, scores, masked_score)]
    own = inner(own_keys, queries)
    own_place = lax.broadcasted_iota(jnp.int32, own.shape, 0)
    own_row = lax.broadcasted_iota(jnp.int32, own.shape, 1) % BLOCK
    return [
        jnp.where(place < meta_ref[0], scores, masked_score),
        jnp.where(own_place <= own_row, own, masked_score),
    ]


def forward_kernel(meta_ref, query_ref, *refs):
    *key_refs, mixed_ref, total_ref = refs
    keys, values_t = key_refs[:2]
    own_keys, own_values_t = key_refs[2:] if len(key_refs) > 2 else (None, None)
    queries = scaled_queries(query_ref)
    parts = block_scores(
        meta_ref, keys[...], None if own_keys is None else own_keys[...], queries
    )
    highest = functools.reduce(
        jnp.maximum, [jnp.max(part, axis=0, keepdims=True) for part in parts]
    )
    weights = [jnp.exp(part - highest) for part in parts]
    total = sum(jnp.sum(weight, axis=0, keepdims=True) for weight in weights)
    mixed = sum(
        inner(ref[...], weight.astype(jnp.bfloat16))
        for ref, weight in zip((values_t, own_values_t), weights)
    )
    mixed_ref[...] = heads_from_lanes(mixed * (1.0 / total)).astype(jnp.bfloat16)
    total_ref[0] = highest + jnp.log(total)


def backward_kernel(meta_ref, query_ref, grad_ref, total_ref, *refs):
    own = len(refs) > 6
    keys, keys_t, values = refs[:3]
    own_keys, own_keys_t, own_values = refs[3:6] if own else (None, None, None)
    query_out, key_out, value_out, *own_out = refs[6:] if own else refs[3:]
    queries = scaled_queries(query_ref)
    grads = lanes_from_heads(grad_ref[...].astype(jnp.float32)).astype(jnp.bfloat16)
    parts = block_scores(meta_ref, keys[...], own_keys[...] if own else None, queries)
    weights = [jnp.exp(part - total_ref[0]) for part in parts]
    grad_weights = [inner(ref[...], grads) for ref, _ in zip((values, own_values), parts)]
    mean = sum(
        jnp.sum(weight * grad, axis=0, keepdims=True)
        for weight, grad in zip(weights, grad_weights)
    )
    grad_scores = [
        (weight * (grad - mean)).astype(jnp.bfloat16)
        for weight, grad in zip(weights, grad_weights)
    ]
    query_grad = sum(inner(ref[...], part) for ref, part in zip((keys_t, own_keys_t), grad_scores))
    query_out[...] = heads_from_lanes(query_grad * score_scale)

    @pl.when(pl.program_id(0) == 0)
    def _():
        key_out[...] = jnp.zeros_like(key_out)
        value_out[...] = jnp.zeros_like(value_out)

    key_out[...] += across(grad_scores[0], queries)
    value_out[...] += across(weights[0].astype(jnp.bfloat16), grads)
    if own:
        own_out[0][...] = across(grad_scores[1], queries)
        own_out[1][...] = across(weights[1].astype(jnp.bfloat16), grads)


def attention_call(kernel, meta, moving, keys, own, outs, products):
    rows = moving[0].shape[1]
    lanes = HEAD_GROUP * BLOCK
    tall = HEAD_GROUP * HEAD_WIDTH
    kinds = {
        "rows": pl.BlockSpec((tall, BLOCK), lambda i, meta: (0, i)),
        "total": pl.BlockSpec((1, 1, lanes), lambda i, meta: (i, 0, 0)),
        "own": pl.BlockSpec((BLOCK, HEAD_WIDTH), lambda i, meta: (i, 0)),
        "own_t": pl.BlockSpec((HEAD_WIDTH, BLOCK), lambda i, meta: (0, i)),
    }

    def whole(shape):
        return pl.BlockSpec(shape, lambda i, meta: (0, 0))

    in_specs = [kinds["total"] if array.ndim == 3 else kinds["rows"] for array in moving]
    in_specs += [whole(array.shape) for array in keys]
    in_specs += [kinds["own" if array.shape[1] == HEAD_WIDTH else "own_t"] for array in own]
    out_specs = [
        whole(out.shape) if kind == "whole" else kinds[kind] for kind, out in outs
    ]
    key_total = keys[0].shape[0] + (BLOCK if own else 0)
    work = HEAD_GROUP * rows * key_total
    return pl.pallas_call(
        kernel,
        out_shape=[out for _, out in outs],
        grid_spec=pltpu.PrefetchScalarGridSpec(
            num_scalar_prefetch=1,
            grid=(rows // BLOCK,),
            in_specs=in_specs,
            out_specs=out_specs,
        ),
        compiler_params=pltpu.CompilerParams(
            dimension_semantics=("arbitrary",), vmem_limit_bytes=40 * 1024 * 1024
        ),
        cost_estimate=pl.CostEstimate(
            flops=2 * products * work * HEAD_WIDTH,
            bytes_accessed=2 * (sum(array.size for array in moving) + 4 * keys[0].size),
            transcendentals=work,
        ),
    )(meta, *moving, *keys, *own)


def attend_forward(meta, queries, keys, values, own_keys, own_values):
    rows = queries.shape[1]
    own = [] if own_keys is None else [own_keys, own_values.T]
    return attention_call(
        forward_kernel,
        meta,
        [queries],
        [keys, values.T],
        own,
        [
            ("rows", jax.ShapeDtypeStruct(queries.shape, jnp.bfloat16)),
            (
                "total",
                jax.ShapeDtypeStruct((rows // BLOCK, 1, HEAD_GROUP * BLOCK), jnp.float32),
            ),
        ],
        2,
    )


def attend_backward(meta, queries, keys, values, own_keys, own_values, totals, upstream):
    own = [] if own_keys is None else [own_keys, own_keys.T, own_values]
    key_shape = jax.ShapeDtypeStruct(keys.shape, jnp.float32)
    outs = [("rows", jax.ShapeDtypeStruct(queries.shape, jnp.float32))]
    outs += [("whole", key_shape), ("whole", key_shape)]
    if own:
        outs += [("own", jax.ShapeDtypeStruct(own_keys.shape, jnp.float32))] * 2
    return attention_call(
        backward_kernel,
        meta,
        [queries, upstream, totals],
        [keys, keys.T, values],
        own,
        outs,
        5,
    )


def picked(me, arrays, keys):
    out = None
    for key in dict.fromkeys(keys.values()):
        if out is None:
            out = arrays[key]
        else:
            chosen = functools.reduce(
                operator.or_, [me == device for device, held in keys.items() if held == key]
            )
            out = jnp.where(chosen, arrays[key], out)
    return out


def slot_tables(count):
    chunk_of = []
    for device in range(count):
        near = min(device, count - 1 - device)
        far = 1 if device < count - 1 - device else -1
        order = [device]
        for slot in range(1, count):
            if slot <= 2 * near:
                distance = (slot + 1) // 2
                order.append(device - distance if slot % 2 else device + distance)
            else:
                order.append(device + far * (slot - near))
        chunk_of.append(order)
    return chunk_of


def hop_step(forward, backward, step, count):
    return (
        lax.ppermute(forward, "tensor", [(i, i + 1) for i in range(step - 1, count - 1)]),
        lax.ppermute(backward, "tensor", [(i, i - 1) for i in range(1, count - step + 1)]),
    )


def added(first, second):
    return (first.astype(jnp.float32) + second.astype(jnp.float32)).astype(jnp.bfloat16)


def sum_step(state, part_at, distance, count):
    to_right = part_at(distance)
    to_left = part_at(-distance)
    if state is not None:
        to_right = added(to_right, state[0])
        to_left = added(to_left, state[1])
    return (
        lax.ppermute(to_right, "tensor", [(i, i + 1) for i in range(0, count - distance)]),
        lax.ppermute(to_left, "tensor", [(i, i - 1) for i in range(distance, count)]),
    )


def stream_step(states, parts, part_of, distance, count, waiting):
    moved = []
    for stream, state in enumerate(states):
        part_at = part_of(parts, stream)
        to_right = part_at(distance)
        to_left = part_at(-distance)
        if state is not None:
            to_right = added(to_right, state[0])
            to_left = added(to_left, state[1])
        to_right, to_left, parts, waiting = tied(to_right, to_left, parts, waiting)
        moved.append(
            (
                lax.ppermute(to_right, "tensor", [(i, i + 1) for i in range(0, count - distance)]),
                lax.ppermute(to_left, "tensor", [(i, i - 1) for i in range(distance, count)]),
            )
        )
    return (moved, parts, waiting)


def sum_end(state, part_at):
    return sum(part.astype(jnp.float32) for part in (part_at(0), *state))


def tied(*values):
    return lax.optimization_barrier(values)


def exchanged(me, send_block, count):
    received = {0: send_block(me)}
    for shift in range(1, count):
        received[shift] = lax.ppermute(
            send_block(lax.rem(me + shift, count)),
            "tensor",
            [(i, (i + shift) % count) for i in range(count)],
        )
    return [
        picked(me, received, {i: (i - source) % count for i in range(count)})
        for source in range(count)
    ]


def pair_sum(values, axis, distance):
    return values + lax.ppermute(
        values, axis, [(i, i ^ distance) for i in range(lax.axis_size(axis))]
    )


def shards(
    prompt_in,
    cont_in,
    prompt_len,
    norm_attn,
    w_query,
    key_weight,
    value_weight,
    w_out,
    norm_mlp,
    w_gate,
    w_up,
    w_down,
    prompt_cot,
    cont_cot,
):
    own_rows = prompt_in.shape[1]
    cont_count = cont_in.shape[1]
    width = prompt_in.shape[2]
    cont_rows = cont_count * CONT_LENGTH
    total_rows = own_rows + cont_rows
    key_width = key_weight.shape[1]
    ctx_index = lax.axis_index("ctx")
    count = lax.axis_size("tensor")
    me = lax.axis_index("tensor")
    share_rows = total_rows // count
    share_start = me * share_rows
    head_half = w_out.shape[0] // 2
    kv_heads = key_weight.shape[1] // HEAD_WIDTH
    group_width = w_out.shape[0] // kv_heads
    order = slot_tables(count)
    slot_chunks = [
        picked(me, {i: jnp.int32(i) for i in range(count)}, {i: order[i][s] for i in range(count)})
        for s in range(count)
    ]
    slot_of = [[order[i].index(c) for c in range(count)] for i in range(count)]
    token_length = prompt_len[0]
    gain_attn = norm_attn.astype(jnp.float32)
    gain_mlp = norm_mlp.astype(jnp.float32)

    def share_of(values):
        return lax.dynamic_slice_in_dim(values, share_start, share_rows, 0)

    def slot_order(values):
        return jnp.concatenate(
            [
                lax.dynamic_slice_in_dim(values, slot_chunks[s] * share_rows, share_rows, 0)
                for s in range(count)
            ],
            axis=0,
        )

    def slots_from(arrived):
        return [
            picked(me, arrived, {i: order[i][s] - i for i in range(count)}) for s in range(count)
        ]

    def slot_part(parts):
        return lambda distance: picked(
            me,
            parts,
            {i: slot_of[i][i + distance] for i in range(count) if 0 <= i + distance < count},
        )

    own_out_half = lax.dynamic_slice_in_dim(w_out, ctx_index * head_half, head_half, 0)
    full_out = lax.all_gather(own_out_half, ("tensor", "ctx"), axis=0, tiled=True)
    token_rows = jnp.concatenate([prompt_in[0], cont_in[0].reshape(cont_rows, width)], axis=0)
    all_rows = token_rows.astype(jnp.float32)
    input_share = share_of(token_rows).astype(jnp.float32)
    within = jnp.arange(cont_rows, dtype=jnp.int32) % CONT_LENGTH
    positions = jnp.concatenate(
        [ctx_index * own_rows + jnp.arange(own_rows, dtype=jnp.int32), token_length + within]
    )
    cos_table, sin_table = (table.T for table in angle_tables(positions))
    act_a = norm_rows(all_rows, gain_attn).astype(jnp.bfloat16)
    query_rows = rotate(
        jnp.einsum("rd,dq->qr", act_a, w_query, preferred_element_type=jnp.float32),
        cos_table,
        sin_table,
    ).astype(jnp.bfloat16)
    joined_keys = (
        rotate(
            jnp.einsum("rd,dq->qr", act_a, key_weight, preferred_element_type=jnp.float32),
            cos_table,
            sin_table,
        )
        .astype(jnp.bfloat16)
        .T
    )
    joined_values = jnp.dot(act_a, value_weight, preferred_element_type=jnp.float32).astype(
        jnp.bfloat16
    )
    local_pairs = jnp.concatenate([joined_keys[:own_rows], joined_values[:own_rows]], axis=1)
    prompt_pairs = lax.all_gather(local_pairs, "ctx", axis=0, tiled=True)
    shared_prompt_keys = prompt_pairs[:, :key_width]
    shared_prompt_values = prompt_pairs[:, key_width:]
    meta = jnp.stack([token_length, ctx_index * own_rows]).astype(jnp.int32)

    def head_inputs(head, prompt):
        wide = slice(head * group_width, (head + 1) * group_width)
        thin = slice(head * HEAD_WIDTH, (head + 1) * HEAD_WIDTH)
        shared = (shared_prompt_keys[:, thin], shared_prompt_values[:, thin])
        if prompt:
            return (meta, query_rows[wide, :own_rows], *shared, None, None)
        return (
            meta,
            query_rows[wide, own_rows:],
            *shared,
            joined_keys[own_rows:, thin],
            joined_values[own_rows:, thin],
        )

    mixed_list = []
    totals = {}
    share_list = []
    for head in range(kv_heads):
        mixed_prompt, totals[head, True] = attend_forward(*head_inputs(head, True))
        mixed_cont, totals[head, False] = attend_forward(*head_inputs(head, False))
        mixed = jnp.concatenate([mixed_prompt, mixed_cont], axis=1).T
        mixed_list.append(mixed)
        share_list.append(
            exchanged(
                me,
                lambda target: lax.dynamic_slice_in_dim(mixed, target * share_rows, share_rows, 0),
                count,
            )
        )
    upstream = jnp.concatenate([prompt_cot[0], cont_cot[0].reshape(cont_rows, width)], axis=0)
    grad_mlp = slot_order((branch_scale * upstream.astype(jnp.float32)).astype(jnp.bfloat16))
    mixed_list[-1], grad_mlp = tied(mixed_list[-1], grad_mlp)
    grad_hidden = jnp.einsum("rd,fd->rf", grad_mlp, w_down, preferred_element_type=jnp.float32)
    share_list[-1], grad_hidden = tied(share_list[-1], grad_hidden)
    mixed_heads = jnp.concatenate(mixed_list, axis=1)
    mixed_share = jnp.concatenate(
        [share_list[head][source] for source in range(count) for head in range(kv_heads)], axis=1
    )
    attn_share = jnp.dot(mixed_share, full_out, preferred_element_type=jnp.float32)
    hidden_share = input_share + branch_scale * attn_share
    act_b_share = norm_rows(hidden_share, gain_mlp).astype(jnp.bfloat16)
    forward, backward = (act_b_share, act_b_share)
    arrived = {0: act_b_share}
    act_b_slots = []
    hidden_list, gate_list, up_list, part_list = ([], [], [], [])
    for s in range(count):
        act_b_slots.append(
            picked(me, arrived, {i: order[i][s] - i for i in range(count)})
        )
        if s + 1 < count:
            forward, backward = hop_step(forward, backward, s + 1, count)
        gate_proj = jnp.dot(act_b_slots[s], w_gate, preferred_element_type=jnp.float32)
        up_proj = jnp.dot(act_b_slots[s], w_up, preferred_element_type=jnp.float32)
        sigmoid_gate = jax.nn.sigmoid(gate_proj)
        silu_gate = gate_proj * sigmoid_gate
        grad_slot = grad_hidden[s * share_rows : (s + 1) * share_rows]
        hidden = (silu_gate * up_proj).astype(jnp.bfloat16)
        grad_gate_slot = (
            grad_slot * up_proj * sigmoid_gate * (1.0 + gate_proj * (1.0 - sigmoid_gate))
        ).astype(jnp.bfloat16)
        grad_up_slot = (grad_slot * silu_gate).astype(jnp.bfloat16)
        part = (
            jnp.einsum("rf,df->rd", grad_gate_slot, w_gate, preferred_element_type=jnp.float32)
            + jnp.einsum("rf,df->rd", grad_up_slot, w_up, preferred_element_type=jnp.float32)
        ).astype(jnp.bfloat16)
        forward, backward, hidden, grad_gate_slot, grad_up_slot, part = tied(
            forward, backward, hidden, grad_gate_slot, grad_up_slot, part
        )
        arrived[-s - 1], arrived[s + 1] = (forward, backward)
        hidden_list.append(hidden)
        gate_list.append(grad_gate_slot)
        up_list.append(grad_up_slot)
        part_list.append(part)
    act_b = jnp.concatenate(act_b_slots, axis=0)
    hidden_act = jnp.concatenate(hidden_list, axis=0)
    grad_gate_act = jnp.concatenate(gate_list, axis=0)
    grad_up_act = jnp.concatenate(up_list, axis=0)

    def over_tokens(values):
        return lax.psum_scatter(
            values.astype(jnp.bfloat16), ("dp", "ctx"), scatter_dimension=0, tiled=True
        )

    fillers = [
        lambda: jnp.einsum("rd,rf->df", act_b, grad_gate_act, preferred_element_type=jnp.float32),
        lambda: jnp.einsum("rd,rf->df", act_b, grad_up_act, preferred_element_type=jnp.float32),
        lambda: jnp.einsum("rf,rd->df", hidden_act, grad_mlp, preferred_element_type=jnp.float32),
    ]
    filled = []
    state = None
    for distance in range(count - 1, 0, -1):
        state = sum_step(state, slot_part(part_list), distance, count)
        if fillers:
            filled.append(fillers.pop(0)().astype(jnp.bfloat16))
            state, filled[-1] = tied(state, filled[-1])
    filled.extend(filler().astype(jnp.bfloat16) for filler in fillers)
    gate_sum, up_sum, down_sum = (over_tokens(product) for product in filled)
    normed_share = sum_end(state, slot_part(part_list))
    through_mlp, gain_mlp_part = norm_back(hidden_share, gain_mlp, normed_share)
    res_share = share_of(upstream).astype(jnp.float32) + through_mlp
    grad_attn_share = (branch_scale * res_share).astype(jnp.bfloat16)
    mixed_grad = jnp.einsum(
        "rd,qd->rq", grad_attn_share, full_out, preferred_element_type=jnp.float32
    ).astype(jnp.bfloat16)
    grad_mixed = jnp.concatenate(
        exchanged(
            me,
            lambda target: lax.dynamic_slice_in_dim(
                mixed_grad, target * w_out.shape[0], w_out.shape[0], 1
            ),
            count,
        ),
        axis=0,
    )
    hidden_act, mixed_grad = tied(hidden_act, mixed_grad)
    mlp_part = jnp.dot(hidden_act, w_down, preferred_element_type=jnp.float32).astype(jnp.bfloat16)
    grad_mixed, mlp_part = tied(grad_mixed, mlp_part)
    mlp_parts = [mlp_part[s * share_rows : (s + 1) * share_rows] for s in range(count)]
    pieces = [(head, prompt) for head in range(kv_heads) for prompt in (True, False)]
    upstream_pieces = {
        (head, prompt): grad_mixed[
            (slice(0, own_rows) if prompt else slice(own_rows, total_rows)),
            head * group_width : (head + 1) * group_width,
        ].T
        for head, prompt in pieces
    }
    piece_grads = {}
    upstream_pieces[pieces[0]], gather_start = tied(upstream_pieces[pieces[0]], grad_attn_share)
    arrived = {0: grad_attn_share}
    forward, backward = (gather_start, gather_start)
    mlp_state = None
    for place in range(max(count, len(pieces))):
        moved = []
        if place < count - 1:
            forward, backward = hop_step(forward, backward, place + 1, count)
            moved += [forward, backward]
        if 1 <= place < count:
            mlp_state = sum_step(mlp_state, slot_part(mlp_parts), count - place, count)
            moved += mlp_state
        if place < len(pieces):
            piece_grads[pieces[place]] = attend_backward(
                *head_inputs(*pieces[place]), totals[pieces[place]], upstream_pieces[pieces[place]]
            )
        if place + 1 < len(pieces):
            following = pieces[place + 1]
            moved, piece_grads[pieces[place]], upstream_pieces[following], mlp_parts = tied(
                moved, piece_grads[pieces[place]], upstream_pieces[following], mlp_parts
            )
        elif place < len(pieces):
            moved, piece_grads[pieces[place]] = tied(moved, piece_grads[pieces[place]])
        if place < count - 1:
            forward, backward, *moved = moved
            arrived[-place - 1], arrived[place + 1] = (forward, backward)
        if 1 <= place < count:
            mlp_state = tuple(moved)
    mlp_share = sum_end(mlp_state, slot_part(mlp_parts))
    result_share = (hidden_share + branch_scale * mlp_share).astype(jnp.bfloat16)
    grad_attn = jnp.concatenate(slots_from(arrived), axis=0)
    query_grad_rows = jnp.concatenate(
        [
            jnp.concatenate([piece_grads[head, True][0], piece_grads[head, False][0]], axis=1)
            for head in range(kv_heads)
        ],
        axis=0,
    )
    query_grad_rows, result_share = tied(query_grad_rows, result_share)
    prompt_pairs_grad = jnp.concatenate(
        [
            piece_grads[head, True][which] + piece_grads[head, False][which]
            for which in (1, 2)
            for head in range(kv_heads)
        ],
        axis=1,
    )
    grad_key_cont, grad_value_cont = (
        jnp.concatenate([piece_grads[head, False][which] for head in range(kv_heads)], axis=1)
        for which in (3, 4)
    )
    other_pairs = lax.ppermute(
        lax.dynamic_slice_in_dim(prompt_pairs_grad, (1 - ctx_index) * own_rows, own_rows, 0),
        "ctx",
        [(0, 1), (1, 0)],
    )
    pair_grads = other_pairs + lax.dynamic_slice_in_dim(
        prompt_pairs_grad, ctx_index * own_rows, own_rows, 0
    )
    key_grad_rows = jnp.concatenate(
        [pair_grads[:, :key_width], grad_key_cont], axis=0
    )
    value_grad_rows = jnp.concatenate(
        [pair_grads[:, key_width:], grad_value_cont], axis=0
    )
    grad_query_lin = rotate(query_grad_rows, cos_table, -sin_table).astype(jnp.bfloat16)
    grad_key_lin = rotate(key_grad_rows.T, cos_table, -sin_table).astype(jnp.bfloat16)
    grad_value_lin = value_grad_rows.astype(jnp.bfloat16)
    input_grad = (
        jnp.einsum("qr,dq->rd", grad_query_lin, w_query, preferred_element_type=jnp.float32)
        + jnp.einsum("qr,dq->rd", grad_key_lin, key_weight, preferred_element_type=jnp.float32)
        + jnp.einsum("rq,dq->rd", grad_value_lin, value_weight, preferred_element_type=jnp.float32)
    )
    input_part = input_grad.astype(jnp.bfloat16)
    streams = (0,)
    half_rows = share_rows // len(streams)

    def half(values, stream):
        return values[stream * half_rows : (stream + 1) * half_rows]

    scaled_rows = all_rows * lax.rsqrt(
        jnp.mean(all_rows * all_rows, axis=-1, keepdims=True) + norm_eps
    )

    def row_part(rows, stream):
        def part_at(distance):
            place = jnp.clip(me + distance, 0, count - 1) * share_rows + stream * half_rows
            return lax.dynamic_slice_in_dim(rows, place, half_rows, 0)

        return part_at

    states = [None]
    forward, backward = hop_step(result_share, result_share, 1, count)
    forward, backward, input_part, gate_sum, up_sum, input_grad, mixed_heads, grad_attn = tied(
        forward, backward, input_part, gate_sum, up_sum, input_grad, mixed_heads, grad_attn
    )
    result_arrived = {0: result_share, -1: forward, 1: backward}
    for distance in range(count - 1, 0, -1):
        states, input_part, act_a = stream_step(
            states, input_part, row_part, distance, count, act_a
        )
        if distance == count - 1:
            gain_attn_part = jnp.sum(input_grad * scaled_rows, axis=0)
            grad_out = jnp.einsum(
                "rq,rd->dq", slot_order(mixed_heads), grad_attn, preferred_element_type=jnp.float32
            )
            states[0], gain_attn_part, grad_out = tied(
                states[0], gain_attn_part, grad_out.astype(jnp.bfloat16)
            )
        if distance == count - 2:
            grad_query = jnp.einsum("rd,qr->dq", act_a, grad_query_lin, preferred_element_type=jnp.float32)
            grad_key = jnp.einsum("rd,qr->dq", act_a, grad_key_lin, preferred_element_type=jnp.float32)
            grad_value = jnp.einsum("rd,rq->dq", act_a, grad_value_lin, preferred_element_type=jnp.float32)
            attn_grads = jnp.concatenate(
                [
                    product.astype(jnp.bfloat16)
                    for product in (grad_query, grad_key, grad_value, grad_out)
                ],
                axis=1,
            )
            states[0], attn_grads = tied(states[0], attn_grads)
        step = count - distance + 1
        if step < count:
            forward, backward = hop_step(forward, backward, step, count)
            states[0], forward, backward, down_sum = tied(states[0], forward, backward, down_sum)
            result_arrived[-step], result_arrived[step] = (forward, backward)

    def rows_from(arrived):
        chunks = [
            picked(me, stream, {i: c - i for i in range(count)})
            for c in range(count)
            for stream in arrived
        ]
        gathered = jnp.concatenate(chunks, axis=0)
        return (
            gathered[:own_rows][None],
            gathered[own_rows:].reshape(1, cont_count, CONT_LENGTH, width),
        )

    prompt_out, cont_out = rows_from([result_arrived])
    travelling = []
    arrived = []
    for stream in streams:
        through_attn, _ = norm_back(
            half(input_share, stream), gain_attn, sum_end(states[stream], row_part(input_part, stream))
        )
        grad_share = (half(res_share, stream) + through_attn).astype(jnp.bfloat16)
        travelling.append((grad_share, grad_share))
        arrived.append({0: grad_share})
    for step in range(1, count):
        travelling = [hop_step(*travelling[stream], step, count) for stream in streams]
        for stream in streams:
            arrived[stream][-step], arrived[stream][step] = travelling[stream]
    prompt_grad, cont_grad = rows_from(arrived)
    gain_parts = jnp.stack([gain_attn_part, gain_mlp_part])
    for bit in range(count.bit_length() - 1):
        gain_parts = pair_sum(gain_parts, "tensor", 1 << bit)
    gain_own = lax.psum_scatter(gain_parts, ("dp", "ctx"), scatter_dimension=1, tiled=True)
    attn_sum = lax.psum_scatter(
        attn_grads,
        ("dp", "ctx"),
        scatter_dimension=0,
        tiled=True,
    ).astype(jnp.float32)
    qw = grad_query.shape[1]
    summed = (
        gain_own[0],
        attn_sum[:, :qw],
        attn_sum[:, qw : qw + key_width],
        attn_sum[:, qw + key_width : qw + 2 * key_width],
        attn_sum[:, qw + 2 * key_width :].T,
        gain_own[1],
        gate_sum.astype(jnp.float32),
        up_sum.astype(jnp.float32),
        down_sum.astype(jnp.float32).T,
    )
    return (
        prompt_out,
        cont_out,
        prompt_grad,
        cont_grad,
        summed[0],
        summed[1],
        summed[2],
        summed[3],
        summed[4],
        summed[5],
        summed[6],
        summed[7],
        summed[8],
    )


def solution(mesh):
    in_specs = (
        P("dp", "ctx", None),
        P("dp", "ctx", None, None),
        P("dp"),
        P(),
        P(None, "tensor"),
        P(None, "tensor"),
        P(None, "tensor"),
        P("tensor", None),
        P(),
        P(None, "tensor"),
        P(None, "tensor"),
        P("tensor", None),
        P("dp", "ctx", None),
        P("dp", "ctx", None, None),
    )
    out_specs = (
        P("dp", "ctx", None),
        P("dp", "ctx", None, None),
        P("dp", "ctx", None),
        P("dp", "ctx", None, None),
        P(("dp", "ctx")),
        P(("dp", "ctx"), "tensor"),
        P(("dp", "ctx"), "tensor"),
        P(("dp", "ctx"), "tensor"),
        P("tensor", ("dp", "ctx")),
        P(("dp", "ctx")),
        P(("dp", "ctx"), "tensor"),
        P(("dp", "ctx"), "tensor"),
        P("tensor", ("dp", "ctx")),
    )
    return jax.shard_map(shards, mesh=mesh, in_specs=in_specs, out_specs=out_specs, check_vma=False)
```

```python
import functools
import math
import operator

import jax
import jax.numpy as jnp
from jax import lax
from jax.experimental import pallas as pl
from jax.experimental.pallas import tpu as pltpu
from jax.sharding import PartitionSpec as P

QUERY_HEADS = 32
KEY_VALUE_HEADS = 8
HEAD_WIDTH = 64
CONT_LENGTH = 128


norm_eps = 1e-05
rope_base = 10000000.0
score_scale = 0.015625
branch_scale = 0.22
masked_score = -1e30


def norm_rows(inputs, weight):
    return inputs * lax.rsqrt(jnp.mean(inputs * inputs, axis=-1, keepdims=True) + norm_eps) * weight


def norm_back(inputs, weight, upstream):
    factor = lax.rsqrt(jnp.mean(inputs * inputs, axis=-1, keepdims=True) + norm_eps)
    scaled = inputs * factor
    weighted = upstream * weight
    through = factor * (weighted - scaled * jnp.mean(weighted * scaled, axis=-1, keepdims=True))
    return (through, jnp.sum(upstream * scaled, axis=0))


def angle_tables(position):
    freq = jnp.exp(
        jnp.arange(HEAD_WIDTH // 2, dtype=jnp.float32) * (-2.0 * math.log(rope_base) / HEAD_WIDTH)
    )
    angle = position.astype(jnp.float32)[:, None] * freq[None, :]
    return (jnp.cos(angle), jnp.sin(angle))


def rotate(inputs, cos_table, sin_table):
    rows = inputs.shape[1]
    halves = inputs.reshape(-1, 2, HEAD_WIDTH // 2, rows)
    first_half = halves[:, 0]
    second_half = halves[:, 1]
    turned = jnp.stack(
        [
            first_half * cos_table[None] - second_half * sin_table[None],
            second_half * cos_table[None] + first_half * sin_table[None],
        ],
        axis=1,
    )
    return turned.reshape(inputs.shape)


HEAD_GROUP = QUERY_HEADS // KEY_VALUE_HEADS
BLOCK = CONT_LENGTH


def lanes_from_heads(block):
    return jnp.concatenate(
        [block[g * HEAD_WIDTH : (g + 1) * HEAD_WIDTH] for g in range(HEAD_GROUP)], axis=1
    )


def heads_from_lanes(block):
    return jnp.concatenate(
        [block[:, g * BLOCK : (g + 1) * BLOCK] for g in range(HEAD_GROUP)], axis=0
    )


def inner(first, second):
    return jnp.dot(first, second, preferred_element_type=jnp.float32)


def across(first, second):
    return lax.dot_general(
        first, second, (((1,), (1,)), ((), ())), preferred_element_type=jnp.float32
    )


def scaled_queries(query_ref):
    return lanes_from_heads(query_ref[...].astype(jnp.float32) * score_scale).astype(jnp.bfloat16)


def block_scores(meta_ref, keys, own_keys, queries):
    lanes = HEAD_GROUP * BLOCK
    scores = inner(keys, queries)
    place = lax.broadcasted_iota(jnp.int32, scores.shape, 0)
    if own_keys is None:
        row = lax.broadcasted_iota(jnp.int32, (1, lanes), 1) % BLOCK
        limit = jnp.minimum(row + (meta_ref[1] + pl.program_id(0) * BLOCK + 1), meta_ref[0])
        return [jnp.where(place < limit, scores, masked_score)]
    own = inner(own_keys, queries)
    own_place = lax.broadcasted_iota(jnp.int32, own.shape, 0)
    own_row = lax.broadcasted_iota(jnp.int32, own.shape, 1) % BLOCK
    return [
        jnp.where(place < meta_ref[0], scores, masked_score),
        jnp.where(own_place <= own_row, own, masked_score),
    ]


def forward_kernel(meta_ref, query_ref, *refs):
    *key_refs, mixed_ref, total_ref = refs
    keys, values_t = key_refs[:2]
    own_keys, own_values_t = key_refs[2:] if len(key_refs) > 2 else (None, None)
    queries = scaled_queries(query_ref)
    parts = block_scores(
        meta_ref, keys[...], None if own_keys is None else own_keys[...], queries
    )
    highest = functools.reduce(
        jnp.maximum, [jnp.max(part, axis=0, keepdims=True) for part in parts]
    )
    weights = [jnp.exp(part - highest) for part in parts]
    total = sum(jnp.sum(weight, axis=0, keepdims=True) for weight in weights)
    mixed = sum(
        inner(ref[...], weight.astype(jnp.bfloat16))
        for ref, weight in zip((values_t, own_values_t), weights)
    )
    mixed_ref[...] = heads_from_lanes(mixed * (1.0 / total)).astype(jnp.bfloat16)
    total_ref[0] = highest + jnp.log(total)


def backward_kernel(meta_ref, query_ref, grad_ref, total_ref, *refs):
    own = len(refs) > 6
    keys, keys_t, values = refs[:3]
    own_keys, own_keys_t, own_values = refs[3:6] if own else (None, None, None)
    query_out, key_out, value_out, *own_out = refs[6:] if own else refs[3:]
    queries = scaled_queries(query_ref)
    grads = lanes_from_heads(grad_ref[...].astype(jnp.float32)).astype(jnp.bfloat16)
    parts = block_scores(meta_ref, keys[...], own_keys[...] if own else None, queries)
    weights = [jnp.exp(part - total_ref[0]) for part in parts]
    grad_weights = [inner(ref[...], grads) for ref, _ in zip((values, own_values), parts)]
    mean = sum(
        jnp.sum(weight * grad, axis=0, keepdims=True)
        for weight, grad in zip(weights, grad_weights)
    )
    grad_scores = [
        (weight * (grad - mean)).astype(jnp.bfloat16)
        for weight, grad in zip(weights, grad_weights)
    ]
    query_grad = sum(inner(ref[...], part) for ref, part in zip((keys_t, own_keys_t), grad_scores))
    query_out[...] = heads_from_lanes(query_grad * score_scale)

    @pl.when(pl.program_id(0) == 0)
    def _():
        key_out[...] = jnp.zeros_like(key_out)
        value_out[...] = jnp.zeros_like(value_out)

    key_out[...] += across(grad_scores[0], queries)
    value_out[...] += across(weights[0].astype(jnp.bfloat16), grads)
    if own:
        own_out[0][...] = across(grad_scores[1], queries)
        own_out[1][...] = across(weights[1].astype(jnp.bfloat16), grads)


def attention_call(kernel, meta, moving, keys, own, outs, products):
    rows = moving[0].shape[1]
    lanes = HEAD_GROUP * BLOCK
    tall = HEAD_GROUP * HEAD_WIDTH
    kinds = {
        "rows": pl.BlockSpec((tall, BLOCK), lambda i, meta: (0, i)),
        "total": pl.BlockSpec((1, 1, lanes), lambda i, meta: (i, 0, 0)),
        "own": pl.BlockSpec((BLOCK, HEAD_WIDTH), lambda i, meta: (i, 0)),
        "own_t": pl.BlockSpec((HEAD_WIDTH, BLOCK), lambda i, meta: (0, i)),
    }

    def whole(shape):
        return pl.BlockSpec(shape, lambda i, meta: (0, 0))

    in_specs = [kinds["total"] if array.ndim == 3 else kinds["rows"] for array in moving]
    in_specs += [whole(array.shape) for array in keys]
    in_specs += [kinds["own" if array.shape[1] == HEAD_WIDTH else "own_t"] for array in own]
    out_specs = [
        whole(out.shape) if kind == "whole" else kinds[kind] for kind, out in outs
    ]
    key_total = keys[0].shape[0] + (BLOCK if own else 0)
    work = HEAD_GROUP * rows * key_total
    return pl.pallas_call(
        kernel,
        out_shape=[out for _, out in outs],
        grid_spec=pltpu.PrefetchScalarGridSpec(
            num_scalar_prefetch=1,
            grid=(rows // BLOCK,),
            in_specs=in_specs,
            out_specs=out_specs,
        ),
        compiler_params=pltpu.CompilerParams(
            dimension_semantics=("arbitrary",), vmem_limit_bytes=40 * 1024 * 1024
        ),
        cost_estimate=pl.CostEstimate(
            flops=2 * products * work * HEAD_WIDTH,
            bytes_accessed=2 * (sum(array.size for array in moving) + 4 * keys[0].size),
            transcendentals=work,
        ),
    )(meta, *moving, *keys, *own)


def attend_forward(meta, queries, keys, values, own_keys, own_values):
    rows = queries.shape[1]
    own = [] if own_keys is None else [own_keys, own_values.T]
    return attention_call(
        forward_kernel,
        meta,
        [queries],
        [keys, values.T],
        own,
        [
            ("rows", jax.ShapeDtypeStruct(queries.shape, jnp.bfloat16)),
            (
                "total",
                jax.ShapeDtypeStruct((rows // BLOCK, 1, HEAD_GROUP * BLOCK), jnp.float32),
            ),
        ],
        2,
    )


def attend_backward(meta, queries, keys, values, own_keys, own_values, totals, upstream):
    own = [] if own_keys is None else [own_keys, own_keys.T, own_values]
    key_shape = jax.ShapeDtypeStruct(keys.shape, jnp.float32)
    outs = [("rows", jax.ShapeDtypeStruct(queries.shape, jnp.float32))]
    outs += [("whole", key_shape), ("whole", key_shape)]
    if own:
        outs += [("own", jax.ShapeDtypeStruct(own_keys.shape, jnp.float32))] * 2
    return attention_call(
        backward_kernel,
        meta,
        [queries, upstream, totals],
        [keys, keys.T, values],
        own,
        outs,
        5,
    )


def picked(me, arrays, keys):
    out = None
    for key in dict.fromkeys(keys.values()):
        if out is None:
            out = arrays[key]
        else:
            chosen = functools.reduce(
                operator.or_, [me == device for device, held in keys.items() if held == key]
            )
            out = jnp.where(chosen, arrays[key], out)
    return out


def slot_tables(count):
    chunk_of = []
    for device in range(count):
        near = min(device, count - 1 - device)
        far = 1 if device < count - 1 - device else -1
        order = [device]
        for slot in range(1, count):
            if slot <= 2 * near:
                distance = (slot + 1) // 2
                order.append(device - distance if slot % 2 else device + distance)
            else:
                order.append(device + far * (slot - near))
        chunk_of.append(order)
    return chunk_of


def hop_step(forward, backward, step, count):
    return (
        lax.ppermute(forward, "tensor", [(i, i + 1) for i in range(step - 1, count - 1)]),
        lax.ppermute(backward, "tensor", [(i, i - 1) for i in range(1, count - step + 1)]),
    )


def added(first, second):
    return (first.astype(jnp.float32) + second.astype(jnp.float32)).astype(jnp.bfloat16)


def sum_step(state, part_at, distance, count):
    to_right = part_at(distance)
    to_left = part_at(-distance)
    if state is not None:
        to_right = added(to_right, state[0])
        to_left = added(to_left, state[1])
    return (
        lax.ppermute(to_right, "tensor", [(i, i + 1) for i in range(0, count - distance)]),
        lax.ppermute(to_left, "tensor", [(i, i - 1) for i in range(distance, count)]),
    )


def stream_step(states, parts, part_of, distance, count):
    moved = []
    for stream, state in enumerate(states):
        part_at = part_of(parts, stream)
        to_right = part_at(distance)
        to_left = part_at(-distance)
        if state is not None:
            to_right = added(to_right, state[0])
            to_left = added(to_left, state[1])
        to_right, to_left, parts = tied(to_right, to_left, parts)
        moved.append(
            (
                lax.ppermute(to_right, "tensor", [(i, i + 1) for i in range(0, count - distance)]),
                lax.ppermute(to_left, "tensor", [(i, i - 1) for i in range(distance, count)]),
            )
        )
    return (moved, parts)


def sum_end(state, part_at):
    return sum(part.astype(jnp.float32) for part in (part_at(0), *state))


def tied(*values):
    return lax.optimization_barrier(values)


def exchanged(me, send_block, count):
    received = {0: send_block(me)}
    for shift in range(1, count):
        received[shift] = lax.ppermute(
            send_block(lax.rem(me + shift, count)),
            "tensor",
            [(i, (i + shift) % count) for i in range(count)],
        )
    return [
        picked(me, received, {i: (i - source) % count for i in range(count)})
        for source in range(count)
    ]


def pair_sum(values, axis, distance):
    return values + lax.ppermute(
        values, axis, [(i, i ^ distance) for i in range(lax.axis_size(axis))]
    )


def shards(
    prompt_in,
    cont_in,
    prompt_len,
    norm_attn,
    w_query,
    key_weight,
    value_weight,
    w_out,
    norm_mlp,
    w_gate,
    w_up,
    w_down,
    prompt_cot,
    cont_cot,
):
    own_rows = prompt_in.shape[1]
    cont_count = cont_in.shape[1]
    width = prompt_in.shape[2]
    cont_rows = cont_count * CONT_LENGTH
    total_rows = own_rows + cont_rows
    key_width = key_weight.shape[1]
    ctx_index = lax.axis_index("ctx")
    count = lax.axis_size("tensor")
    me = lax.axis_index("tensor")
    share_rows = total_rows // count
    share_start = me * share_rows
    head_half = w_out.shape[0] // 2
    kv_heads = key_weight.shape[1] // HEAD_WIDTH
    group_width = w_out.shape[0] // kv_heads
    order = slot_tables(count)
    slot_chunks = [
        picked(me, {i: jnp.int32(i) for i in range(count)}, {i: order[i][s] for i in range(count)})
        for s in range(count)
    ]
    slot_of = [[order[i].index(c) for c in range(count)] for i in range(count)]
    token_length = prompt_len[0]
    gain_attn = norm_attn.astype(jnp.float32)
    gain_mlp = norm_mlp.astype(jnp.float32)

    def share_of(values):
        return lax.dynamic_slice_in_dim(values, share_start, share_rows, 0)

    def slot_order(values):
        return jnp.concatenate(
            [
                lax.dynamic_slice_in_dim(values, slot_chunks[s] * share_rows, share_rows, 0)
                for s in range(count)
            ],
            axis=0,
        )

    def slots_from(arrived):
        return [
            picked(me, arrived, {i: order[i][s] - i for i in range(count)}) for s in range(count)
        ]

    def slot_part(parts):
        return lambda distance: picked(
            me,
            parts,
            {i: slot_of[i][i + distance] for i in range(count) if 0 <= i + distance < count},
        )

    own_out_half = lax.dynamic_slice_in_dim(w_out, ctx_index * head_half, head_half, 0)
    full_out = lax.all_gather(own_out_half, ("tensor", "ctx"), axis=0, tiled=True)
    token_rows = jnp.concatenate([prompt_in[0], cont_in[0].reshape(cont_rows, width)], axis=0)
    all_rows = token_rows.astype(jnp.float32)
    input_share = share_of(token_rows).astype(jnp.float32)
    within = jnp.arange(cont_rows, dtype=jnp.int32) % CONT_LENGTH
    positions = jnp.concatenate(
        [ctx_index * own_rows + jnp.arange(own_rows, dtype=jnp.int32), token_length + within]
    )
    cos_table, sin_table = (table.T for table in angle_tables(positions))
    act_a = norm_rows(all_rows, gain_attn).astype(jnp.bfloat16)
    query_rows = rotate(
        jnp.einsum("rd,dq->qr", act_a, w_query, preferred_element_type=jnp.float32),
        cos_table,
        sin_table,
    ).astype(jnp.bfloat16)
    joined_keys = (
        rotate(
            jnp.einsum("rd,dq->qr", act_a, key_weight, preferred_element_type=jnp.float32),
            cos_table,
            sin_table,
        )
        .astype(jnp.bfloat16)
        .T
    )
    joined_values = jnp.dot(act_a, value_weight, preferred_element_type=jnp.float32).astype(
        jnp.bfloat16
    )
    local_pairs = jnp.concatenate([joined_keys[:own_rows], joined_values[:own_rows]], axis=1)
    prompt_pairs = lax.all_gather(local_pairs, "ctx", axis=0, tiled=True)
    shared_prompt_keys = prompt_pairs[:, :key_width]
    shared_prompt_values = prompt_pairs[:, key_width:]
    meta = jnp.stack([token_length, ctx_index * own_rows]).astype(jnp.int32)

    def head_inputs(head, prompt):
        wide = slice(head * group_width, (head + 1) * group_width)
        thin = slice(head * HEAD_WIDTH, (head + 1) * HEAD_WIDTH)
        shared = (shared_prompt_keys[:, thin], shared_prompt_values[:, thin])
        if prompt:
            return (meta, query_rows[wide, :own_rows], *shared, None, None)
        return (
            meta,
            query_rows[wide, own_rows:],
            *shared,
            joined_keys[own_rows:, thin],
            joined_values[own_rows:, thin],
        )

    mixed_list = []
    totals = {}
    share_list = []
    for head in range(kv_heads):
        mixed_prompt, totals[head, True] = attend_forward(*head_inputs(head, True))
        mixed_cont, totals[head, False] = attend_forward(*head_inputs(head, False))
        mixed = jnp.concatenate([mixed_prompt, mixed_cont], axis=1).T
        mixed_list.append(mixed)
        share_list.append(
            exchanged(
                me,
                lambda target: lax.dynamic_slice_in_dim(mixed, target * share_rows, share_rows, 0),
                count,
            )
        )
    upstream = jnp.concatenate([prompt_cot[0], cont_cot[0].reshape(cont_rows, width)], axis=0)
    grad_mlp = slot_order((branch_scale * upstream.astype(jnp.float32)).astype(jnp.bfloat16))
    mixed_list[-1], grad_mlp = tied(mixed_list[-1], grad_mlp)
    grad_hidden = jnp.einsum("rd,fd->rf", grad_mlp, w_down, preferred_element_type=jnp.float32)
    share_list[-1], grad_hidden = tied(share_list[-1], grad_hidden)
    mixed_heads = jnp.concatenate(mixed_list, axis=1)
    mixed_share = jnp.concatenate(
        [share_list[head][source] for source in range(count) for head in range(kv_heads)], axis=1
    )
    attn_share = jnp.dot(mixed_share, full_out, preferred_element_type=jnp.float32)
    hidden_share = input_share + branch_scale * attn_share
    act_b_share = norm_rows(hidden_share, gain_mlp).astype(jnp.bfloat16)
    forward, backward = (act_b_share, act_b_share)
    arrived = {0: act_b_share}
    act_b_slots = []
    hidden_list, gate_list, up_list, part_list = ([], [], [], [])
    for s in range(count):
        act_b_slots.append(
            picked(me, arrived, {i: order[i][s] - i for i in range(count)})
        )
        if s + 1 < count:
            forward, backward = hop_step(forward, backward, s + 1, count)
        gate_proj = jnp.dot(act_b_slots[s], w_gate, preferred_element_type=jnp.float32)
        up_proj = jnp.dot(act_b_slots[s], w_up, preferred_element_type=jnp.float32)
        sigmoid_gate = jax.nn.sigmoid(gate_proj)
        silu_gate = gate_proj * sigmoid_gate
        grad_slot = grad_hidden[s * share_rows : (s + 1) * share_rows]
        hidden = (silu_gate * up_proj).astype(jnp.bfloat16)
        grad_gate_slot = (
            grad_slot * up_proj * sigmoid_gate * (1.0 + gate_proj * (1.0 - sigmoid_gate))
        ).astype(jnp.bfloat16)
        grad_up_slot = (grad_slot * silu_gate).astype(jnp.bfloat16)
        part = (
            jnp.einsum("rf,df->rd", grad_gate_slot, w_gate, preferred_element_type=jnp.float32)
            + jnp.einsum("rf,df->rd", grad_up_slot, w_up, preferred_element_type=jnp.float32)
        ).astype(jnp.bfloat16)
        forward, backward, hidden, grad_gate_slot, grad_up_slot, part = tied(
            forward, backward, hidden, grad_gate_slot, grad_up_slot, part
        )
        arrived[-s - 1], arrived[s + 1] = (forward, backward)
        hidden_list.append(hidden)
        gate_list.append(grad_gate_slot)
        up_list.append(grad_up_slot)
        part_list.append(part)
    act_b = jnp.concatenate(act_b_slots, axis=0)
    hidden_act = jnp.concatenate(hidden_list, axis=0)
    grad_gate_act = jnp.concatenate(gate_list, axis=0)
    grad_up_act = jnp.concatenate(up_list, axis=0)

    def over_tokens(values):
        return lax.psum_scatter(
            values.astype(jnp.bfloat16), ("dp", "ctx"), scatter_dimension=0, tiled=True
        )

    fillers = [
        lambda: jnp.einsum("rd,rf->df", act_b, grad_gate_act, preferred_element_type=jnp.float32),
        lambda: jnp.einsum("rd,rf->df", act_b, grad_up_act, preferred_element_type=jnp.float32),
        lambda: jnp.einsum("rf,rd->df", hidden_act, grad_mlp, preferred_element_type=jnp.float32),
    ]
    filled = []
    state = None
    for distance in range(count - 1, 0, -1):
        state = sum_step(state, slot_part(part_list), distance, count)
        if fillers:
            filled.append(fillers.pop(0)().astype(jnp.bfloat16))
            state, filled[-1] = tied(state, filled[-1])
    filled.extend(filler().astype(jnp.bfloat16) for filler in fillers)
    gate_sum, up_sum, down_sum = (over_tokens(product) for product in filled)
    normed_share = sum_end(state, slot_part(part_list))
    through_mlp, gain_mlp_part = norm_back(hidden_share, gain_mlp, normed_share)
    res_share = share_of(upstream).astype(jnp.float32) + through_mlp
    grad_attn_share = (branch_scale * res_share).astype(jnp.bfloat16)
    mixed_grad = jnp.einsum(
        "rd,qd->rq", grad_attn_share, full_out, preferred_element_type=jnp.float32
    ).astype(jnp.bfloat16)
    grad_mixed = jnp.concatenate(
        exchanged(
            me,
            lambda target: lax.dynamic_slice_in_dim(
                mixed_grad, target * w_out.shape[0], w_out.shape[0], 1
            ),
            count,
        ),
        axis=0,
    )
    hidden_act, mixed_grad = tied(hidden_act, mixed_grad)
    mlp_part = jnp.dot(hidden_act, w_down, preferred_element_type=jnp.float32).astype(jnp.bfloat16)
    grad_mixed, mlp_part = tied(grad_mixed, mlp_part)
    mlp_parts = [mlp_part[s * share_rows : (s + 1) * share_rows] for s in range(count)]
    pieces = [(head, prompt) for head in range(kv_heads) for prompt in (True, False)]
    upstream_pieces = {
        (head, prompt): grad_mixed[
            (slice(0, own_rows) if prompt else slice(own_rows, total_rows)),
            head * group_width : (head + 1) * group_width,
        ].T
        for head, prompt in pieces
    }
    piece_grads = {}
    upstream_pieces[pieces[0]], gather_start = tied(upstream_pieces[pieces[0]], grad_attn_share)
    arrived = {0: grad_attn_share}
    forward, backward = (gather_start, gather_start)
    mlp_state = None
    for place in range(max(count, len(pieces))):
        moved = []
        if place < count - 1:
            forward, backward = hop_step(forward, backward, place + 1, count)
            moved += [forward, backward]
        if 1 <= place < count:
            mlp_state = sum_step(mlp_state, slot_part(mlp_parts), count - place, count)
            moved += mlp_state
        if place < len(pieces):
            piece_grads[pieces[place]] = attend_backward(
                *head_inputs(*pieces[place]), totals[pieces[place]], upstream_pieces[pieces[place]]
            )
        if place + 1 < len(pieces):
            following = pieces[place + 1]
            moved, piece_grads[pieces[place]], upstream_pieces[following], mlp_parts = tied(
                moved, piece_grads[pieces[place]], upstream_pieces[following], mlp_parts
            )
        elif place < len(pieces):
            moved, piece_grads[pieces[place]] = tied(moved, piece_grads[pieces[place]])
        if place < count - 1:
            forward, backward, *moved = moved
            arrived[-place - 1], arrived[place + 1] = (forward, backward)
        if 1 <= place < count:
            mlp_state = tuple(moved)
    mlp_share = sum_end(mlp_state, slot_part(mlp_parts))
    result_share = (hidden_share + branch_scale * mlp_share).astype(jnp.bfloat16)
    grad_attn = jnp.concatenate(slots_from(arrived), axis=0)
    query_grad_rows = jnp.concatenate(
        [
            jnp.concatenate([piece_grads[head, True][0], piece_grads[head, False][0]], axis=1)
            for head in range(kv_heads)
        ],
        axis=0,
    )
    query_grad_rows, result_share = tied(query_grad_rows, result_share)
    prompt_pairs_grad = jnp.concatenate(
        [
            piece_grads[head, True][which] + piece_grads[head, False][which]
            for which in (1, 2)
            for head in range(kv_heads)
        ],
        axis=1,
    )
    grad_key_cont, grad_value_cont = (
        jnp.concatenate([piece_grads[head, False][which] for head in range(kv_heads)], axis=1)
        for which in (3, 4)
    )
    other_pairs = lax.ppermute(
        lax.dynamic_slice_in_dim(prompt_pairs_grad, (1 - ctx_index) * own_rows, own_rows, 0),
        "ctx",
        [(0, 1), (1, 0)],
    )
    pair_grads = other_pairs + lax.dynamic_slice_in_dim(
        prompt_pairs_grad, ctx_index * own_rows, own_rows, 0
    )
    key_grad_rows = jnp.concatenate(
        [pair_grads[:, :key_width], grad_key_cont], axis=0
    )
    value_grad_rows = jnp.concatenate(
        [pair_grads[:, key_width:], grad_value_cont], axis=0
    )
    grad_query_lin = rotate(query_grad_rows, cos_table, -sin_table).astype(jnp.bfloat16)
    grad_key_lin = rotate(key_grad_rows.T, cos_table, -sin_table).astype(jnp.bfloat16)
    grad_value_lin = value_grad_rows.astype(jnp.bfloat16)
    input_grad = (
        jnp.einsum("qr,dq->rd", grad_query_lin, w_query, preferred_element_type=jnp.float32)
        + jnp.einsum("qr,dq->rd", grad_key_lin, key_weight, preferred_element_type=jnp.float32)
        + jnp.einsum("rq,dq->rd", grad_value_lin, value_weight, preferred_element_type=jnp.float32)
    )
    input_part = input_grad.astype(jnp.bfloat16)
    streams = (0,)
    half_rows = share_rows // len(streams)

    def half(values, stream):
        return values[stream * half_rows : (stream + 1) * half_rows]

    scaled_rows = all_rows * lax.rsqrt(
        jnp.mean(all_rows * all_rows, axis=-1, keepdims=True) + norm_eps
    )

    def row_part(rows, stream):
        def part_at(distance):
            place = jnp.clip(me + distance, 0, count - 1) * share_rows + stream * half_rows
            return lax.dynamic_slice_in_dim(rows, place, half_rows, 0)

        return part_at

    states = [None]
    forward, backward = hop_step(result_share, result_share, 1, count)
    forward, backward, input_part, gate_sum, up_sum, input_grad, mixed_heads, act_a = tied(
        forward, backward, input_part, gate_sum, up_sum, input_grad, mixed_heads, act_a
    )
    result_arrived = {0: result_share, -1: forward, 1: backward}
    for distance in range(count - 1, 0, -1):
        states, input_part = stream_step(states, input_part, row_part, distance, count)
        if distance == count - 1:
            gain_attn_part = jnp.sum(input_grad * scaled_rows, axis=0)
            grad_out = jnp.einsum(
                "rq,rd->dq", slot_order(mixed_heads), grad_attn, preferred_element_type=jnp.float32
            )
            grad_query = jnp.einsum("rd,qr->dq", act_a, grad_query_lin, preferred_element_type=jnp.float32)
            grad_key = jnp.einsum("rd,qr->dq", act_a, grad_key_lin, preferred_element_type=jnp.float32)
            grad_value = jnp.einsum("rd,rq->dq", act_a, grad_value_lin, preferred_element_type=jnp.float32)
            products = [
                product.astype(jnp.bfloat16)
                for product in (grad_query, grad_key, grad_value, grad_out)
            ]
            states[0], gain_attn_part, products = tied(states[0], gain_attn_part, products)
        if distance == count - 2:
            attn_grads = jnp.concatenate(products, axis=1)
            states[0], attn_grads, gain_attn_part = tied(states[0], attn_grads, gain_attn_part)
        step = count - distance + 1
        if step < count:
            forward, backward = hop_step(forward, backward, step, count)
            states[0], forward, backward, down_sum = tied(states[0], forward, backward, down_sum)
            result_arrived[-step], result_arrived[step] = (forward, backward)

    def rows_from(arrived):
        chunks = [
            picked(me, stream, {i: c - i for i in range(count)})
            for c in range(count)
            for stream in arrived
        ]
        gathered = jnp.concatenate(chunks, axis=0)
        return (
            gathered[:own_rows][None],
            gathered[own_rows:].reshape(1, cont_count, CONT_LENGTH, width),
        )

    prompt_out, cont_out = rows_from([result_arrived])
    travelling = []
    arrived = []
    for stream in streams:
        through_attn, _ = norm_back(
            half(input_share, stream), gain_attn, sum_end(states[stream], row_part(input_part, stream))
        )
        grad_share = (half(res_share, stream) + through_attn).astype(jnp.bfloat16)
        travelling.append((grad_share, grad_share))
        arrived.append({0: grad_share})
    for step in range(1, count):
        travelling = [hop_step(*travelling[stream], step, count) for stream in streams]
        for stream in streams:
            arrived[stream][-step], arrived[stream][step] = travelling[stream]
    prompt_grad, cont_grad = rows_from(arrived)
    gain_parts = jnp.stack([gain_attn_part, gain_mlp_part])
    for bit in range(count.bit_length() - 1):
        gain_parts = pair_sum(gain_parts, "tensor", 1 << bit)
    gain_own = lax.psum_scatter(gain_parts, ("dp", "ctx"), scatter_dimension=1, tiled=True)
    attn_sum = lax.psum_scatter(
        attn_grads,
        ("dp", "ctx"),
        scatter_dimension=0,
        tiled=True,
    ).astype(jnp.float32)
    qw = grad_query.shape[1]
    summed = (
        gain_own[0],
        attn_sum[:, :qw],
        attn_sum[:, qw : qw + key_width],
        attn_sum[:, qw + key_width : qw + 2 * key_width],
        attn_sum[:, qw + 2 * key_width :].T,
        gain_own[1],
        gate_sum.astype(jnp.float32),
        up_sum.astype(jnp.float32),
        down_sum.astype(jnp.float32).T,
    )
    return (
        prompt_out,
        cont_out,
        prompt_grad,
        cont_grad,
        summed[0],
        summed[1],
        summed[2],
        summed[3],
        summed[4],
        summed[5],
        summed[6],
        summed[7],
        summed[8],
    )


def solution(mesh):
    in_specs = (
        P("dp", "ctx", None),
        P("dp", "ctx", None, None),
        P("dp"),
        P(),
        P(None, "tensor"),
        P(None, "tensor"),
        P(None, "tensor"),
        P("tensor", None),
        P(),
        P(None, "tensor"),
        P(None, "tensor"),
        P("tensor", None),
        P("dp", "ctx", None),
        P("dp", "ctx", None, None),
    )
    out_specs = (
        P("dp", "ctx", None),
        P("dp", "ctx", None, None),
        P("dp", "ctx", None),
        P("dp", "ctx", None, None),
        P(("dp", "ctx")),
        P(("dp", "ctx"), "tensor"),
        P(("dp", "ctx"), "tensor"),
        P(("dp", "ctx"), "tensor"),
        P("tensor", ("dp", "ctx")),
        P(("dp", "ctx")),
        P(("dp", "ctx"), "tensor"),
        P(("dp", "ctx"), "tensor"),
        P("tensor", ("dp", "ctx")),
    )
    return jax.shard_map(shards, mesh=mesh, in_specs=in_specs, out_specs=out_specs, check_vma=False)
```
